128 devices in a mesh: aa: 32 (over z, y, core), ba: 4 (over x).
Axes of the slice: x: 4, y: 4, z: 4, core: 2. Of those that a mesh axis runs over, the one named last changes fastest.
Arguments:
- features: bfloat16 [262144, 256], P(('aa', 'ba')), may hold values from -6 to 6
- tile_ids: int32 [262144, 1], P(('aa', 'ba')), may hold values from 0 to 127; in each aligned block of 2048 rows (0 to 2047, 2048 to 4095, ...) at most 24 rows name the same one
- cell_ids: int32 [262144], P(('aa', 'ba')), may hold values from 0 to 2047
- spread_weight: float32 [262144], P(('aa', 'ba')), may hold values from 0.1 to 0.6
- read_weight: float32 [262144], P(('aa', 'ba')), may hold values from 0.5 to 2
- message_weight: bfloat16 [256, 256], replicated, may hold values from -0.375 to 0.375
- skip_weight: bfloat16 [256, 256], replicated, may hold values from -0.375 to 0.375
- spectral_weight: bfloat16 [16, 256, 256, 256], P('ba', 'aa'), may hold values from -1.5 to 1.5
- hidden_weight: bfloat16 [256, 256], replicated, may hold values from -0.375 to 0.375
- output_weight: bfloat16 [256, 256], replicated, may hold values from -0.75 to 0.75
Outputs:
- point_out: bfloat16 [262144, 256], P(('aa', 'ba'))
The draws below stay inside these ranges and needn't reach their ends.
Inputs may be any that keep to these rules, and one draw needn't show every extreme that they name: `tile_ids`: among the rows of one device no index appears more than 24 times, and some index appears exactly 24 times.
All inputs are finite; a program needn't handle non-finite values.
Results may differ from the reference program's by a relative error of at most 0.015.
Values may be sent and summed in bfloat16 or wider, within the bound.
No kernel may reach another device: no remote copies, remote signals or barrier semaphores. Data moves between devices by JAX's collectives and lax.ppermute only.
A program may use at most 64 MiB of HBM per device.

```python
import math
import jax
import jax.numpy as jnp
import numpy as np
from jax import lax

C = 256
G = 64
M = 16
P_DEV = 2048
POINTS = 262144
CAP = 24
GXD = 2
GYD = 16
CELLS_DEV = 2048
N_BA = 4
DEVICES = 128


def touch_ends(values, rng, low, largest):
    extent = values.shape
    index_at = [jax.random.randint(jax.random.fold_in(rng, axis), (), 0, extent[axis]) for axis in range(len(extent))]
    values = values.at[tuple(index_at)].set(low)
    longest = extent.index(max(extent))
    index_at[longest] = (index_at[longest] + 1) % extent[longest]
    return values.at[tuple(index_at)].set(largest)


def block_scale(stream_key, shape, pieces, low, top_value):
    factor_of, own = 1.0, jax.random.fold_in(stream_key, 6)
    for axis_at, shards_of in pieces:
        steps = jnp.exp(jax.random.uniform(jax.random.fold_in(own, axis_at), (shards_of,), jnp.float32, low / len(pieces), top_value / len(pieces)))
        factor_of = factor_of * jnp.repeat(steps, shape[axis_at] // shards_of).reshape([-1 if axis == axis_at else 1 for axis in range(len(shape))])
    return factor_of


def deal_out(own_key, own, number, rows, count, top, reach, lean):
    sequence = jax.random.permutation(own_key, count)
    heavy_load, usual = shares(count, rows * top, reach, lean, True), shares(count, rows * top, reach, lean, False)
    places = jnp.arange(count)

    def named(tallies, rotation):
        used = int((tallies > 0).sum())
        fixed = max(1, used // 4)
        moved = fixed + (places - fixed + rotation * (used - fixed)) % max(1, count - fixed)
        return jnp.zeros((count,), jnp.int32).at[sequence[jnp.where(places < fixed, places, moved)]].set(jnp.asarray(tallies, jnp.int32))

    tallies = jnp.where(number % 4 == 0, named(heavy_load, number // 4), named(usual, number - number // 4 - 1))
    mixed = jax.random.permutation(jax.random.fold_in(own, 3), count)
    giver, sink = mixed[0:count // 2 * 2:2], mixed[1:count // 2 * 2:2]
    margin = jnp.minimum(tallies[giver] - 1, reach - tallies[sink]) // 2
    margin = jnp.where((giver == sequence[0]) | (sink == sequence[0]) | (tallies[sink] == 0), 0, jnp.maximum(margin, 0))
    moved = jax.random.randint(jax.random.fold_in(own, 4), (count // 2,), 0, 1 << 20) % (margin + 1)
    tallies = tallies.at[giver].add(-moved).at[sink].add(moved)
    labels = jnp.searchsorted(jnp.cumsum(tallies), jnp.arange(rows * top), side="right").astype(jnp.int32)
    grid = labels.reshape(top, rows).T
    grid = grid[jax.random.permutation(jax.random.fold_in(own, 1), rows)]
    rotation = jax.random.randint(jax.random.fold_in(own, 2), (rows, 1), 0, top)
    return jnp.take_along_axis(grid, (jnp.arange(top)[None, :] + rotation) % top, axis=1)


def shares(count, total, bound, skew, full):
    loads = [(1 << 20) // math.isqrt(grade ** skew) + 1 for grade in range(1, count + 1)]
    largest = bound if full else min(bound, max(-(-total // count), total * loads[0] // sum(loads)))
    least = 1 if total - largest >= count - 1 else 0
    holding, spare = [largest] + [least] * (count - 1), total - largest - least * (count - 1)
    while spare > 0:
        candidates = [i for i in range(1, count) if holding[i] < largest] or [i for i in range(1, count) if holding[i] < bound]
        whole, budget = sum([loads[i] for i in candidates]), spare
        for i in candidates:
            more = min(bound - holding[i], max(1, budget * loads[i] // whole), spare)
            holding[i] = holding[i] + more
            spare = spare - more
    return np.array(holding)


def bell_draw(rng, shape, spread, most, shards=(), kind=jnp.bfloat16):
    entries = jax.random.normal(rng, shape, jnp.float32) * spread
    if len(shards) > 0:
        entries = block_scale(rng, shape, shards, -0.22, 0.18) * entries
    return jnp.clip(entries, min=-most, max=most).astype(kind)


def setup_inputs(seed: int = 0) -> dict:
    splits = jax.random.split(jax.random.key(seed), 11)
    features = bell_draw(splits[0], (POINTS, C), 1.0, 6.0, ((0, 128),))
    tile_ids_keys = jax.random.split(jax.random.fold_in(splits[1], 1), POINTS // P_DEV)
    tile_ids_turns = jax.random.permutation(jax.random.fold_in(splits[1], 3), POINTS // P_DEV)
    tile_ids = jax.vmap(lambda own, number: deal_out(jax.random.fold_in(splits[1], 2), own, number, P_DEV, DEVICES, 1, CAP, 2))(tile_ids_keys, tile_ids_turns).reshape((POINTS, 1))
    cell_ids = touch_ends(jax.random.randint(splits[2], (POINTS,), 0, CELLS_DEV), jax.random.fold_in(splits[2], 1), 0, CELLS_DEV - 1).astype(jnp.int32)
    spread_weight = jnp.clip(0.1 + 0.5 * jax.random.uniform(splits[3], (POINTS,), jnp.float32) ** block_scale(splits[3], (POINTS,), ((0, 128),), -0.2, 0.2), 0.1, 0.6)
    read_weight = jnp.clip(0.5 + 1.5 * jax.random.uniform(splits[4], (POINTS,), jnp.float32) ** block_scale(splits[4], (POINTS,), ((0, 128),), -0.2, 0.2), 0.5, 2.0)
    message_weight = bell_draw(splits[5], (C, C), C ** -0.5, 0.375)
    skip_weight = bell_draw(splits[6], (C, C), C ** -0.5, 0.375)
    spectral_weight = bell_draw(splits[7], (M, M * M, C, C), (C // 16) ** -0.5, 1.5, ((0, 4), (1, 32)))
    hidden_weight = bell_draw(splits[8], (C, C), C ** -0.5, 0.375)
    output_weight = bell_draw(splits[9], (C, C), (C // 4) ** -0.5, 0.75)
    return dict(features=features, tile_ids=tile_ids, cell_ids=cell_ids, spread_weight=spread_weight, read_weight=read_weight, message_weight=message_weight, skip_weight=skip_weight, spectral_weight=spectral_weight, hidden_weight=hidden_weight, output_weight=output_weight)


def basis_table(mode_count, grid_length, positions):
    mode_index = jnp.arange(mode_count, dtype=jnp.int32)[:, None]
    half_modes = mode_count // 2
    frequency = jnp.where(mode_index < half_modes, mode_index, mode_index - half_modes + 1).astype(jnp.float32)
    phase_angle = 2.0 * math.pi * frequency * positions.astype(jnp.float32)[None, :] / grid_length
    waveform = jnp.where(mode_index < half_modes, jnp.cos(phase_angle), jnp.sin(phase_angle))
    norm_scale = jnp.where(mode_index == 0, math.sqrt(1.0 / grid_length), math.sqrt(2.0 / grid_length))
    return (waveform * norm_scale).astype(jnp.float32)

def global_cell(tiles, cells):
    grid_x = tiles // N_BA * GXD + cells // (GYD * G)
    grid_y = tiles % N_BA * GYD + cells // G % GYD
    grid_z = cells % G
    return ((grid_x * G + grid_y) * G + grid_z).astype(jnp.int32)

def reference(features, tile_ids, cell_ids, spread_weight, read_weight, message_weight, skip_weight, spectral_weight, hidden_weight, output_weight):
    highest = lax.Precision.HIGHEST
    block_count = POINTS // P_DEV
    feat_blocks = features.reshape(block_count, P_DEV, C)
    tile_blocks = tile_ids.reshape(block_count, P_DEV)
    cell_blocks = cell_ids.reshape(block_count, P_DEV)
    spread_blocks = spread_weight.reshape(block_count, P_DEV)
    read_blocks = read_weight.reshape(block_count, P_DEV)

    def spread_step(latent_sum, block):
        feat_block, tile_block, cell_block, spread_block = block
        product = jnp.dot(feat_block, message_weight, preferred_element_type=jnp.float32)
        message = (spread_block[:, None] * product).astype(jnp.bfloat16)
        latent_sum = latent_sum.at[global_cell(tile_block, cell_block)].add(message.astype(jnp.float32))
        return (latent_sum, jnp.zeros((), jnp.float32))
    latent_sum, unused = lax.scan(spread_step, jnp.zeros((G * G * G, C), jnp.float32), (feat_blocks, tile_blocks, cell_blocks, spread_blocks))
    latent = latent_sum.astype(jnp.bfloat16)
    basis = basis_table(M, G, jnp.arange(G, dtype=jnp.int32))
    cube = latent.astype(jnp.float32).reshape(G, G, G, C)
    along_z = jnp.einsum('kz,xyzc->xykc', basis, cube, precision=highest)
    along_y = jnp.einsum('jy,xykc->xjkc', basis, along_z, precision=highest)
    spectrum = jnp.einsum('ix,xjkc->jikc', basis, along_y, precision=highest)
    spectrum = spectrum.reshape(M, M * M, C).astype(jnp.bfloat16)

    def mix_row(pair):
        spec_row, weight_row = pair
        return jnp.einsum('mc,mco->mo', spec_row.astype(jnp.float32), weight_row.astype(jnp.float32), precision=highest).astype(jnp.bfloat16)
    mixed = lax.map(mix_row, (spectrum, spectral_weight))
    mixed_cube = mixed.astype(jnp.float32).reshape(M, M, M, C)
    inv_z = jnp.einsum('kz,jikc->jizc', basis, mixed_cube, precision=highest)
    inv_x = jnp.einsum('ix,jizc->jxzc', basis, inv_z, precision=highest)
    inverse = jnp.einsum('jy,jxzc->xyzc', basis, inv_x, precision=highest)
    skip = jnp.dot(latent, skip_weight, preferred_element_type=jnp.float32)
    latent_out = jax.nn.gelu(inverse.reshape(G * G * G, C) + skip).astype(jnp.bfloat16)

    def read_step(carry, block):
        tile_block, cell_block, read_block = block
        rows = latent_out[global_cell(tile_block, cell_block)]
        gathered = (read_block[:, None] * rows.astype(jnp.float32)).astype(jnp.bfloat16)
        hidden = jax.nn.gelu(jnp.dot(gathered, hidden_weight, preferred_element_type=jnp.float32)).astype(jnp.bfloat16)
        result = jnp.dot(hidden, output_weight, preferred_element_type=jnp.float32).astype(jnp.bfloat16)
        return (carry, result)
    carry_out, results = lax.scan(read_step, jnp.zeros((), jnp.float32), (tile_blocks, cell_blocks, read_blocks))
    return results.reshape(POINTS, C)
```

```python
import math

import jax
import jax.numpy as jnp
from jax import lax
from jax.experimental import pallas as pl
from jax.experimental.pallas import tpu as pltpu
from jax.sharding import PartitionSpec as P

G = 64
M = 16
F32 = jnp.float32
BF16 = jnp.bfloat16
VMEM = pl.BlockSpec(memory_space=pltpu.VMEM)
SMEM = pl.BlockSpec(memory_space=pltpu.SMEM)


def iota(shape, dim):
    return lax.broadcasted_iota(jnp.int32, shape, dim)


def mm(a, b):
    return lax.dot_general(a, b, (((1,), (0,)), ((), ())), preferred_element_type=F32)


def mm_nt(a, b):
    return lax.dot_general(a, b, (((1,), (1,)), ((), ())), preferred_element_type=F32)


def as_column(row, lanes):
    n = row.shape[1]
    return jnp.transpose(jnp.broadcast_to(row, (lanes, n)))


def call(body, outs, ins, scratch=(), name=None):
    single = not isinstance(outs, (tuple, list))
    specs = [VMEM if s != "smem" else SMEM for s in ins[1]]
    fn = pl.pallas_call(
        body,
        out_shape=outs,
        in_specs=specs,
        out_specs=VMEM if single else [VMEM] * len(outs),
        scratch_shapes=list(scratch),
        name=name,
    )
    return fn(*ins[0])


def spread_body(feat, tile, cell, spread, weight, send, slots, message, rank_row):
    devices = send.shape[0]
    points = feat.shape[0]
    cap = 24
    upper = (iota((256, 256), 0) < iota((256, 256), 1)).astype(BF16)
    ones = jnp.ones((256, 128), BF16)
    used = jnp.zeros((devices, 256), F32)
    for at in range(0, points, 256):
        hot = tile[:, at : at + 256] == iota((devices, 256), 0)
        hot = hot.astype(F32)
        hot16 = hot.astype(BF16)
        before = mm(hot16, upper) + used
        total = mm(hot16, ones)
        used = used + jnp.concatenate([total, total], axis=1)
        rank = jnp.sum(hot * before, axis=0, keepdims=True).astype(jnp.int32)
        rank_row[:, at : at + 256] = rank
        slots[:, at : at + 256] = tile[:, at : at + 256] * cap + rank
    for at in range(0, points, 128):
        product = mm(feat[at : at + 128, :], weight[...])
        scale = as_column(spread[:, at : at + 128], 128)
        scale = jnp.concatenate([scale, scale], axis=1)
        message[at : at + 128, :] = (scale * product).astype(BF16)
    rank = rank_row[...]
    group = lax.shift_right_logical(rank, 3)
    low = tile[...] * 8 + lax.bitwise_and(rank, 7)
    high_part = lax.shift_right_logical(cell[...], 6).astype(F32)
    low_part = lax.bitwise_and(cell[...], 63).astype(F32)
    lane = iota((128, points), 0)
    where = jnp.where(lane == 2 * group, high_part, 0.0)
    where = jnp.where(lane == 2 * group + 1, low_part, where).astype(BF16)
    slot = slots[...]

    def fill(step, carry):
        base = step * 16
        hot = (slot - base * cap == iota((16 * cap, points), 0)).astype(BF16)
        rows = mm(hot, message[...])
        left = rows[:, :128].reshape(16, cap, 128).astype(BF16)
        right = rows[:, 128:].reshape(16, cap, 128).astype(BF16)
        hot8 = (low - base * 8 == iota((128, points), 0)).astype(BF16)
        placing = mm_nt(hot8, where).reshape(16, 8, 128).astype(BF16)
        send[pl.ds(base, 16), 0:cap, :] = left
        send[pl.ds(base, 16), cap : 2 * cap, :] = right
        send[pl.ds(base, 16), 2 * cap :, :] = placing
        return carry

    lax.fori_loop(0, devices // 16, fill, 0)


def collect_body(recv, basis, latent, places, p0, p1, p2, p3, rows, ids):
    picks = jnp.where(
        iota((8, 128), 1) == 2 * iota((8, 128), 0),
        64.0,
        jnp.where(iota((8, 128), 1) == 2 * iota((8, 128), 0) + 1, 1.0, 0.0),
    ).astype(BF16)

    def unpack(step, carry):
        block = recv[pl.ds(step * 16, 16)].astype(F32)
        place = block[:, 48:56, :].reshape(128, 128).astype(BF16)
        places[pl.ds(step * 128, 128), :] = place
        ids[step] = mm_nt(picks, place).astype(jnp.int32)
        for g in range(3):
            left = block[:, g * 8 : g * 8 + 8, :].reshape(128, 128)
            right = block[:, 24 + g * 8 : 32 + g * 8, :].reshape(128, 128)
            both = jnp.concatenate([left, right], axis=1).astype(BF16)
            rows[pl.ds(step * 384 + g * 128, 128), :] = both
        return carry

    lax.fori_loop(0, 8, unpack, 0)
    tile = 256

    def total(step, carry):
        at = step * tile
        cells = iota((tile, 128), 0) + at
        hot = [
            (ids[i, g : g + 1, :] == cells).astype(BF16) for i in range(8) for g in range(3)
        ]
        latent[pl.ds(at, tile), :] = mm(jnp.concatenate(hot, axis=1), rows[...]).astype(BF16)
        return carry

    lax.fori_loop(0, latent.shape[0] // tile, total, 0)
    for x in range(2):
        part = mm(basis[...], latent[x * 1024 : x * 1024 + 1024, :]).astype(BF16)
        for s, p in enumerate((p0, p1, p2, p3)):
            p[x] = part[s * 64 : s * 64 + 64, :]


def widen_body(a, b, c, d, coef, out):
    total = [
        a[x].astype(F32) + b[x].astype(F32) + c[x].astype(F32) + d[x].astype(F32)
        for x in range(2)
    ]
    halves = [t.reshape(4, 2, 8, 256) for t in total]

    def one(i, carry):
        for h in range(2):
            v = coef[2 * i] * halves[0][:, h] + coef[2 * i + 1] * halves[1][:, h]
            out[2 * i + h] = v.reshape(32, 256).astype(BF16)
        return carry

    lax.fori_loop(0, 16, one, 0)


def mix_body(recv, weight, out):
    spec = jnp.sum(recv[...].astype(F32), axis=0).astype(BF16)
    row = iota((8, 256), 0)
    mixed = jnp.zeros((8, 256), F32)
    for m in range(8):
        mixed = jnp.where(row == m, mm(spec, weight[0, m]), mixed)
    out[...] = jnp.broadcast_to(mixed.astype(BF16)[None], out.shape)


def mix(recv, weight):
    return pl.pallas_call(
        mix_body,
        grid=(4,),
        in_specs=[
            pl.BlockSpec((32, 8, 256), lambda j: (0, j, 0)),
            pl.BlockSpec((1, 8, 256, 256), lambda j: (j, 0, 0, 0)),
        ],
        out_specs=pl.BlockSpec((32, 8, 256), lambda j: (0, j, 0)),
        out_shape=jax.ShapeDtypeStruct((32, 32, 256), BF16),
        name="mix",
    )(recv, weight)


def narrow_body(recv, coef, out):
    for h in range(2):
        acc = [jnp.zeros((4, 8, 256), F32) for x in range(2)]
        for i in range(16):
            v = recv[2 * i + h].astype(F32).reshape(4, 8, 256)
            for x in range(2):
                acc[x] = acc[x] + coef[2 * i + x] * v
        for x in range(2):
            for j in range(4):
                out[x, j * 16 + h * 8 : j * 16 + h * 8 + 8, :] = acc[x][j].astype(BF16)


def finish_body(a, b, c, d, basis, latent, skip, places, out, values):
    for x in range(2):
        modes = jnp.concatenate([a[x], b[x], c[x], d[x]], axis=0)
        for at in range(0, 1024, 256):
            v = mm(basis[at : at + 256, :], modes)
            v = v + mm(latent[x * 1024 + at : x * 1024 + at + 256, :], skip[...])
            values[x * 1024 + at : x * 1024 + at + 256, :] = jax.nn.gelu(v).astype(BF16)

    def back(step, carry):
        place = places[pl.ds(step * 128, 128), :]
        for g in range(3):
            lane = iota((128, 128), 0)
            pick = jnp.where(lane == 2 * g, 64.0, jnp.where(lane == 2 * g + 1, 1.0, 0.0))
            cell = mm(place, pick.astype(BF16)).astype(jnp.int32)
            hot = [
                (cell == iota((128, 128), 1) + 128 * k).astype(BF16) for k in range(16)
            ]
            got = mm(jnp.concatenate(hot, axis=1), values[...])
            out[pl.ds(step * 16, 16), g * 8 : g * 8 + 8, :] = got.reshape(16, 8, 256).astype(BF16)
        return carry

    lax.fori_loop(0, 8, back, 0)


def decode_body(returned, slots, read, hidden_weight, output_weight, out):
    def some(step, carry):
        at = step * 256
        hot = []
        scale = []
        for part in range(2):
            slot = as_column(slots[:, pl.ds(at + part * 128, 128)], 128)
            one = [(slot == iota((128, 128), 1) + 128 * k).astype(BF16) for k in range(24)]
            hot.append(jnp.concatenate(one, axis=1))
            w = as_column(read[:, pl.ds(at + part * 128, 128)], 128)
            scale.append(jnp.concatenate([w, w], axis=1))
        own = mm(jnp.concatenate(hot, axis=0), returned[...])
        gathered = (jnp.concatenate(scale, axis=0) * own).astype(BF16)
        hidden = jax.nn.gelu(mm(gathered, hidden_weight[...])).astype(BF16)
        out[pl.ds(at, 256), :] = mm(hidden, output_weight[...]).astype(BF16)
        return carry

    lax.fori_loop(0, out.shape[0] // 256, some, 0)


def basis_table(mode, position):
    mode = mode[:, None]
    half = M // 2
    frequency = jnp.where(mode < half, mode, mode - half + 1).astype(F32)
    phase = 2.0 * math.pi * frequency * position.astype(F32)[None, :] / G
    wave = jnp.where(mode < half, jnp.cos(phase), jnp.sin(phase))
    return wave * jnp.where(mode == 0, math.sqrt(1.0 / G), math.sqrt(2.0 / G))


def shifted(shard, s):
    return lax.ppermute(shard, "ba", [(i, (i + s) % 4) for i in range(4)])


def per_device(
    features,
    tile_ids,
    cell_ids,
    spread_weight,
    read_weight,
    message_weight,
    skip_weight,
    spectral_weight,
    hidden_weight,
    output_weight,
):
    points, width = features.shape
    devices = lax.axis_size("aa") * lax.axis_size("ba")
    cells = 2048
    shape = jax.ShapeDtypeStruct
    first = lax.axis_index("aa")
    second = lax.axis_index("ba")
    own_y = second * 16 + jnp.arange(16, dtype=jnp.int32)
    modes = jnp.arange(M, dtype=jnp.int32)
    every = jnp.arange(G, dtype=jnp.int32)
    table_z = basis_table(modes, every)
    to_y = basis_table((modes + 4 * second) % M, own_y)
    quarter = modes // 4
    from_y = basis_table(4 * ((second - quarter) % 4) + modes % 4, own_y)
    table_x = basis_table(modes, 2 * first + jnp.arange(2, dtype=jnp.int32))
    table_z, to_y, from_y, table_x = lax.optimization_barrier((table_z, to_y, from_y, table_x))
    coef = table_x.reshape(32)
    basis_to = (to_y[:, None, :, None] * table_z[None, :, None, :]).reshape(256, 1024)
    basis_to = basis_to.astype(BF16)
    basis_from = (jnp.transpose(from_y)[:, None, :, None] * jnp.transpose(table_z)[None, :, None, :])
    basis_from = basis_from.reshape(1024, 256).astype(BF16)

    send, slots = call(
        spread_body,
        (shape((devices, 56, 128), BF16), shape((1, points), jnp.int32)),
        (
            (
                features,
                tile_ids.reshape(1, points),
                cell_ids.reshape(1, points),
                spread_weight.reshape(1, points),
                message_weight,
            ),
            "vvvvv",
        ),
        (pltpu.VMEM((points, width), BF16), pltpu.VMEM((1, points), jnp.int32)),
        "spread",
    )
    recv = lax.all_to_all(send, ("aa", "ba"), 0, 0, tiled=True)
    latent, places, p0, p1, p2, p3 = call(
        collect_body,
        (shape((cells, width), BF16), shape((1024, 128), BF16))
        + (shape((2, 64, width), BF16),) * 4,
        ((recv, basis_to), "vv"),
        (pltpu.VMEM((3072, width), BF16), pltpu.VMEM((8, 8, 128), jnp.int32)),
        "collect",
    )
    wide = call(
        widen_body,
        shape((32, 32, width), BF16),
        ((p0, shifted(p1, 1), shifted(p2, 2), shifted(p3, 3), coef), ["v"] * 4 + ["smem"]),
        (),
        "widen",
    )
    mixed = mix(lax.all_to_all(wide, "aa", 0, 0, tiled=True), spectral_weight)
    lines = call(
        narrow_body,
        shape((2, 64, width), BF16),
        ((lax.all_to_all(mixed, "aa", 0, 0, tiled=True), coef), ["v", "smem"]),
        (),
        "narrow",
    )
    back = call(
        finish_body,
        shape((devices, 24, width), BF16),
        (
            (
                lines,
                shifted(lines, 1),
                shifted(lines, 2),
                shifted(lines, 3),
                basis_from,
                latent,
                skip_weight,
                places,
            ),
            "vvvvvvvv",
        ),
        (pltpu.VMEM((cells, width), BF16),),
        "finish",
    )
    returned = lax.all_to_all(back, ("aa", "ba"), 0, 0, tiled=True)
    return call(
        decode_body,
        shape((points, width), BF16),
        (
            (
                returned.reshape(devices * 24, width),
                slots,
                read_weight.reshape(1, points),
                hidden_weight,
                output_weight,
            ),
            "vvvvv",
        ),
        (),
        "decode",
    )


def solution(mesh):
    placed = (
        P(("aa", "ba"), None),
        P(("aa", "ba"), None),
        P(("aa", "ba")),
        P(("aa", "ba")),
        P(("aa", "ba")),
        P(),
        P(),
        P("ba", "aa", None, None),
        P(),
        P(),
    )
    return jax.shard_map(
        per_device, mesh=mesh, in_specs=placed, out_specs=P(("aa", "ba"), None), check_vma=False
    )
```

```python
import math

import jax
import jax.numpy as jnp
from jax import lax
from jax.experimental import pallas as pl
from jax.experimental.pallas import tpu as pltpu
from jax.sharding import PartitionSpec as P

G = 64
M = 16
F32 = jnp.float32
BF16 = jnp.bfloat16
VMEM = pl.BlockSpec(memory_space=pltpu.VMEM)
SMEM = pl.BlockSpec(memory_space=pltpu.SMEM)


def iota(shape, dim):
    return lax.broadcasted_iota(jnp.int32, shape, dim)


def mm(a, b):
    return lax.dot_general(a, b, (((1,), (0,)), ((), ())), preferred_element_type=F32)


def mm_nt(a, b):
    return lax.dot_general(a, b, (((1,), (1,)), ((), ())), preferred_element_type=F32)


def as_column(row, lanes):
    n = row.shape[1]
    return jnp.transpose(jnp.broadcast_to(row, (lanes, n)))


def call(body, outs, ins, scratch=(), name=None):
    single = not isinstance(outs, (tuple, list))
    specs = [VMEM if s != "smem" else SMEM for s in ins[1]]
    fn = pl.pallas_call(
        body,
        out_shape=outs,
        in_specs=specs,
        out_specs=VMEM if single else [VMEM] * len(outs),
        scratch_shapes=list(scratch),
        name=name,
        compiler_params=pltpu.CompilerParams(vmem_limit_bytes=20 * 2**20),
    )
    return fn(*ins[0])


def spread_body(feat, tile, cell, spread, weight, send, slots, message, rank_row):
    devices = send.shape[0]
    points = feat.shape[0]
    cap = 24
    upper = (iota((256, 256), 0) < iota((256, 256), 1)).astype(BF16)
    ones = jnp.ones((256, 128), BF16)
    used = jnp.zeros((devices, 256), F32)
    for at in range(0, points, 256):
        hot = tile[:, at : at + 256] == iota((devices, 256), 0)
        hot = hot.astype(F32)
        hot16 = hot.astype(BF16)
        before = mm(hot16, upper) + used
        total = mm(hot16, ones)
        used = used + jnp.concatenate([total, total], axis=1)
        rank = jnp.sum(hot * before, axis=0, keepdims=True).astype(jnp.int32)
        rank_row[:, at : at + 256] = rank
        slots[:, at : at + 256] = tile[:, at : at + 256] * cap + rank
    for at in range(0, points, 128):
        product = mm(feat[at : at + 128, :], weight[...])
        scale = as_column(spread[:, at : at + 128], 128)
        scale = jnp.concatenate([scale, scale], axis=1)
        message[at : at + 128, :] = (scale * product).astype(BF16)
    rank = rank_row[...]
    group = lax.shift_right_logical(rank, 3)
    low = tile[...] * 8 + lax.bitwise_and(rank, 7)
    high_part = lax.shift_right_logical(cell[...], 6).astype(F32)
    low_part = lax.bitwise_and(cell[...], 63).astype(F32)
    lane = iota((128, points), 0)
    where = jnp.where(lane == 2 * group, high_part, 0.0)
    where = jnp.where(lane == 2 * group + 1, low_part, where).astype(BF16)
    slot = slots[...]

    def fill(step, carry):
        base = step * 16
        hot = (slot - base * cap == iota((16 * cap, points), 0)).astype(BF16)
        rows = mm(hot, message[...])
        left = rows[:, :128].reshape(16, cap, 128).astype(BF16)
        right = rows[:, 128:].reshape(16, cap, 128).astype(BF16)
        hot8 = (low - base * 8 == iota((128, points), 0)).astype(BF16)
        placing = mm_nt(hot8, where).reshape(16, 8, 128).astype(BF16)
        send[pl.ds(base, 16), 0:cap, :] = left
        send[pl.ds(base, 16), cap : 2 * cap, :] = right
        send[pl.ds(base, 16), 2 * cap :, :] = placing
        return carry

    lax.fori_loop(0, devices // 16, fill, 0)


def collect_body(recv, basis, latent, places, p0, p1, p2, p3, rows, ids):
    picks = jnp.where(
        iota((8, 128), 1) == 2 * iota((8, 128), 0),
        64.0,
        jnp.where(iota((8, 128), 1) == 2 * iota((8, 128), 0) + 1, 1.0, 0.0),
    ).astype(BF16)

    def unpack(step, carry):
        block = recv[pl.ds(step * 16, 16)].astype(F32)
        place = block[:, 48:56, :].reshape(128, 128).astype(BF16)
        places[pl.ds(step * 128, 128), :] = place
        ids[step] = mm_nt(picks, place).astype(jnp.int32)
        for g in range(3):
            left = block[:, g * 8 : g * 8 + 8, :].reshape(128, 128)
            right = block[:, 24 + g * 8 : 32 + g * 8, :].reshape(128, 128)
            both = jnp.concatenate([left, right], axis=1).astype(BF16)
            rows[pl.ds(step * 384 + g * 128, 128), :] = both
        return carry

    lax.fori_loop(0, 8, unpack, 0)
    tile = 256

    def total(step, carry):
        at = step * tile
        cells = iota((tile, 128), 0) + at
        hot = [
            (ids[i, g : g + 1, :] == cells).astype(BF16) for i in range(8) for g in range(3)
        ]
        latent[pl.ds(at, tile), :] = mm(jnp.concatenate(hot, axis=1), rows[...]).astype(BF16)
        return carry

    lax.fori_loop(0, latent.shape[0] // tile, total, 0)
    for x in range(2):
        part = mm(basis[...], latent[x * 1024 : x * 1024 + 1024, :]).astype(BF16)
        for s, p in enumerate((p0, p1, p2, p3)):
            p[x] = part[s * 64 : s * 64 + 64, :]


def widen_body(a, b, c, d, coef, out):
    total = [
        a[x].astype(F32) + b[x].astype(F32) + c[x].astype(F32) + d[x].astype(F32)
        for x in range(2)
    ]
    halves = [t.reshape(4, 2, 8, 256) for t in total]

    def one(i, carry):
        for h in range(2):
            v = coef[2 * i] * halves[0][:, h] + coef[2 * i + 1] * halves[1][:, h]
            out[2 * i + h] = v.reshape(32, 256).astype(BF16)
        return carry

    lax.fori_loop(0, 16, one, 0)


def mix_body(recv, weight, out):
    spec = jnp.sum(recv[...].astype(F32), axis=0).astype(BF16)
    row = iota((8, 256), 0)
    mixed = jnp.zeros((8, 256), F32)
    for m in range(8):
        mixed = jnp.where(row == m, mm(spec, weight[0, m]), mixed)
    out[...] = jnp.broadcast_to(mixed.astype(BF16)[None], out.shape)


def mix(recv, weight):
    return pl.pallas_call(
        mix_body,
        grid=(4,),
        in_specs=[
            pl.BlockSpec((32, 8, 256), lambda j: (0, j, 0)),
            pl.BlockSpec((1, 8, 256, 256), lambda j: (j, 0, 0, 0)),
        ],
        out_specs=pl.BlockSpec((32, 8, 256), lambda j: (0, j, 0)),
        out_shape=jax.ShapeDtypeStruct((32, 32, 256), BF16),
        name="mix",
        compiler_params=pltpu.CompilerParams(vmem_limit_bytes=16 * 2**20),
    )(recv, weight)


def narrow_body(recv, coef, out):
    for h in range(2):
        acc = [jnp.zeros((4, 8, 256), F32) for x in range(2)]
        for i in range(16):
            v = recv[2 * i + h].astype(F32).reshape(4, 8, 256)
            for x in range(2):
                acc[x] = acc[x] + coef[2 * i + x] * v
        for x in range(2):
            for j in range(4):
                out[x, j * 16 + h * 8 : j * 16 + h * 8 + 8, :] = acc[x][j].astype(BF16)


def finish_body(a, b, c, d, basis, latent, skip, places, out, values):
    for x in range(2):
        modes = jnp.concatenate([a[x], b[x], c[x], d[x]], axis=0)
        for at in range(0, 1024, 256):
            v = mm(basis[at : at + 256, :], modes)
            v = v + mm(latent[x * 1024 + at : x * 1024 + at + 256, :], skip[...])
            values[x * 1024 + at : x * 1024 + at + 256, :] = jax.nn.gelu(v).astype(BF16)

    def back(step, carry):
        place = places[pl.ds(step * 128, 128), :]
        for g in range(3):
            lane = iota((128, 128), 0)
            pick = jnp.where(lane == 2 * g, 64.0, jnp.where(lane == 2 * g + 1, 1.0, 0.0))
            cell = mm(place, pick.astype(BF16)).astype(jnp.int32)
            hot = [
                (cell == iota((128, 128), 1) + 128 * k).astype(BF16) for k in range(16)
            ]
            got = mm(jnp.concatenate(hot, axis=1), values[...])
            out[pl.ds(step * 16, 16), g * 8 : g * 8 + 8, :] = got.reshape(16, 8, 256).astype(BF16)
        return carry

    lax.fori_loop(0, 8, back, 0)


def decode_body(returned, slots, read, hidden_weight, output_weight, out):
    def some(step, carry):
        at = step * 256
        hot = []
        scale = []
        for part in range(2):
            slot = as_column(slots[:, pl.ds(at + part * 128, 128)], 128)
            one = [(slot == iota((128, 128), 1) + 128 * k).astype(BF16) for k in range(24)]
            hot.append(jnp.concatenate(one, axis=1))
            w = as_column(read[:, pl.ds(at + part * 128, 128)], 128)
            scale.append(jnp.concatenate([w, w], axis=1))
        own = mm(jnp.concatenate(hot, axis=0), returned[...])
        gathered = (jnp.concatenate(scale, axis=0) * own).astype(BF16)
        hidden = jax.nn.gelu(mm(gathered, hidden_weight[...])).astype(BF16)
        out[pl.ds(at, 256), :] = mm(hidden, output_weight[...]).astype(BF16)
        return carry

    lax.fori_loop(0, out.shape[0] // 256, some, 0)


def basis_table(mode, position):
    mode = mode[:, None]
    half = M // 2
    frequency = jnp.where(mode < half, mode, mode - half + 1).astype(F32)
    phase = 2.0 * math.pi * frequency * position.astype(F32)[None, :] / G
    wave = jnp.where(mode < half, jnp.cos(phase), jnp.sin(phase))
    return wave * jnp.where(mode == 0, math.sqrt(1.0 / G), math.sqrt(2.0 / G))


def shifted(shard, s):
    return lax.ppermute(shard, "ba", [(i, (i + s) % 4) for i in range(4)])


def per_device(
    features,
    tile_ids,
    cell_ids,
    spread_weight,
    read_weight,
    message_weight,
    skip_weight,
    spectral_weight,
    hidden_weight,
    output_weight,
):
    points, width = features.shape
    devices = lax.axis_size("aa") * lax.axis_size("ba")
    cells = 2048
    shape = jax.ShapeDtypeStruct
    first = lax.axis_index("aa")
    second = lax.axis_index("ba")
    own_y = second * 16 + jnp.arange(16, dtype=jnp.int32)
    modes = jnp.arange(M, dtype=jnp.int32)
    every = jnp.arange(G, dtype=jnp.int32)
    table_z = basis_table(modes, every)
    to_y = basis_table((modes + 4 * second) % M, own_y)
    quarter = modes // 4
    from_y = basis_table(4 * ((second - quarter) % 4) + modes % 4, own_y)
    table_x = basis_table(modes, 2 * first + jnp.arange(2, dtype=jnp.int32))
    table_z, to_y, from_y, table_x = lax.optimization_barrier((table_z, to_y, from_y, table_x))
    coef = table_x.reshape(32)
    basis_to = (to_y[:, None, :, None] * table_z[None, :, None, :]).reshape(256, 1024)
    basis_to = basis_to.astype(BF16)
    basis_from = (jnp.transpose(from_y)[:, None, :, None] * jnp.transpose(table_z)[None, :, None, :])
    basis_from = basis_from.reshape(1024, 256).astype(BF16)

    send, slots = call(
        spread_body,
        (shape((devices, 56, 128), BF16), shape((1, points), jnp.int32)),
        (
            (
                features,
                tile_ids.reshape(1, points),
                cell_ids.reshape(1, points),
                spread_weight.reshape(1, points),
                message_weight,
            ),
            "vvvvv",
        ),
        (pltpu.VMEM((points, width), BF16), pltpu.VMEM((1, points), jnp.int32)),
        "spread",
    )
    recv = lax.all_to_all(send, ("aa", "ba"), 0, 0, tiled=True)
    latent, places, p0, p1, p2, p3 = call(
        collect_body,
        (shape((cells, width), BF16), shape((1024, 128), BF16))
        + (shape((2, 64, width), BF16),) * 4,
        ((recv, basis_to), "vv"),
        (pltpu.VMEM((3072, width), BF16), pltpu.VMEM((8, 8, 128), jnp.int32)),
        "collect",
    )
    wide = call(
        widen_body,
        shape((32, 32, width), BF16),
        ((p0, shifted(p1, 1), shifted(p2, 2), shifted(p3, 3), coef), ["v"] * 4 + ["smem"]),
        (),
        "widen",
    )
    mixed = mix(lax.all_to_all(wide, "aa", 0, 0, tiled=True), spectral_weight)
    lines = call(
        narrow_body,
        shape((2, 64, width), BF16),
        ((lax.all_to_all(mixed, "aa", 0, 0, tiled=True), coef), ["v", "smem"]),
        (),
        "narrow",
    )
    back = call(
        finish_body,
        shape((devices, 24, width), BF16),
        (
            (
                lines,
                shifted(lines, 1),
                shifted(lines, 2),
                shifted(lines, 3),
                basis_from,
                latent,
                skip_weight,
                places,
            ),
            "vvvvvvvv",
        ),
        (pltpu.VMEM((cells, width), BF16),),
        "finish",
    )
    returned = lax.all_to_all(back, ("aa", "ba"), 0, 0, tiled=True)
    return call(
        decode_body,
        shape((points, width), BF16),
        (
            (
                returned.reshape(devices * 24, width),
                slots,
                read_weight.reshape(1, points),
                hidden_weight,
                output_weight,
            ),
            "vvvvv",
        ),
        (),
        "decode",
    )


def solution(mesh):
    placed = (
        P(("aa", "ba"), None),
        P(("aa", "ba"), None),
        P(("aa", "ba")),
        P(("aa", "ba")),
        P(("aa", "ba")),
        P(),
        P(),
        P("ba", "aa", None, None),
        P(),
        P(),
    )
    return jax.shard_map(
        per_device, mesh=mesh, in_specs=placed, out_specs=P(("aa", "ba"), None), check_vma=False
    )
```

```python
import math

import jax
import jax.numpy as jnp
from jax import lax
from jax.experimental import pallas as pl
from jax.experimental.pallas import tpu as pltpu
from jax.sharding import Mesh
from jax.sharding import PartitionSpec as P

G = 64
M = 16
F32 = jnp.float32
BF16 = jnp.bfloat16
VMEM = pl.BlockSpec(memory_space=pltpu.VMEM)


def iota(shape, dim):
    return lax.broadcasted_iota(jnp.int32, shape, dim)


def mm(a, b):
    return lax.dot_general(a, b, (((1,), (0,)), ((), ())), preferred_element_type=F32)


def mm_nt(a, b):
    return lax.dot_general(a, b, (((1,), (1,)), ((), ())), preferred_element_type=F32)


def as_column(row, lanes):
    n = row.shape[1]
    return jnp.transpose(jnp.broadcast_to(row, (lanes, n)))


def call(body, outs, ins, scratch=(), name=None, limit=20, flops=1000000):
    single = not isinstance(outs, (tuple, list))
    fn = pl.pallas_call(
        body,
        out_shape=outs,
        in_specs=[VMEM] * len(ins),
        out_specs=VMEM if single else [VMEM] * len(outs),
        scratch_shapes=list(scratch),
        name=name,
        compiler_params=pltpu.CompilerParams(vmem_limit_bytes=limit * 2**20),
        cost_estimate=pl.CostEstimate(flops=flops, transcendentals=0, bytes_accessed=4000000),
    )
    return fn(*ins)


def spread_body(feat, tile, cell, spread, weight, send, slots, message, rank_row):
    devices = send.shape[0]
    points = feat.shape[0]
    cap = 24
    upper = (iota((256, 256), 0) < iota((256, 256), 1)).astype(BF16)
    ones = jnp.ones((256, 128), BF16)
    used = jnp.zeros((devices, 256), F32)
    for at in range(0, points, 256):
        hot = tile[:, at : at + 256] == iota((devices, 256), 0)
        hot = hot.astype(F32)
        hot16 = hot.astype(BF16)
        before = mm(hot16, upper) + used
        total = mm(hot16, ones)
        used = used + jnp.concatenate([total, total], axis=1)
        rank = jnp.sum(hot * before, axis=0, keepdims=True).astype(jnp.int32)
        rank_row[:, at : at + 256] = rank
        slots[:, at : at + 256] = tile[:, at : at + 256] * cap + rank
    for at in range(0, points, 128):
        product = mm(feat[at : at + 128, :], weight[...])
        scale = as_column(spread[:, at : at + 128], 128)
        scale = jnp.concatenate([scale, scale], axis=1)
        message[at : at + 128, :] = (scale * product).astype(BF16)
    rank = rank_row[...]
    group = lax.shift_right_logical(rank, 3)
    low = tile[...] * 8 + lax.bitwise_and(rank, 7)
    high_part = lax.shift_right_logical(cell[...], 6).astype(F32)
    low_part = lax.bitwise_and(cell[...], 63).astype(F32)
    lane = iota((128, points), 0)
    where = jnp.where(lane == 2 * group, high_part, 0.0)
    where = jnp.where(lane == 2 * group + 1, low_part, where).astype(BF16)
    slot = slots[...]

    def fill(step, carry):
        base = step * 16
        hot = (slot - base * cap == iota((16 * cap, points), 0)).astype(BF16)
        rows = mm(hot, message[...])
        left = rows[:, :128].reshape(16, cap, 128).astype(BF16)
        right = rows[:, 128:].reshape(16, cap, 128).astype(BF16)
        hot8 = (low - base * 8 == iota((128, points), 0)).astype(BF16)
        placing = mm_nt(hot8, where).reshape(16, 8, 128).astype(BF16)
        send[pl.ds(base, 16), 0:cap, :] = left
        send[pl.ds(base, 16), cap : 2 * cap, :] = right
        send[pl.ds(base, 16), 2 * cap :, :] = placing
        return carry

    lax.fori_loop(0, devices // 16, fill, 0)


def positions(tile, cell):
    x = lax.shift_right_logical(tile, 2) * 2 + lax.shift_right_logical(cell, 10)
    y = lax.bitwise_and(tile, 3) * 16 + lax.bitwise_and(lax.shift_right_logical(cell, 6), 15)
    return x, y, lax.bitwise_and(cell, 63)


def spectrum_body(message, tile, cell, table_x, table_y, table_z, out, ys, yz, xs):
    points = message.shape[0]
    x, y, z = positions(tile[...], cell[...])

    def values(table, at):
        hot = (at == iota((64, points), 0)).astype(BF16)
        both = mm(table[...], hot)
        half = both.shape[0] // 2
        return both[:half] + both[half:]

    xs[...] = values(table_x, x)
    ys[...] = values(table_y, y)
    zs = values(table_z, z)

    def some(s, carry):
        for j in range(4):
            yz[j * 8 : j * 8 + 8, :] = zs * ys[pl.ds(s * 4 + j, 1), :]
        rows = [(xs[i : i + 1, :] * yz[...]).astype(BF16) for i in range(16)]
        part = mm(jnp.concatenate(rows, axis=0), message[...])
        out[pl.ds(s * 512, 512), :] = part.astype(BF16)
        return carry

    lax.fori_loop(0, 4, some, 0)


def spectrum(message, tile, cell, table_x, table_y, table_z, name):
    points = message.shape[0]
    return call(
        spectrum_body,
        jax.ShapeDtypeStruct((2048, 256), BF16),
        (message, tile, cell, table_x, table_y, table_z),
        (
            pltpu.VMEM((16, points), F32),
            pltpu.VMEM((32, points), F32),
            pltpu.VMEM((16, points), F32),
        ),
        name,
        flops=2 * 2048 * 2048 * 256,
    )


def add_body(*refs):
    count = len(refs) - 4
    total = refs[0][...].astype(F32)
    for r in refs[1:count]:
        total = total + r[...].astype(F32)
    rows = total.shape[0] // 4
    for s in range(4):
        refs[count + s][...] = total[s * rows : s * rows + rows].astype(BF16)


def add_and_cut(parts, name):
    rows, width = parts[0].shape
    piece = jax.ShapeDtypeStruct((rows // 4, width), BF16)
    return call(add_body, (piece,) * 4, parts, (), name)


def join_body(*refs):
    rows = refs[0].shape[0]
    for s in range(4):
        refs[4][s * rows : s * rows + rows, :] = refs[s][...]


def joined(parts, name):
    rows, width = parts[0].shape
    return call(join_body, jax.ShapeDtypeStruct((rows * 4, width), BF16), parts, (), name)


def collect_body(recv, out, rows, ids, places, latent):
    picks = jnp.where(
        iota((8, 128), 1) == 2 * iota((8, 128), 0),
        64.0,
        jnp.where(iota((8, 128), 1) == 2 * iota((8, 128), 0) + 1, 1.0, 0.0),
    ).astype(BF16)

    def unpack(step, carry):
        block = recv[pl.ds(step * 16, 16)].astype(F32)
        place = block[:, 48:56, :].reshape(128, 128).astype(BF16)
        places[pl.ds(step * 128, 128), :] = place
        ids[step] = mm_nt(picks, place).astype(jnp.int32)
        for g in range(3):
            left = block[:, g * 8 : g * 8 + 8, :].reshape(128, 128)
            right = block[:, 24 + g * 8 : 32 + g * 8, :].reshape(128, 128)
            both = jnp.concatenate([left, right], axis=1).astype(BF16)
            rows[pl.ds(step * 384 + g * 128, 128), :] = both
        return carry

    lax.fori_loop(0, 8, unpack, 0)
    tile = 256

    def total(step, carry):
        at = step * tile
        cells = iota((tile, 128), 0) + at
        hot = [
            (ids[i, g : g + 1, :] == cells).astype(BF16) for i in range(8) for g in range(3)
        ]
        latent[pl.ds(at, tile), :] = mm(jnp.concatenate(hot, axis=1), rows[...]).astype(BF16)
        return carry

    lax.fori_loop(0, latent.shape[0] // tile, total, 0)

    def back(step, carry):
        place = places[pl.ds(step * 128, 128), :]
        for g in range(3):
            lane = iota((128, 128), 0)
            pick = jnp.where(lane == 2 * g, 64.0, jnp.where(lane == 2 * g + 1, 1.0, 0.0))
            cell = mm(place, pick.astype(BF16)).astype(jnp.int32)
            hot = [
                (cell == iota((128, 128), 1) + 128 * k).astype(BF16) for k in range(16)
            ]
            got = mm(jnp.concatenate(hot, axis=1), latent[...])
            out[pl.ds(step * 16, 16), g * 8 : g * 8 + 8, :] = got.reshape(16, 8, 256).astype(BF16)
        return carry

    lax.fori_loop(0, 8, back, 0)


def mix_body(a, b, c, d, weight, out):
    spec = a[...].astype(F32) + b[...].astype(F32) + c[...].astype(F32) + d[...].astype(F32)
    spec = spec.astype(BF16)
    row = iota((8, 256), 0)
    for j in range(4):
        mixed = jnp.zeros((8, 256), F32)
        for m in range(8):
            mixed = jnp.where(row == m, mm(spec[j * 8 : j * 8 + 8], weight[j, m]), mixed)
        out[j * 8 : j * 8 + 8, :] = mixed.astype(BF16)


def own_body(returned, slots, skip, out):
    def some(step, carry):
        at = step * 256
        hot = []
        for part in range(2):
            slot = as_column(slots[:, pl.ds(at + part * 128, 128)], 128)
            one = [(slot == iota((128, 128), 1) + 128 * k).astype(BF16) for k in range(24)]
            hot.append(jnp.concatenate(one, axis=1))
        own = mm(jnp.concatenate(hot, axis=0), returned[...]).astype(BF16)
        out[pl.ds(at, 256), :] = mm(own, skip[...])
        return carry

    lax.fori_loop(0, out.shape[0] // 256, some, 0)


def decode_body(
    m0, m1, m2, m3, m4, m5, m6, m7, tile, cell, wide_x, wide_y, wide_z,
    base, read, hidden_weight, output_weight, out, spots,
):
    x, y, z = positions(tile[...], cell[...])
    spots[0:1, :] = x
    spots[1:2, :] = y
    spots[2:3, :] = z
    modes = (m0, m1, m2, m3, m4, m5, m6, m7)
    lane = lax.bitwise_and(iota((256, 128), 1), 63)

    def some(step, carry):
        at = step * 256

        def column(row):
            return jnp.concatenate(
                [as_column(row(at + 128 * part), 128) for part in range(2)], axis=0
            )

        def values(which, table):
            col = column(lambda lo: spots[which : which + 1, pl.ds(lo, 128)])
            return mm((col == lane).astype(BF16), table[...])

        vx = values(0, wide_x)
        vy = values(1, wide_y)
        vz = values(2, wide_z)
        total = base[pl.ds(at, 256), :]
        for h in range(2):
            for s in range(4):
                yz = vy[:, s * 128 : s * 128 + 128] * vz[:, h * 128 : h * 128 + 128]
                wave = [(yz * vx[:, i * 128 : i * 128 + 128]).astype(BF16) for i in range(4)]
                total = total + mm(jnp.concatenate(wave, axis=1), modes[h * 4 + s][...])
        value = jax.nn.gelu(total).astype(BF16).astype(F32)
        scale = column(lambda lo: read[:, pl.ds(lo, 128)])
        gathered = (jnp.concatenate([scale, scale], axis=1) * value).astype(BF16)
        hidden = jax.nn.gelu(mm(gathered, hidden_weight[...])).astype(BF16)
        out[pl.ds(at, 256), :] = mm(hidden, output_weight[...]).astype(BF16)
        return carry

    lax.fori_loop(0, out.shape[0] // 256, some, 0)


def basis_table(mode, position):
    half = M // 2
    frequency = jnp.where(mode < half, mode, mode - half + 1).astype(F32)
    phase = 2.0 * math.pi * frequency * position.astype(F32) / G
    wave = jnp.where(mode < half, jnp.cos(phase), jnp.sin(phase))
    return wave * jnp.where(mode == 0, math.sqrt(1.0 / G), math.sqrt(2.0 / G))


def two_terms(table):
    high = lax.reduce_precision(table, 8, 7)
    return jnp.concatenate([high, table - high], axis=0).astype(BF16)


def around(shard, axis, s):
    return lax.ppermute(shard, axis, [(i, (i + s) % 4) for i in range(4)])


def from_others(pieces, axis):
    return (pieces[0],) + tuple(around(pieces[s], axis, s) for s in (1, 2, 3))


def swapped(shard):
    return lax.ppermute(shard, "core", [(0, 1), (1, 0)])


def per_device(
    features,
    tile_ids,
    cell_ids,
    spread_weight,
    read_weight,
    message_weight,
    skip_weight,
    spectral_weight,
    hidden_weight,
    output_weight,
):
    points, width = features.shape
    everyone = ("z", "y", "core", "ba")
    devices = lax.axis_size(everyone)
    shape = jax.ShapeDtypeStruct
    at_z, at_y, at_core, at_b = (lax.axis_index(a) for a in everyone)
    tile = tile_ids.reshape(1, points)
    cell = cell_ids.reshape(1, points)
    grid = jnp.arange(G, dtype=jnp.int32)

    def mode_x(i, sign):
        return 4 * ((at_z + sign * (i // 4)) % 4) + (at_y + sign * (i % 4)) % 4

    def mode_y(s, j, sign):
        return 4 * ((at_b + sign * s) % 4) + j

    i16 = jnp.arange(16, dtype=jnp.int32)
    k8 = jnp.arange(8, dtype=jnp.int32)
    to_x = two_terms(basis_table(mode_x(i16, 1)[:, None], grid[None, :]))
    to_y = two_terms(basis_table(mode_y(i16 // 4, i16 % 4, 1)[:, None], grid[None, :]))
    other_z = two_terms(basis_table((8 * (1 - at_core) + k8)[:, None], grid[None, :]))
    own_z = two_terms(basis_table((8 * at_core + k8)[:, None], grid[None, :]))
    lane = jnp.arange(512, dtype=jnp.int32)
    wide_x = two_terms(basis_table(mode_x(lane // 32, -1)[None, :], grid[:, None]))
    wide_y = two_terms(
        basis_table(mode_y(lane // 128, lane // 8 % 4, -1)[None, :], grid[:, None])
    )
    lane = lane[:256]
    wide_z = two_terms(
        basis_table((8 * ((at_core + lane // 128) % 2) + lane % 8)[None, :], grid[:, None])
    )

    send, slots, message = call(
        spread_body,
        (
            shape((devices, 56, 128), BF16),
            shape((1, points), jnp.int32),
            shape((points, width), BF16),
        ),
        (features, tile, cell, spread_weight.reshape(1, points), message_weight),
        (pltpu.VMEM((1, points), jnp.int32),),
        "spread",
        limit=60,
    )
    recv = lax.all_to_all(send, everyone, 0, 0, tiled=True)
    away = spectrum(message, tile, cell, to_x, to_y, other_z, "spectrum_away")
    near = spectrum(message, tile, cell, to_x, to_y, own_z, "spectrum_near")
    parts = add_and_cut((near, swapped(away)), "add_core")
    parts = add_and_cut(from_others(parts, "ba"), "add_ba")
    parts = add_and_cut(from_others(parts, "z"), "add_z")
    mixed = call(
        mix_body,
        shape((32, width), BF16),
        from_others(parts, "y") + (spectral_weight,),
        (),
        "mix",
    )
    line = joined(from_others((mixed,) * 4, "y"), "join_y")
    plane = joined(from_others((line,) * 4, "z"), "join_z")
    modes = from_others((plane,) * 4, "ba")
    modes = modes + tuple(swapped(m) for m in modes)

    back = call(
        collect_body,
        shape((devices, 24, width), BF16),
        (recv,),
        (
            pltpu.VMEM((3072, width), BF16),
            pltpu.VMEM((8, 8, 128), jnp.int32),
            pltpu.VMEM((1024, 128), BF16),
            pltpu.VMEM((2048, width), BF16),
        ),
        "collect",
        flops=4 * 3072 * 2048 * 256,
    )
    returned = lax.all_to_all(back, everyone, 0, 0, tiled=True)
    base = call(
        own_body,
        shape((points, width), F32),
        (returned.reshape(devices * 24, width), slots, skip_weight),
        (),
        "own",
        flops=2 * 3072 * 2048 * 256,
    )
    return call(
        decode_body,
        shape((points, width), BF16),
        modes
        + (
            tile,
            cell,
            wide_x,
            wide_y,
            wide_z,
            base,
            read_weight.reshape(1, points),
            hidden_weight,
            output_weight,
        ),
        (pltpu.VMEM((8, points), jnp.int32),),
        "decode",
        flops=2 * 4096 * 2048 * 256,
    )


def solution(mesh):
    finer = Mesh(mesh.devices.reshape(4, 4, 2, 4), ("z", "y", "core", "ba"))
    rows = P(("z", "y", "core", "ba"))
    every = P()
    placed = (
        P(("z", "y", "core", "ba"), None),
        P(("z", "y", "core", "ba"), None),
        rows,
        rows,
        rows,
        every,
        every,
        P("ba", ("z", "y", "core"), None, None),
        every,
        every,
    )
    return jax.shard_map(
        per_device,
        mesh=finer,
        in_specs=placed,
        out_specs=P(("z", "y", "core", "ba"), None),
        check_vma=False,
    )
```

```python
import math

import jax
import jax.numpy as jnp
from jax import lax
from jax.experimental import pallas as pl
from jax.experimental.pallas import tpu as pltpu
from jax.sharding import Mesh
from jax.sharding import PartitionSpec as P

G = 64
M = 16
F32 = jnp.float32
BF16 = jnp.bfloat16
VMEM = pl.BlockSpec(memory_space=pltpu.VMEM)


def iota(shape, dim):
    return lax.broadcasted_iota(jnp.int32, shape, dim)


def mm(a, b):
    return lax.dot_general(a, b, (((1,), (0,)), ((), ())), preferred_element_type=F32)


def mm_nt(a, b):
    return lax.dot_general(a, b, (((1,), (1,)), ((), ())), preferred_element_type=F32)


def as_column(row, lanes):
    n = row.shape[1]
    return jnp.transpose(jnp.broadcast_to(row, (lanes, n)))


def call(body, outs, ins, scratch=(), limit=20, flops=1000000):
    single = not isinstance(outs, (tuple, list))
    fn = pl.pallas_call(
        body,
        out_shape=outs,
        in_specs=[VMEM] * len(ins),
        out_specs=VMEM if single else [VMEM] * len(outs),
        scratch_shapes=list(scratch),
        compiler_params=pltpu.CompilerParams(vmem_limit_bytes=limit * 2**20),
        cost_estimate=pl.CostEstimate(flops=flops, transcendentals=0, bytes_accessed=4000000),
    )
    return fn(*ins)


def spread_body(feat, tile, cell, spread, weight, send, slots, message, rank_row):
    devices = send.shape[0]
    points = feat.shape[0]
    cap = 24
    upper = (iota((256, 256), 0) < iota((256, 256), 1)).astype(BF16)
    ones = jnp.ones((256, 128), BF16)
    used = jnp.zeros((devices, 256), F32)
    for at in range(0, points, 256):
        hot = tile[:, at : at + 256] == iota((devices, 256), 0)
        hot = hot.astype(F32)
        hot16 = hot.astype(BF16)
        before = mm(hot16, upper) + used
        total = mm(hot16, ones)
        used = used + jnp.concatenate([total, total], axis=1)
        rank = jnp.sum(hot * before, axis=0, keepdims=True).astype(jnp.int32)
        rank_row[:, at : at + 256] = rank
        slots[:, at : at + 256] = tile[:, at : at + 256] * cap + rank
    for at in range(0, points, 128):
        product = mm(feat[at : at + 128, :], weight[...])
        scale = as_column(spread[:, at : at + 128], 128)
        scale = jnp.concatenate([scale, scale], axis=1)
        message[at : at + 128, :] = (scale * product).astype(BF16)
    rank = rank_row[...]
    group = lax.shift_right_logical(rank, 3)
    low = tile[...] * 8 + lax.bitwise_and(rank, 7)
    high_part = lax.shift_right_logical(cell[...], 6).astype(F32)
    low_part = lax.bitwise_and(cell[...], 63).astype(F32)
    lane = iota((128, points), 0)
    where = jnp.where(lane == 2 * group, high_part, 0.0)
    where = jnp.where(lane == 2 * group + 1, low_part, where).astype(BF16)
    slot = slots[...]

    def fill(step, carry):
        base = step * 16
        hot = (slot - base * cap == iota((16 * cap, points), 0)).astype(BF16)
        rows = mm(hot, message[...])
        left = rows[:, :128].reshape(16, cap, 128).astype(BF16)
        right = rows[:, 128:].reshape(16, cap, 128).astype(BF16)
        hot8 = (low - base * 8 == iota((128, points), 0)).astype(BF16)
        placing = mm_nt(hot8, where).reshape(16, 8, 128).astype(BF16)
        send[pl.ds(base, 16), 0:cap, :] = left
        send[pl.ds(base, 16), cap : 2 * cap, :] = right
        send[pl.ds(base, 16), 2 * cap :, :] = placing
        return carry

    lax.fori_loop(0, devices // 16, fill, 0)


def positions(tile, cell):
    x = lax.shift_right_logical(tile, 2) * 2 + lax.shift_right_logical(cell, 10)
    y = lax.bitwise_and(tile, 3) * 16 + lax.bitwise_and(lax.shift_right_logical(cell, 6), 15)
    return x, y, lax.bitwise_and(cell, 63)


def spectrum_body(message, tile, cell, table_x, table_y, table_z, out, ys, yz, xs):
    points = message.shape[0]
    x, y, z = positions(tile[...], cell[...])

    def values(table, at):
        hot = (at == iota((64, points), 0)).astype(BF16)
        both = mm(table[...], hot)
        half = both.shape[0] // 2
        return both[:half] + both[half:]

    xs[...] = values(table_x, x)
    ys[...] = values(table_y, y)
    zs = values(table_z, z)

    def some(s, carry):
        for j in range(4):
            yz[j * 8 : j * 8 + 8, :] = zs * ys[pl.ds(s * 4 + j, 1), :]
        rows = [(xs[i : i + 1, :] * yz[...]).astype(BF16) for i in range(16)]
        part = mm(jnp.concatenate(rows, axis=0), message[...])
        out[pl.ds(s * 512, 512), :] = part.astype(BF16)
        return carry

    lax.fori_loop(0, 4, some, 0)


def spectrum(message, tile, cell, table_x, table_y, table_z):
    points = message.shape[0]
    return call(
        spectrum_body,
        jax.ShapeDtypeStruct((2048, 256), BF16),
        (message, tile, cell, table_x, table_y, table_z),
        (
            pltpu.VMEM((16, points), F32),
            pltpu.VMEM((32, points), F32),
            pltpu.VMEM((16, points), F32),
        ),
        flops=2 * 2048 * 2048 * 256,
    )


def add_body(*refs):
    count = len(refs) - 4
    total = refs[0][...].astype(F32)
    for r in refs[1:count]:
        total = total + r[...].astype(F32)
    rows = total.shape[0] // 4
    for s in range(4):
        refs[count + s][...] = total[s * rows : s * rows + rows].astype(BF16)


def add_and_cut(parts):
    rows, width = parts[0].shape
    piece = jax.ShapeDtypeStruct((rows // 4, width), BF16)
    return call(add_body, (piece,) * 4, parts, ())


def join_body(*refs):
    rows = refs[0].shape[0]
    for s in range(4):
        refs[4][s * rows : s * rows + rows, :] = refs[s][...]


def joined(parts):
    rows, width = parts[0].shape
    return call(join_body, jax.ShapeDtypeStruct((rows * 4, width), BF16), parts, ())


def collect_body(recv, latent, places, rows, ids):
    picks = jnp.where(
        iota((8, 128), 1) == 2 * iota((8, 128), 0),
        64.0,
        jnp.where(iota((8, 128), 1) == 2 * iota((8, 128), 0) + 1, 1.0, 0.0),
    ).astype(BF16)

    def unpack(step, carry):
        block = recv[pl.ds(step * 16, 16)].astype(F32)
        place = block[:, 48:56, :].reshape(128, 128).astype(BF16)
        places[pl.ds(step * 128, 128), :] = place
        ids[step] = mm_nt(picks, place).astype(jnp.int32)
        for g in range(3):
            left = block[:, g * 8 : g * 8 + 8, :].reshape(128, 128)
            right = block[:, 24 + g * 8 : 32 + g * 8, :].reshape(128, 128)
            both = jnp.concatenate([left, right], axis=1).astype(BF16)
            rows[pl.ds(step * 384 + g * 128, 128), :] = both
        return carry

    lax.fori_loop(0, 8, unpack, 0)
    tile = 256

    def total(step, carry):
        at = step * tile
        cells = iota((tile, 128), 0) + at
        hot = [
            (ids[i, g : g + 1, :] == cells).astype(BF16) for i in range(8) for g in range(3)
        ]
        latent[pl.ds(at, tile), :] = mm(jnp.concatenate(hot, axis=1), rows[...]).astype(BF16)
        return carry

    lax.fori_loop(0, latent.shape[0] // tile, total, 0)


def reply_body(latent, places, weight, out, held, done):
    copy = pltpu.make_async_copy(weight, held, done)
    copy.start()
    lane = iota((128, 128), 0)
    column = iota((128, 128), 1)

    def back(step, carry):
        place = places[pl.ds(step * 128, 128), :]
        tall = []
        for g in range(3):
            pick = jnp.where(lane == 2 * g, 64.0, jnp.where(lane == 2 * g + 1, 1.0, 0.0))
            cell = mm(place, pick.astype(BF16)).astype(jnp.int32)
            hot = [(cell == column + 128 * k).astype(BF16) for k in range(16)]
            tall.append(jnp.concatenate(hot, axis=1))
        got = mm(jnp.concatenate(tall, axis=0), latent[...])
        for g in range(3):
            piece = got[g * 128 : g * 128 + 128].reshape(16, 8, 256).astype(BF16)
            out[pl.ds(step * 16, 16), g * 8 : g * 8 + 8, :] = piece
        return carry

    lax.fori_loop(0, 8, back, 0)
    copy.wait()


def mix_body(a, b, c, d, weight, out):
    spec = a[...].astype(F32) + b[...].astype(F32) + c[...].astype(F32) + d[...].astype(F32)
    spec = spec.astype(BF16)
    row = iota((8, 256), 0)
    for j in range(4):
        mixed = jnp.zeros((8, 256), F32)
        for m in range(8):
            mixed = jnp.where(row == m, mm(spec[j * 8 : j * 8 + 8], weight[j, m]), mixed)
        out[j * 8 : j * 8 + 8, :] = mixed.astype(BF16)


def own_body(returned, slots, skip, out):
    def some(step, carry):
        at = step * 256
        hot = []
        for part in range(2):
            slot = as_column(slots[:, pl.ds(at + part * 128, 128)], 128)
            one = [(slot == iota((128, 128), 1) + 128 * k).astype(BF16) for k in range(24)]
            hot.append(jnp.concatenate(one, axis=1))
        own = mm(jnp.concatenate(hot, axis=0), returned[...]).astype(BF16)
        out[pl.ds(at, 256), :] = mm(own, skip[...])
        return carry

    lax.fori_loop(0, out.shape[0] // 256, some, 0)


def waves_body(tile, cell, wide_x, wide_y, wide_z, out_x, out_yz, spots):
    x, y, z = positions(tile[...], cell[...])
    spots[0:1, :] = x
    spots[1:2, :] = y
    spots[2:3, :] = z
    lane = lax.bitwise_and(iota((128, 128), 1), 63)

    def some(step, carry):
        at = step * 128

        def values(which, table):
            col = as_column(spots[which : which + 1, pl.ds(at, 128)], 128)
            return mm((col == lane).astype(BF16), table[...])

        out_x[pl.ds(at, 128), :] = values(0, wide_x).astype(BF16)
        vy = values(1, wide_y)
        vz = values(2, wide_z)
        for h in range(2):
            for s in range(4):
                yz = vy[:, s * 128 : s * 128 + 128] * vz[:, h * 128 : h * 128 + 128]
                to = (h * 4 + s) * 128
                out_yz[pl.ds(at, 128), to : to + 128] = yz.astype(BF16)
        return carry

    lax.fori_loop(0, out_x.shape[0] // 128, some, 0)


def decode_body(
    m0, m1, m2, m3, m4, m5, m6, m7, wave_x, wave_yz, base, read, hidden_weight, output_weight, out
):
    modes = (m0, m1, m2, m3, m4, m5, m6, m7)

    def some(step, carry):
        at = step * 256
        total = base[pl.ds(at, 256), :]
        for q in range(8):
            yz = wave_yz[pl.ds(at, 256), q * 128 : q * 128 + 128]
            wave = [yz * wave_x[pl.ds(at, 256), i * 128 : i * 128 + 128] for i in range(4)]
            total = total + mm(jnp.concatenate(wave, axis=1), modes[q][...])
        value = jax.nn.gelu(total).astype(BF16).astype(F32)
        scale = jnp.concatenate(
            [as_column(read[:, pl.ds(at + 128 * part, 128)], 128) for part in range(2)], axis=0
        )
        gathered = (jnp.concatenate([scale, scale], axis=1) * value).astype(BF16)
        hidden = jax.nn.gelu(mm(gathered, hidden_weight[...])).astype(BF16)
        out[pl.ds(at, 256), :] = mm(hidden, output_weight[...]).astype(BF16)
        return carry

    lax.fori_loop(0, out.shape[0] // 256, some, 0)


def basis_table(mode, position):
    half = M // 2
    frequency = jnp.where(mode < half, mode, mode - half + 1).astype(F32)
    phase = 2.0 * math.pi * frequency * position.astype(F32) / G
    wave = jnp.where(mode < half, jnp.cos(phase), jnp.sin(phase))
    return wave * jnp.where(mode == 0, math.sqrt(1.0 / G), math.sqrt(2.0 / G))


def two_terms(table):
    high = lax.reduce_precision(table, 8, 7)
    return jnp.concatenate([high, table - high], axis=0).astype(BF16)


def around(shard, axis, s):
    return lax.ppermute(shard, axis, [(i, (i + s) % 4) for i in range(4)])


def from_others(pieces, axis):
    got = [pieces[0]]
    for s in (1, 2, 3):
        got.append(around(pieces[s], axis, s))
    return tuple(got)


def swapped(shard):
    return lax.ppermute(shard, "core", [(0, 1), (1, 0)])


def per_device(
    features,
    tile_ids,
    cell_ids,
    spread_weight,
    read_weight,
    message_weight,
    skip_weight,
    spectral_weight,
    hidden_weight,
    output_weight,
):
    points, width = features.shape
    everyone = ("z", "y", "core", "ba")
    devices = lax.axis_size(everyone)
    shape = jax.ShapeDtypeStruct
    at_z, at_y, at_core, at_b = (lax.axis_index(a) for a in everyone)
    tile = tile_ids.reshape(1, points)
    cell = cell_ids.reshape(1, points)
    grid = jnp.arange(G, dtype=jnp.int32)

    def mode_x(i, sign):
        return 4 * ((at_z + sign * (i // 4)) % 4) + (at_y + sign * (i % 4)) % 4

    def mode_y(s, j, sign):
        return 4 * ((at_b + sign * s) % 4) + j

    i16 = jnp.arange(16, dtype=jnp.int32)
    k8 = jnp.arange(8, dtype=jnp.int32)
    to_x = two_terms(basis_table(mode_x(i16, 1)[:, None], grid[None, :]))
    to_y = two_terms(basis_table(mode_y(i16 // 4, i16 % 4, 1)[:, None], grid[None, :]))
    other_z = two_terms(basis_table((8 * (1 - at_core) + k8)[:, None], grid[None, :]))
    own_z = two_terms(basis_table((8 * at_core + k8)[:, None], grid[None, :]))
    lane = jnp.arange(512, dtype=jnp.int32)
    wide_x = two_terms(basis_table(mode_x(lane // 32, -1)[None, :], grid[:, None]))
    wide_y = two_terms(
        basis_table(mode_y(lane // 128, lane // 8 % 4, -1)[None, :], grid[:, None])
    )
    lane = lane[:256]
    wide_z = two_terms(
        basis_table((8 * ((at_core + lane // 128) % 2) + lane % 8)[None, :], grid[:, None])
    )

    send, slots, message = call(
        spread_body,
        (
            shape((devices, 56, 128), BF16),
            shape((1, points), jnp.int32),
            shape((points, width), BF16),
        ),
        (features, tile, cell, spread_weight.reshape(1, points), message_weight),
        (pltpu.VMEM((1, points), jnp.int32),),
        limit=60,
    )
    recv = lax.all_to_all(send, everyone, 0, 0, tiled=True)
    away = spectrum(message, tile, cell, to_x, to_y, other_z)
    near = spectrum(message, tile, cell, to_x, to_y, own_z)
    wave_x, wave_yz = call(
        waves_body,
        (shape((points, 512), BF16), shape((points, 1024), BF16)),
        (tile, cell, wide_x, wide_y, wide_z),
        (pltpu.VMEM((8, points), jnp.int32),),
        flops=10**9,
    )
    parts = add_and_cut((near, swapped(away)))
    parts = add_and_cut(from_others(parts, "ba"))
    parts = add_and_cut(from_others(parts, "z"))
    latent, places = call(
        collect_body,
        (shape((2048, width), BF16), shape((1024, 128), BF16)),
        (recv,),
        (pltpu.VMEM((3072, width), BF16), pltpu.VMEM((8, 8, 128), jnp.int32)),
        flops=2 * 3072 * 2048 * 256,
    )
    back, weight = pl.pallas_call(
        reply_body,
        out_shape=(
            shape((devices, 24, width), BF16),
            shape(spectral_weight.shape, BF16),
        ),
        in_specs=[VMEM, VMEM, pl.BlockSpec(memory_space=pl.ANY)],
        out_specs=[VMEM, VMEM],
        scratch_shapes=[pltpu.SemaphoreType.DMA(())],
        name="reply",
        compiler_params=pltpu.CompilerParams(vmem_limit_bytes=20 * 2**20),
        cost_estimate=pl.CostEstimate(
            flops=2 * 3072 * 2048 * 256, transcendentals=0, bytes_accessed=4000000
        ),
    )(latent, places, spectral_weight)
    mixed = call(mix_body, shape((32, width), BF16), from_others(parts, "y") + (weight,), ())
    line = joined(from_others((mixed,) * 4, "y"))
    plane = joined(from_others((line,) * 4, "z"))
    modes = from_others((plane,) * 4, "ba")
    modes = modes + tuple(swapped(m) for m in modes)

    returned = lax.all_to_all(back, everyone, 0, 0, tiled=True)
    base = call(
        own_body,
        shape((points, width), F32),
        (returned.reshape(devices * 24, width), slots, skip_weight),
        (),
        flops=2 * 3072 * 2048 * 256,
    )
    return call(
        decode_body,
        shape((points, width), BF16),
        modes
        + (wave_x, wave_yz, base, read_weight.reshape(1, points), hidden_weight, output_weight),
        (),
        limit=32,
        flops=2 * 4096 * 2048 * 256,
    )


def solution(mesh):
    finer = Mesh(mesh.devices.reshape(4, 4, 2, 4), ("z", "y", "core", "ba"))
    rows = P(("z", "y", "core", "ba"))
    every = P()
    placed = (
        P(("z", "y", "core", "ba"), None),
        P(("z", "y", "core", "ba"), None),
        rows,
        rows,
        rows,
        every,
        every,
        P("ba", ("z", "y", "core"), None, None),
        every,
        every,
    )

    return jax.shard_map(
        per_device,
        mesh=finer,
        in_specs=placed,
        out_specs=P(("z", "y", "core", "ba"), None),
        check_vma=False,
    )
```

```python
import functools

import jax
import jax.numpy as jnp
import numpy as np
from jax import lax
from jax.experimental import pallas as pl
from jax.experimental.pallas import tpu as pltpu
from jax.sharding import Mesh
from jax.sharding import PartitionSpec as P

G = 64
M = 16
F32 = jnp.float32
BF16 = jnp.bfloat16
VMEM = pl.BlockSpec(memory_space=pltpu.VMEM)
SMEM = pl.BlockSpec(memory_space=pltpu.SMEM)


def iota(shape, dim):
    return lax.broadcasted_iota(jnp.int32, shape, dim)


def mm(a, b):
    return lax.dot_general(a, b, (((1,), (0,)), ((), ())), preferred_element_type=F32)


def mm_nt(a, b):
    return lax.dot_general(a, b, (((1,), (1,)), ((), ())), preferred_element_type=F32)


def as_column(row, lanes):
    n = row.shape[1]
    return jnp.transpose(jnp.broadcast_to(row, (lanes, n)))


def call(body, outs, ins, scratch=(), limit=20, flops=1000000, scalars=0):
    single = not isinstance(outs, (tuple, list))
    fn = pl.pallas_call(
        body,
        out_shape=outs,
        in_specs=[VMEM] * (len(ins) - scalars) + [SMEM] * scalars,
        out_specs=VMEM if single else [VMEM] * len(outs),
        scratch_shapes=list(scratch),
        compiler_params=pltpu.CompilerParams(vmem_limit_bytes=limit * 2**20),
        cost_estimate=pl.CostEstimate(flops=flops, transcendentals=0, bytes_accessed=4000000),
    )
    return fn(*ins)


def spread_body(feat, tile, cell, spread, weight, send, slots, message, rank_row):
    devices = send.shape[0]
    points = feat.shape[0]
    cap = 24
    upper = (iota((256, 256), 0) < iota((256, 256), 1)).astype(BF16)
    ones = jnp.ones((256, 128), BF16)
    used = jnp.zeros((devices, 256), F32)
    for at in range(0, points, 256):
        hot = tile[:, at : at + 256] == iota((devices, 256), 0)
        hot = hot.astype(F32)
        hot16 = hot.astype(BF16)
        before = mm(hot16, upper) + used
        total = mm(hot16, ones)
        used = used + jnp.concatenate([total, total], axis=1)
        rank = jnp.sum(hot * before, axis=0, keepdims=True).astype(jnp.int32)
        rank_row[:, at : at + 256] = rank
        slots[:, at : at + 256] = tile[:, at : at + 256] * cap + rank
    for at in range(0, points, 128):
        product = mm(feat[at : at + 128, :], weight[...])
        scale = as_column(spread[:, at : at + 128], 128)
        scale = jnp.concatenate([scale, scale], axis=1)
        message[at : at + 128, :] = (scale * product).astype(BF16)
    rank = rank_row[...]
    group = lax.shift_right_logical(rank, 3)
    low = tile[...] * 8 + lax.bitwise_and(rank, 7)
    high_part = lax.shift_right_logical(cell[...], 6).astype(F32)
    low_part = lax.bitwise_and(cell[...], 63).astype(F32)
    lane = iota((128, points), 0)
    where = jnp.where(lane == 2 * group, high_part, 0.0)
    where = jnp.where(lane == 2 * group + 1, low_part, where).astype(BF16)
    slot = slots[...]

    def fill(step, carry):
        base = step * 16
        hot = (slot - base * cap == iota((16 * cap, points), 0)).astype(BF16)
        rows = mm(hot, message[...])
        left = rows[:, :128].reshape(16, cap, 128).astype(BF16)
        right = rows[:, 128:].reshape(16, cap, 128).astype(BF16)
        hot8 = (low - base * 8 == iota((128, points), 0)).astype(BF16)
        placing = mm_nt(hot8, where).reshape(16, 8, 128).astype(BF16)
        send[pl.ds(base, 16), 0:cap, :] = left
        send[pl.ds(base, 16), cap : 2 * cap, :] = right
        send[pl.ds(base, 16), 2 * cap :, :] = placing
        return carry

    lax.fori_loop(0, devices // 16, fill, 0)


def positions(tile, cell):
    x = lax.shift_right_logical(tile, 2) * 2 + lax.shift_right_logical(cell, 10)
    y = lax.bitwise_and(tile, 3) * 16 + lax.bitwise_and(lax.shift_right_logical(cell, 6), 15)
    return x, y, lax.bitwise_and(cell, 63)


def device_at(where):
    d = where[0]
    return d // 32, d // 8 % 4, d // 4 % 2, d % 4


def bits(value, low, mask):
    return lax.bitwise_and(lax.shift_right_logical(value, low), mask)


def spectrum_body(message, tile, cell, basis, where, out, xy, away):
    points = message.shape[0]
    at_z, at_y, core, at_b = device_at(where)
    core = 1 - core if away else core
    r = iota((256, 16), 0)
    wide, near, last, j4 = bits(r, 6, 3), bits(r, 4, 3), bits(r, 2, 3), bits(r, 0, 3)
    shift_x = near + core * (wide - near)
    shift_y = wide + near - shift_x
    mode_x = 4 * bits(at_z + shift_x, 0, 3) + bits(at_y + last, 0, 3)
    mode_y = 4 * bits(at_b + shift_y, 0, 3) + j4
    mode_z = 8 * core + iota((8, 16), 0)
    x, y, z = positions(tile[...], cell[...])
    row = lax.bitwise_and(iota((128, points), 0), 63)

    def values(mode, at):
        pick = (mode == iota(mode.shape, 1)).astype(BF16)
        table = mm(pick, basis[...]).astype(BF16)
        return mm(table, (at == row).astype(BF16))

    xy[...] = values(mode_x, x) * values(mode_y, y)
    zs = values(mode_z, z)

    def some(s, carry):
        rows = [(xy[pl.ds(s * 64 + i, 1), :] * zs).astype(F32) for i in range(64)]
        wave = jnp.concatenate(rows, axis=0).astype(BF16)
        out[pl.ds(s * 512, 512), :] = mm(wave, message[...]).astype(BF16)
        return carry

    lax.fori_loop(0, 4, some, 0)


def spectrum(message, tile, cell, basis, where, away):
    points = message.shape[0]
    return call(
        functools.partial(spectrum_body, away=away),
        jax.ShapeDtypeStruct((2048, 256), BF16),
        (message, tile, cell, basis, where),
        (pltpu.VMEM((256, points), F32),),
        flops=2 * 2048 * 2048 * 256,
        scalars=1,
    )


def add_body(*refs):
    count = len(refs) - 4
    total = refs[0][...].astype(F32)
    for r in refs[1:count]:
        total = total + r[...].astype(F32)
    rows = total.shape[0] // 4
    for s in range(4):
        refs[count + s][...] = total[s * rows : s * rows + rows].astype(BF16)


def add_and_cut(parts):
    rows, width = parts[0].shape
    piece = jax.ShapeDtypeStruct((rows // 4, width), BF16)
    return call(add_body, (piece,) * 4, parts, ())


def join_body(*refs):
    rows = refs[0].shape[0]
    for s in range(4):
        refs[4][s * rows : s * rows + rows, :] = refs[s][...]


def joined(parts):
    rows, width = parts[0].shape
    return call(join_body, jax.ShapeDtypeStruct((rows * 4, width), BF16), parts, ())


def collect_body(recv, latent, places, rows, ids):
    picks = jnp.where(
        iota((8, 128), 1) == 2 * iota((8, 128), 0),
        64.0,
        jnp.where(iota((8, 128), 1) == 2 * iota((8, 128), 0) + 1, 1.0, 0.0),
    ).astype(BF16)

    def unpack(step, carry):
        block = recv[pl.ds(step * 16, 16)].astype(F32)
        place = block[:, 48:56, :].reshape(128, 128).astype(BF16)
        places[pl.ds(step * 128, 128), :] = place
        ids[step] = mm_nt(picks, place).astype(jnp.int32)
        for g in range(3):
            left = block[:, g * 8 : g * 8 + 8, :].reshape(128, 128)
            right = block[:, 24 + g * 8 : 32 + g * 8, :].reshape(128, 128)
            both = jnp.concatenate([left, right], axis=1).astype(BF16)
            rows[pl.ds(step * 384 + g * 128, 128), :] = both
        return carry

    lax.fori_loop(0, 8, unpack, 0)
    tile = 256

    def total(step, carry):
        at = step * tile
        cells = iota((tile, 128), 0) + at
        hot = [
            (ids[i, g : g + 1, :] == cells).astype(BF16) for i in range(8) for g in range(3)
        ]
        latent[pl.ds(at, tile), :] = mm(jnp.concatenate(hot, axis=1), rows[...]).astype(BF16)
        return carry

    lax.fori_loop(0, latent.shape[0] // tile, total, 0)


def reply_body(latent, places, weight, out, held, done):
    copy = pltpu.make_async_copy(weight, held, done)
    copy.start()
    lane = iota((128, 128), 0)
    column = iota((128, 128), 1)

    def back(step, carry):
        place = places[pl.ds(step * 128, 128), :]
        tall = []
        for g in range(3):
            pick = jnp.where(lane == 2 * g, 64.0, jnp.where(lane == 2 * g + 1, 1.0, 0.0))
            cell = mm(place, pick.astype(BF16)).astype(jnp.int32)
            hot = [(cell == column + 128 * k).astype(BF16) for k in range(16)]
            tall.append(jnp.concatenate(hot, axis=1))
        got = mm(jnp.concatenate(tall, axis=0), latent[...])
        for g in range(3):
            piece = got[g * 128 : g * 128 + 128].reshape(16, 8, 256).astype(BF16)
            out[pl.ds(step * 16, 16), g * 8 : g * 8 + 8, :] = piece
        return carry

    lax.fori_loop(0, 8, back, 0)
    copy.wait()


def mix_body(a, b, c, d, weight, out):
    spec = a[...].astype(F32) + b[...].astype(F32) + c[...].astype(F32) + d[...].astype(F32)
    spec = spec.astype(BF16)
    row = iota((8, 256), 0)
    for j in range(4):
        mixed = jnp.zeros((8, 256), F32)
        for m in range(8):
            mixed = jnp.where(row == m, mm(spec[j * 8 : j * 8 + 8], weight[j, m]), mixed)
        out[j * 8 : j * 8 + 8, :] = mixed.astype(BF16)


def own_body(returned, slots, skip, out):
    def some(step, carry):
        at = step * 256
        hot = []
        for part in range(2):
            slot = as_column(slots[:, pl.ds(at + part * 128, 128)], 128)
            one = [(slot == iota((128, 128), 1) + 128 * k).astype(BF16) for k in range(24)]
            hot.append(jnp.concatenate(one, axis=1))
        own = mm(jnp.concatenate(hot, axis=0), returned[...]).astype(BF16)
        out[pl.ds(at, 256), :] = mm(own, skip[...])
        return carry

    lax.fori_loop(0, out.shape[0] // 256, some, 0)


def waves_body(tile, cell, basis, where, out_p, out_qz, spots, wide_p, wide_q, wide_z):
    at_z, at_y, at_core, at_b = device_at(where)
    lane = iota((16, 1024), 1)
    outer, last, j4 = bits(lane, 7, 3), bits(lane, 5, 3), bits(lane, 3, 3)
    mode_x = 4 * bits(at_z - outer, 0, 3) + bits(at_y - last, 0, 3)
    mode_y = 4 * bits(at_b - outer, 0, 3) + j4
    lane = iota((16, 256), 1)
    mode_z = 8 * lax.bitwise_xor(bits(lane, 7, 1), at_core) + bits(lane, 0, 7)

    def table(mode):
        return mm(basis[...], (mode == iota(mode.shape, 0)).astype(BF16))

    straight = lax.bitwise_xor(bits(iota((128, 1024), 1), 9, 1), at_core) == 0
    factor = table(mode_x)
    wide_p[0:128, :] = jnp.where(straight, factor, 0.0).astype(BF16)
    wide_q[0:128, :] = jnp.where(straight, 0.0, factor).astype(BF16)
    factor = table(mode_y)
    wide_p[128:256, :] = jnp.where(straight, 0.0, factor).astype(BF16)
    wide_q[128:256, :] = jnp.where(straight, factor, 0.0).astype(BF16)
    wide_z[...] = table(mode_z).astype(BF16)
    x, y, z = positions(tile[...], cell[...])
    spots[0:1, :] = x
    spots[1:2, :] = y
    spots[2:3, :] = z
    lane = lax.bitwise_and(iota((128, 128), 1), 63)

    def some(step, carry):
        at = step * 128

        def hot(which):
            col = as_column(spots[which : which + 1, pl.ds(at, 128)], 128)
            return (col == lane).astype(BF16)

        xy = jnp.concatenate([hot(0), hot(1)], axis=1)
        out_p[pl.ds(at, 128), :] = mm(xy, wide_p[...]).astype(BF16)
        q = mm(xy, wide_q[...])
        vz = mm(hot(2), wide_z[...])
        for h in range(2):
            for o in range(4):
                to = (h * 4 + o) * 128
                qz = q[:, to : to + 128] * vz[:, h * 128 : h * 128 + 128]
                out_qz[pl.ds(at, 128), to : to + 128] = qz.astype(BF16)
        return carry

    lax.fori_loop(0, out_p.shape[0] // 128, some, 0)


def decode_body(
    m0, m1, m2, m3, m4, m5, m6, m7, wave_p, wave_qz, base, read, hidden_weight, output_weight, out
):
    modes = (m0, m1, m2, m3, m4, m5, m6, m7)

    def some(step, carry):
        at = step * 256
        total = base[pl.ds(at, 256), :]
        for q in range(8):
            qz = wave_qz[pl.ds(at, 256), q * 128 : q * 128 + 128]
            lane = q // 4 * 512
            wave = [
                qz * wave_p[pl.ds(at, 256), lane + i * 128 : lane + i * 128 + 128]
                for i in range(4)
            ]
            total = total + mm(jnp.concatenate(wave, axis=1), modes[q][...])
        value = jax.nn.gelu(total).astype(BF16).astype(F32)
        scale = jnp.concatenate(
            [as_column(read[:, pl.ds(at + 128 * part, 128)], 128) for part in range(2)], axis=0
        )
        gathered = (jnp.concatenate([scale, scale], axis=1) * value).astype(BF16)
        hidden = jax.nn.gelu(mm(gathered, hidden_weight[...])).astype(BF16)
        out[pl.ds(at, 256), :] = mm(hidden, output_weight[...]).astype(BF16)
        return carry

    lax.fori_loop(0, out.shape[0] // 256, some, 0, unroll=2)


def basis_terms():
    mode = np.arange(M)[:, None]
    frequency = np.where(mode < M // 2, mode, mode - M // 2 + 1)
    phase = 2.0 * np.pi * frequency * np.arange(G)[None, :] / G
    wave = np.where(mode < M // 2, np.cos(phase), np.sin(phase))
    wave = wave * np.where(mode == 0, np.sqrt(1.0 / G), np.sqrt(2.0 / G))
    high = wave.astype(np.float32).astype(jnp.bfloat16)
    low = (wave - high.astype(np.float64)).astype(np.float32).astype(jnp.bfloat16)
    return np.concatenate([high, low], axis=1)


def around(shard, stage, s):
    if stage == "y":
        return lax.ppermute(shard, "y", [(i, (i + s) % 4) for i in range(4)])
    pairs = []
    for z in range(4):
        for core in range(2):
            for b in range(4):
                along_b = (core == 0) == (stage == "wide")
                to = (z, (b + s) % 4) if along_b else ((z + s) % 4, b)
                pairs.append(((z * 2 + core) * 4 + b, (to[0] * 2 + core) * 4 + to[1]))
    return lax.ppermute(shard, ("z", "core", "ba"), pairs)


def from_others(pieces, stage):
    got = [pieces[0]]
    for s in (1, 2, 3):
        got.append(around(pieces[s], stage, s))
    return tuple(got)


def swapped(shard):
    return lax.ppermute(shard, "core", [(0, 1), (1, 0)])


def per_device(
    features,
    tile_ids,
    cell_ids,
    spread_weight,
    read_weight,
    message_weight,
    skip_weight,
    spectral_weight,
    hidden_weight,
    output_weight,
):
    points, width = features.shape
    everyone = ("z", "y", "core", "ba")
    devices = lax.axis_size(everyone)
    shape = jax.ShapeDtypeStruct
    where = lax.axis_index(everyone).astype(jnp.int32).reshape(1)
    tile = tile_ids.reshape(1, points)
    cell = cell_ids.reshape(1, points)
    terms = basis_terms()
    basis = jnp.asarray(terms)
    basis_tall = jnp.asarray(np.ascontiguousarray(terms.T))

    send, slots, message = call(
        spread_body,
        (
            shape((devices, 56, 128), BF16),
            shape((1, points), jnp.int32),
            shape((points, width), BF16),
        ),
        (features, tile, cell, spread_weight.reshape(1, points), message_weight),
        (pltpu.VMEM((1, points), jnp.int32),),
        limit=60,
    )
    recv = lax.all_to_all(send, everyone, 0, 0, tiled=True)
    away = spectrum(message, tile, cell, basis, where, True)
    near = spectrum(message, tile, cell, basis, where, False)
    wave_p, wave_qz = call(
        waves_body,
        (shape((points, 1024), BF16), shape((points, 1024), BF16)),
        (tile, cell, basis_tall, where),
        (
            pltpu.VMEM((8, points), jnp.int32),
            pltpu.VMEM((256, 1024), BF16),
            pltpu.VMEM((256, 1024), BF16),
            pltpu.VMEM((128, 256), BF16),
        ),
        flops=10**9,
        scalars=1,
    )
    parts = add_and_cut((near, swapped(away)))
    parts = add_and_cut(from_others(parts, "wide"))
    parts = add_and_cut(from_others(parts, "near"))
    latent, places = call(
        collect_body,
        (shape((2048, width), BF16), shape((1024, 128), BF16)),
        (recv,),
        (pltpu.VMEM((3072, width), BF16), pltpu.VMEM((8, 8, 128), jnp.int32)),
        flops=2 * 3072 * 2048 * 256,
    )
    back, weight = pl.pallas_call(
        reply_body,
        out_shape=(
            shape((devices, 24, width), BF16),
            shape(spectral_weight.shape, BF16),
        ),
        in_specs=[VMEM, VMEM, pl.BlockSpec(memory_space=pl.ANY)],
        out_specs=[VMEM, VMEM],
        scratch_shapes=[pltpu.SemaphoreType.DMA(())],
        name="reply",
        compiler_params=pltpu.CompilerParams(vmem_limit_bytes=20 * 2**20),
        cost_estimate=pl.CostEstimate(
            flops=2 * 3072 * 2048 * 256, transcendentals=0, bytes_accessed=4000000
        ),
    )(latent, places, spectral_weight)
    mixed = call(mix_body, shape((32, width), BF16), from_others(parts, "y") + (weight,), ())
    line = joined(from_others((mixed,) * 4, "y"))
    plane = joined(from_others((line,) * 4, "near"))
    modes = from_others((plane,) * 4, "wide")
    modes = modes + tuple(swapped(m) for m in modes)

    returned = lax.all_to_all(back, everyone, 0, 0, tiled=True)
    base = call(
        own_body,
        shape((points, width), F32),
        (returned.reshape(devices * 24, width), slots, skip_weight),
        (),
        flops=2 * 3072 * 2048 * 256,
    )
    return call(
        decode_body,
        shape((points, width), BF16),
        modes
        + (wave_p, wave_qz, base, read_weight.reshape(1, points), hidden_weight, output_weight),
        (),
        limit=32,
        flops=2 * 4096 * 2048 * 256,
    )


def solution(mesh):
    finer = Mesh(mesh.devices.reshape(4, 4, 2, 4), ("z", "y", "core", "ba"))
    rows = P(("z", "y", "core", "ba"))
    every = P()
    placed = (
        P(("z", "y", "core", "ba"), None),
        P(("z", "y", "core", "ba"), None),
        rows,
        rows,
        rows,
        every,
        every,
        P("ba", ("z", "y", "core"), None, None),
        every,
        every,
    )

    return jax.shard_map(
        per_device,
        mesh=finer,
        in_specs=placed,
        out_specs=P(("z", "y", "core", "ba"), None),
        check_vma=False,
    )
```

```python
import functools

import jax
import jax.numpy as jnp
import numpy as np
from jax import lax
from jax.experimental import pallas as pl
from jax.experimental.pallas import tpu as pltpu
from jax.sharding import Mesh
from jax.sharding import PartitionSpec as P

G = 64
M = 16
F32 = jnp.float32
BF16 = jnp.bfloat16
VMEM = pl.BlockSpec(memory_space=pltpu.VMEM)
SMEM = pl.BlockSpec(memory_space=pltpu.SMEM)


def iota(shape, dim):
    return lax.broadcasted_iota(jnp.int32, shape, dim)


def mm(a, b):
    return lax.dot_general(a, b, (((1,), (0,)), ((), ())), preferred_element_type=F32)


def mm_nt(a, b):
    return lax.dot_general(a, b, (((1,), (1,)), ((), ())), preferred_element_type=F32)


def as_column(row, lanes):
    n = row.shape[1]
    return jnp.transpose(jnp.broadcast_to(row, (lanes, n)))


def call(body, outs, ins, scratch=(), limit=20, flops=1000000, scalars=0):
    single = not isinstance(outs, (tuple, list))
    fn = pl.pallas_call(
        body,
        out_shape=outs,
        in_specs=[VMEM] * (len(ins) - scalars) + [SMEM] * scalars,
        out_specs=VMEM if single else [VMEM] * len(outs),
        scratch_shapes=list(scratch),
        compiler_params=pltpu.CompilerParams(vmem_limit_bytes=limit * 2**20),
        cost_estimate=pl.CostEstimate(flops=flops, transcendentals=0, bytes_accessed=4000000),
    )
    return fn(*ins)


def spread_body(
    feat, tile, cell, spread, weight, send, slots, message, rank_row, local, place, built, loads, saves
):
    devices = built.shape[0]
    points = local.shape[0]
    cap = 24
    load = pltpu.make_async_copy(feat, local, loads)
    load.start()
    upper = (iota((256, 256), 0) < iota((256, 256), 1)).astype(BF16)
    ones = jnp.ones((256, 128), BF16)
    used = jnp.zeros((devices, 256), F32)
    for at in range(0, points, 256):
        hot = tile[:, at : at + 256] == iota((devices, 256), 0)
        hot = hot.astype(F32)
        hot16 = hot.astype(BF16)
        before = mm(hot16, upper) + used
        total = mm(hot16, ones)
        used = used + jnp.concatenate([total, total], axis=1)
        rank = jnp.sum(hot * before, axis=0, keepdims=True).astype(jnp.int32)
        rank_row[:, at : at + 256] = rank
        slots[:, at : at + 256] = tile[:, at : at + 256] * cap + rank
    load.wait()
    lane = iota((128, 128), 1)

    def weigh(step, carry):
        at = step * 128
        product = mm(local[pl.ds(at, 128), :], weight[...])
        scale = as_column(spread[:, pl.ds(at, 128)], 128)
        scale = jnp.concatenate([scale, scale], axis=1)
        message[pl.ds(at, 128), :] = (scale * product).astype(BF16)
        group = as_column(lax.shift_right_logical(rank_row[:, pl.ds(at, 128)], 3), 128)
        where = as_column(cell[:, pl.ds(at, 128)], 128)
        high_part = lax.shift_right_logical(where, 6).astype(F32)
        low_part = lax.bitwise_and(where, 63).astype(F32)
        both = jnp.where(lane == 2 * group, high_part, 0.0)
        both = jnp.where(lane == 2 * group + 1, low_part, both)
        place[pl.ds(at, 128), :] = both.astype(BF16)
        return carry

    lax.fori_loop(0, points // 128, weigh, 0, unroll=2)
    rank = rank_row[...]
    low = tile[...] * 8 + lax.bitwise_and(rank, 7)
    slot = slots[...]

    def save(step):
        rows = pl.ds(step * 16, 16)
        return pltpu.make_async_copy(built.at[rows], send.at[rows], saves.at[step])

    def fill(step, carry):
        base = step * 16
        hot = (slot - base * cap == iota((16 * cap, points), 0)).astype(BF16)
        rows = mm(hot, message[...])
        left = rows[:, :128].reshape(16, cap, 128).astype(BF16)
        right = rows[:, 128:].reshape(16, cap, 128).astype(BF16)
        hot8 = (low - base * 8 == iota((128, points), 0)).astype(BF16)
        placing = mm(hot8, place[...]).reshape(16, 8, 128).astype(BF16)
        built[pl.ds(base, 16), 0:cap, :] = left
        built[pl.ds(base, 16), cap : 2 * cap, :] = right
        built[pl.ds(base, 16), 2 * cap :, :] = placing
        save(step).start()
        return carry

    lax.fori_loop(0, devices // 16, fill, 0)
    for step in range(devices // 16):
        save(step).wait()


def positions(tile, cell):
    x = lax.shift_right_logical(tile, 2) * 2 + lax.shift_right_logical(cell, 10)
    y = lax.bitwise_and(tile, 3) * 16 + lax.bitwise_and(lax.shift_right_logical(cell, 6), 15)
    return x, y, lax.bitwise_and(cell, 63)


def device_at(where):
    d = where[0]
    return d // 32, d // 8 % 4, d // 4 % 2, d % 4


def bits(value, low, mask):
    return lax.bitwise_and(lax.shift_right_logical(value, low), mask)


def spectrum_body(message, tile, cell, basis, where, out, xy, away):
    points = message.shape[0]
    at_z, at_y, core, at_b = device_at(where)
    core = 1 - core if away else core
    r = iota((256, 16), 0)
    wide, near, last, j4 = bits(r, 6, 3), bits(r, 4, 3), bits(r, 2, 3), bits(r, 0, 3)
    shift_x = near + core * (wide - near)
    shift_y = wide + near - shift_x
    mode_x = 4 * bits(at_z + shift_x, 0, 3) + bits(at_y + last, 0, 3)
    mode_y = 4 * bits(at_b + shift_y, 0, 3) + j4
    mode_z = 8 * core + iota((8, 16), 0)
    x, y, z = positions(tile[...], cell[...])
    row = lax.bitwise_and(iota((128, points), 0), 63)

    def values(mode, at):
        pick = (mode == iota(mode.shape, 1)).astype(BF16)
        table = mm(pick, basis[...]).astype(BF16)
        return mm(table, (at == row).astype(BF16))

    xy[...] = values(mode_x, x) * values(mode_y, y)
    zs = values(mode_z, z)

    def some(s, carry):
        rows = [(xy[pl.ds(s * 64 + i, 1), :] * zs).astype(F32) for i in range(64)]
        wave = jnp.concatenate(rows, axis=0).astype(BF16)
        out[pl.ds(s * 512, 512), :] = mm(wave, message[...]).astype(BF16)
        return carry

    lax.fori_loop(0, 4, some, 0)


def spectrum(message, tile, cell, basis, where, away):
    points = message.shape[0]
    return call(
        functools.partial(spectrum_body, away=away),
        jax.ShapeDtypeStruct((2048, 256), BF16),
        (message, tile, cell, basis, where),
        (pltpu.VMEM((256, points), F32),),
        flops=2 * 2048 * 2048 * 256,
        scalars=1,
    )


def add_body(*refs):
    count = len(refs) - 4
    total = refs[0][...].astype(F32)
    for r in refs[1:count]:
        total = total + r[...].astype(F32)
    rows = total.shape[0] // 4
    for s in range(4):
        refs[count + s][...] = total[s * rows : s * rows + rows].astype(BF16)


def add_and_cut(parts):
    rows, width = parts[0].shape
    piece = jax.ShapeDtypeStruct((rows // 4, width), BF16)
    return call(add_body, (piece,) * 4, parts, ())


def join_body(*refs):
    rows = refs[0].shape[0]
    for s in range(4):
        refs[4][s * rows : s * rows + rows, :] = refs[s][...]


def joined(parts):
    rows, width = parts[0].shape
    return call(join_body, jax.ShapeDtypeStruct((rows * 4, width), BF16), parts, ())


def collect_body(recv, latent, places, rows, ids):
    picks = jnp.where(
        iota((8, 128), 1) == 2 * iota((8, 128), 0),
        64.0,
        jnp.where(iota((8, 128), 1) == 2 * iota((8, 128), 0) + 1, 1.0, 0.0),
    ).astype(BF16)

    def unpack(step, carry):
        block = recv[pl.ds(step * 16, 16)].astype(F32)
        place = block[:, 48:56, :].reshape(128, 128).astype(BF16)
        places[pl.ds(step * 128, 128), :] = place
        ids[step] = mm_nt(picks, place).astype(jnp.int32)
        for g in range(3):
            left = block[:, g * 8 : g * 8 + 8, :].reshape(128, 128)
            right = block[:, 24 + g * 8 : 32 + g * 8, :].reshape(128, 128)
            both = jnp.concatenate([left, right], axis=1).astype(BF16)
            rows[pl.ds(step * 384 + g * 128, 128), :] = both
        return carry

    lax.fori_loop(0, 8, unpack, 0)
    tile = 512

    def total(step, carry):
        at = step * tile
        cells = iota((tile, 128), 0) + at
        hot = [
            (ids[i, g : g + 1, :] == cells).astype(BF16) for i in range(8) for g in range(3)
        ]
        latent[pl.ds(at, tile), :] = mm(jnp.concatenate(hot, axis=1), rows[...]).astype(BF16)
        return carry

    lax.fori_loop(0, latent.shape[0] // tile, total, 0)


def reply_body(latent, places, weight, out, held, done):
    copy = pltpu.make_async_copy(weight, held, done)
    copy.start()
    lane = iota((128, 128), 0)
    column = iota((128, 128), 1)

    def back(step, carry):
        place = places[pl.ds(step * 128, 128), :]
        tall = []
        for g in range(3):
            pick = jnp.where(lane == 2 * g, 64.0, jnp.where(lane == 2 * g + 1, 1.0, 0.0))
            cell = mm(place, pick.astype(BF16)).astype(jnp.int32)
            hot = [(cell == column + 128 * k).astype(BF16) for k in range(16)]
            tall.append(jnp.concatenate(hot, axis=1))
        got = mm(jnp.concatenate(tall, axis=0), latent[...])
        for g in range(3):
            piece = got[g * 128 : g * 128 + 128].reshape(16, 8, 256).astype(BF16)
            out[pl.ds(step * 16, 16), g * 8 : g * 8 + 8, :] = piece
        return carry

    lax.fori_loop(0, 8, back, 0)
    copy.wait()


def mix_body(a, b, c, d, weight, out):
    spec = a[...].astype(F32) + b[...].astype(F32) + c[...].astype(F32) + d[...].astype(F32)
    spec = spec.astype(BF16)
    row = iota((8, 256), 0)
    for j in range(4):
        mixed = jnp.zeros((8, 256), F32)
        for m in range(8):
            mixed = jnp.where(row == m, mm(spec[j * 8 : j * 8 + 8], weight[j, m]), mixed)
        out[j * 8 : j * 8 + 8, :] = mixed.astype(BF16)


def own_body(returned, slots, skip, part, out):
    def some(step, carry):
        at = step * 512
        hot = []
        for p in range(4):
            slot = as_column(slots[:, pl.ds(at + p * 128, 128)], 128)
            one = [(slot == iota((128, 128), 1) + 128 * k).astype(BF16) for k in range(24)]
            hot.append(jnp.concatenate(one, axis=1))
        own = mm(jnp.concatenate(hot, axis=0), returned[...]).astype(BF16)
        out[pl.ds(at, 512), :] = mm(own, skip[...]) + part[pl.ds(at, 512), :]
        return carry

    lax.fori_loop(0, out.shape[0] // 512, some, 0)


def waves_body(tile, cell, basis, where, out_p, out_qz, spots, wide_p, wide_q, wide_z):
    at_z, at_y, at_core, at_b = device_at(where)
    lane = iota((16, 1024), 1)
    outer, last, j4 = bits(lane, 7, 3), bits(lane, 5, 3), bits(lane, 3, 3)
    mode_x = 4 * bits(at_z - outer, 0, 3) + bits(at_y - last, 0, 3)
    mode_y = 4 * bits(at_b - outer, 0, 3) + j4
    lane = iota((16, 256), 1)
    mode_z = 8 * lax.bitwise_xor(bits(lane, 7, 1), at_core) + bits(lane, 0, 7)

    def table(mode):
        return mm(basis[...], (mode == iota(mode.shape, 0)).astype(BF16))

    straight = lax.bitwise_xor(bits(iota((128, 1024), 1), 9, 1), at_core) == 0
    factor = table(mode_x)
    wide_p[0:128, :] = jnp.where(straight, factor, 0.0).astype(BF16)
    wide_q[0:128, :] = jnp.where(straight, 0.0, factor).astype(BF16)
    factor = table(mode_y)
    wide_p[128:256, :] = jnp.where(straight, 0.0, factor).astype(BF16)
    wide_q[128:256, :] = jnp.where(straight, factor, 0.0).astype(BF16)
    wide_z[...] = table(mode_z).astype(BF16)
    x, y, z = positions(tile[...], cell[...])
    spots[0:1, :] = x
    spots[1:2, :] = y
    spots[2:3, :] = z
    lane = lax.bitwise_and(iota((128, 128), 1), 63)

    def some(step, carry):
        at = step * 128

        def hot(which):
            col = as_column(spots[which : which + 1, pl.ds(at, 128)], 128)
            return (col == lane).astype(BF16)

        xy = jnp.concatenate([hot(0), hot(1)], axis=1)
        out_p[pl.ds(at, 128), :] = mm(xy, wide_p[...]).astype(BF16)
        q = mm(xy, wide_q[...])
        vz = mm(hot(2), wide_z[...])
        for h in range(2):
            for o in range(4):
                to = (h * 4 + o) * 128
                qz = q[:, to : to + 128] * vz[:, h * 128 : h * 128 + 128]
                out_qz[pl.ds(at, 128), to : to + 128] = qz.astype(BF16)
        return carry

    lax.fori_loop(0, out_p.shape[0] // 128, some, 0)


def wave_of(wave_p, wave_qz, at, rows, h, o):
    qz = wave_qz[pl.ds(at, rows), (h * 4 + o) * 128 : (h * 4 + o) * 128 + 128]
    wave = [
        qz * wave_p[pl.ds(at, rows), h * 512 + i * 128 : h * 512 + i * 128 + 128]
        for i in range(4)
    ]
    return jnp.concatenate(wave, axis=1)


def begin_body(near, far, wave_p, wave_qz, out):
    def some(step, carry):
        at = step * 512
        total = mm(wave_of(wave_p, wave_qz, at, 512, 0, 0), near[...])
        out[pl.ds(at, 512), :] = total + mm(wave_of(wave_p, wave_qz, at, 512, 1, 0), far[...])
        return carry

    lax.fori_loop(0, out.shape[0] // 512, some, 0)


def decode_body(
    m1, m2, m3, m5, m6, m7, wave_p, wave_qz, base, read, hidden_weight, output_weight, out
):
    modes = ((m1, m2, m3), (m5, m6, m7))

    def some(step, carry):
        at = step * 512
        total = base[pl.ds(at, 512), :]
        for h in range(2):
            for o in range(3):
                wave = wave_of(wave_p, wave_qz, at, 512, h, o + 1)
                total = total + mm(wave, modes[h][o][...])
        value = jax.nn.gelu(total).astype(BF16).astype(F32)
        scale = jnp.concatenate(
            [as_column(read[:, pl.ds(at + 128 * part, 128)], 128) for part in range(4)], axis=0
        )
        gathered = (jnp.concatenate([scale, scale], axis=1) * value).astype(BF16)
        hidden = jax.nn.gelu(mm(gathered, hidden_weight[...])).astype(BF16)
        out[pl.ds(at, 512), :] = mm(hidden, output_weight[...]).astype(BF16)
        return carry

    lax.fori_loop(0, out.shape[0] // 512, some, 0)


def basis_terms():
    mode = np.arange(M)[:, None]
    frequency = np.where(mode < M // 2, mode, mode - M // 2 + 1)
    phase = 2.0 * np.pi * frequency * np.arange(G)[None, :] / G
    wave = np.where(mode < M // 2, np.cos(phase), np.sin(phase))
    wave = wave * np.where(mode == 0, np.sqrt(1.0 / G), np.sqrt(2.0 / G))
    high = wave.astype(np.float32).astype(jnp.bfloat16)
    low = (wave - high.astype(np.float64)).astype(np.float32).astype(jnp.bfloat16)
    return np.concatenate([high, low], axis=1)


def around(shard, stage, s):
    if stage == "y":
        return lax.ppermute(shard, "y", [(i, (i + s) % 4) for i in range(4)])
    pairs = []
    for z in range(4):
        for core in range(2):
            for b in range(4):
                along_b = (core == 0) == (stage == "wide")
                to = (z, (b + s) % 4) if along_b else ((z + s) % 4, b)
                pairs.append(((z * 2 + core) * 4 + b, (to[0] * 2 + core) * 4 + to[1]))
    return lax.ppermute(shard, ("z", "core", "ba"), pairs)


def from_others(pieces, stage):
    got = [pieces[0]]
    for s in (1, 2, 3):
        got.append(around(pieces[s], stage, s))
    return tuple(got)


def swapped(shard):
    return lax.ppermute(shard, "core", [(0, 1), (1, 0)])


def per_device(
    features,
    tile_ids,
    cell_ids,
    spread_weight,
    read_weight,
    message_weight,
    skip_weight,
    spectral_weight,
    hidden_weight,
    output_weight,
):
    points, width = features.shape
    everyone = ("z", "y", "core", "ba")
    devices = lax.axis_size(everyone)
    shape = jax.ShapeDtypeStruct
    where = lax.axis_index(everyone).astype(jnp.int32).reshape(1)
    tile = tile_ids.reshape(1, points)
    cell = cell_ids.reshape(1, points)
    terms = basis_terms()
    basis = jnp.asarray(terms)
    basis_tall = jnp.asarray(np.ascontiguousarray(terms.T))

    anywhere = pl.BlockSpec(memory_space=pl.ANY)
    send, slots, message = pl.pallas_call(
        spread_body,
        out_shape=(
            shape((devices, 56, 128), BF16),
            shape((1, points), jnp.int32),
            shape((points, width), BF16),
        ),
        in_specs=[anywhere, VMEM, VMEM, VMEM, VMEM],
        out_specs=[anywhere, VMEM, VMEM],
        scratch_shapes=[
            pltpu.VMEM((1, points), jnp.int32),
            pltpu.VMEM((points, width), BF16),
            pltpu.VMEM((points, 128), BF16),
            pltpu.VMEM((devices, 56, 128), BF16),
            pltpu.SemaphoreType.DMA(()),
            pltpu.SemaphoreType.DMA((devices // 16,)),
        ],
        name="spread",
        compiler_params=pltpu.CompilerParams(vmem_limit_bytes=60 * 2**20),
    )(features, tile, cell, spread_weight.reshape(1, points), message_weight)
    recv = lax.all_to_all(send, everyone, 0, 0, tiled=True)
    away = spectrum(message, tile, cell, basis, where, True)
    near = spectrum(message, tile, cell, basis, where, False)
    wave_p, wave_qz = call(
        waves_body,
        (shape((points, 1024), BF16), shape((points, 1024), BF16)),
        (tile, cell, basis_tall, where),
        (
            pltpu.VMEM((8, points), jnp.int32),
            pltpu.VMEM((256, 1024), BF16),
            pltpu.VMEM((256, 1024), BF16),
            pltpu.VMEM((128, 256), BF16),
        ),
        flops=10**9,
        scalars=1,
    )
    parts = add_and_cut((near, swapped(away)))
    parts = add_and_cut(from_others(parts, "wide"))
    parts = add_and_cut(from_others(parts, "near"))
    latent, places = call(
        collect_body,
        (shape((2048, width), BF16), shape((1024, 128), BF16)),
        (recv,),
        (pltpu.VMEM((3072, width), BF16), pltpu.VMEM((8, 8, 128), jnp.int32)),
        flops=2 * 3072 * 2048 * 256,
    )
    back, weight = pl.pallas_call(
        reply_body,
        out_shape=(
            shape((devices, 24, width), BF16),
            shape(spectral_weight.shape, BF16),
        ),
        in_specs=[VMEM, VMEM, anywhere],
        out_specs=[VMEM, VMEM],
        scratch_shapes=[pltpu.SemaphoreType.DMA(())],
        name="reply",
        compiler_params=pltpu.CompilerParams(vmem_limit_bytes=20 * 2**20),
        cost_estimate=pl.CostEstimate(
            flops=2 * 3072 * 2048 * 256, transcendentals=0, bytes_accessed=4000000
        ),
    )(latent, places, spectral_weight)
    mixed = call(mix_body, shape((32, width), BF16), from_others(parts, "y") + (weight,), ())
    line = joined(from_others((mixed,) * 4, "y"))
    plane = joined(from_others((line,) * 4, "near"))
    modes = from_others((plane,) * 4, "wide")
    modes = modes + tuple(swapped(m) for m in modes)

    returned = lax.all_to_all(back, everyone, 0, 0, tiled=True)
    part = call(
        begin_body,
        shape((points, width), F32),
        (modes[0], modes[4], wave_p, wave_qz),
        (),
        flops=2 * 1024 * 2048 * 256,
    )
    base = call(
        own_body,
        shape((points, width), F32),
        (returned.reshape(devices * 24, width), slots, skip_weight, part),
        (),
        flops=2 * 3072 * 2048 * 256,
    )
    return call(
        decode_body,
        shape((points, width), BF16),
        modes[1:4]
        + modes[5:]
        + (wave_p, wave_qz, base, read_weight.reshape(1, points), hidden_weight, output_weight),
        (),
        limit=32,
        flops=2 * 4096 * 2048 * 256,
    )


def solution(mesh):
    finer = Mesh(mesh.devices.reshape(4, 4, 2, 4), ("z", "y", "core", "ba"))
    rows = P(("z", "y", "core", "ba"))
    every = P()
    placed = (
        P(("z", "y", "core", "ba"), None),
        P(("z", "y", "core", "ba"), None),
        rows,
        rows,
        rows,
        every,
        every,
        P("ba", ("z", "y", "core"), None, None),
        every,
        every,
    )

    return jax.shard_map(
        per_device,
        mesh=finer,
        in_specs=placed,
        out_specs=P(("z", "y", "core", "ba"), None),
        check_vma=False,
    )
```

```python
import functools

import jax
import jax.numpy as jnp
import numpy as np
from jax import lax
from jax.experimental import pallas as pl
from jax.experimental.pallas import tpu as pltpu
from jax.sharding import Mesh
from jax.sharding import PartitionSpec as P

G = 64
M = 16
F32 = jnp.float32
BF16 = jnp.bfloat16
VMEM = pl.BlockSpec(memory_space=pltpu.VMEM)
SMEM = pl.BlockSpec(memory_space=pltpu.SMEM)


def iota(shape, dim):
    return lax.broadcasted_iota(jnp.int32, shape, dim)


def mm(a, b):
    return lax.dot_general(a, b, (((1,), (0,)), ((), ())), preferred_element_type=F32)


def mm_nt(a, b):
    return lax.dot_general(a, b, (((1,), (1,)), ((), ())), preferred_element_type=F32)


def as_column(row, lanes):
    n = row.shape[1]
    return jnp.transpose(jnp.broadcast_to(row, (lanes, n)))


def call(body, outs, ins, scratch=(), limit=20, flops=1000000, scalars=0):
    single = not isinstance(outs, (tuple, list))
    fn = pl.pallas_call(
        body,
        out_shape=outs,
        in_specs=[VMEM] * (len(ins) - scalars) + [SMEM] * scalars,
        out_specs=VMEM if single else [VMEM] * len(outs),
        scratch_shapes=list(scratch),
        compiler_params=pltpu.CompilerParams(vmem_limit_bytes=limit * 2**20),
        cost_estimate=pl.CostEstimate(flops=flops, transcendentals=0, bytes_accessed=4000000),
    )
    return fn(*ins)


def spread_body(
    feat, tile, cell, spread, weight, send, slots, sent, rank_row, message, place, built, saves
):
    devices = built.shape[0]
    points = message.shape[0]
    cap = 24
    upper = (iota((256, 256), 0) < iota((256, 256), 1)).astype(BF16)
    ones = jnp.ones((256, 128), BF16)
    used = jnp.zeros((devices, 256), F32)
    for at in range(0, points, 256):
        hot = tile[:, at : at + 256] == iota((devices, 256), 0)
        hot = hot.astype(F32)
        hot16 = hot.astype(BF16)
        before = mm(hot16, upper) + used
        total = mm(hot16, ones)
        used = used + jnp.concatenate([total, total], axis=1)
        rank = jnp.sum(hot * before, axis=0, keepdims=True).astype(jnp.int32)
        rank_row[:, at : at + 256] = rank
        slots[:, at : at + 256] = tile[:, at : at + 256] * cap + rank
    lane = iota((128, 128), 1)

    def weigh(step, carry):
        at = step * 128
        product = mm(feat[pl.ds(at, 128), :], weight[...])
        scale = as_column(spread[:, pl.ds(at, 128)], 128)
        scale = jnp.concatenate([scale, scale], axis=1)
        message[pl.ds(at, 128), :] = (scale * product).astype(BF16)
        group = as_column(lax.shift_right_logical(rank_row[:, pl.ds(at, 128)], 3), 128)
        where = as_column(cell[:, pl.ds(at, 128)], 128)
        high_part = lax.shift_right_logical(where, 6).astype(F32)
        low_part = lax.bitwise_and(where, 63).astype(F32)
        both = jnp.where(lane == 2 * group, high_part, 0.0)
        both = jnp.where(lane == 2 * group + 1, low_part, both)
        place[pl.ds(at, 128), :] = both.astype(BF16)
        return carry

    lax.fori_loop(0, points // 128, weigh, 0, unroll=2)
    save_message = pltpu.make_async_copy(message, sent, saves.at[devices // 16])
    save_message.start()
    rank = rank_row[...]
    low = tile[...] * 8 + lax.bitwise_and(rank, 7)
    slot = slots[...]

    def save(step):
        rows = pl.ds(step * 16, 16)
        return pltpu.make_async_copy(built.at[rows], send.at[rows], saves.at[step])

    def fill(step, carry):
        base = step * 16
        hot = (slot - base * cap == iota((16 * cap, points), 0)).astype(BF16)
        rows = mm(hot, message[...])
        left = rows[:, :128].reshape(16, cap, 128).astype(BF16)
        right = rows[:, 128:].reshape(16, cap, 128).astype(BF16)
        hot8 = (low - base * 8 == iota((128, points), 0)).astype(BF16)
        placing = mm(hot8, place[...]).reshape(16, 8, 128).astype(BF16)
        built[pl.ds(base, 16), 0:cap, :] = left
        built[pl.ds(base, 16), cap : 2 * cap, :] = right
        built[pl.ds(base, 16), 2 * cap :, :] = placing
        save(step).start()
        return carry

    lax.fori_loop(0, devices // 16, fill, 0)
    save_message.wait()
    for step in range(devices // 16):
        save(step).wait()


def positions(tile, cell):
    x = lax.shift_right_logical(tile, 2) * 2 + lax.shift_right_logical(cell, 10)
    y = lax.bitwise_and(tile, 3) * 16 + lax.bitwise_and(lax.shift_right_logical(cell, 6), 15)
    return x, y, lax.bitwise_and(cell, 63)


def device_at(where):
    d = where[0]
    return d // 32, d // 8 % 4, d // 4 % 2, d % 4


def bits(value, low, mask):
    return lax.bitwise_and(lax.shift_right_logical(value, low), mask)


def spectrum_body(message, tile, cell, basis, where, out, xy, away):
    points = message.shape[0]
    at_z, at_y, core, at_b = device_at(where)
    core = 1 - core if away else core
    r = iota((256, 16), 0)
    wide, near, last, j4 = bits(r, 6, 3), bits(r, 4, 3), bits(r, 2, 3), bits(r, 0, 3)
    shift_x = near + core * (wide - near)
    shift_y = wide + near - shift_x
    mode_x = 4 * bits(at_z + shift_x, 0, 3) + bits(at_y + last, 0, 3)
    mode_y = 4 * bits(at_b + shift_y, 0, 3) + j4
    mode_z = 8 * core + iota((8, 16), 0)
    x, y, z = positions(tile[...], cell[...])
    row = lax.bitwise_and(iota((128, points), 0), 63)

    def values(mode, at):
        pick = (mode == iota(mode.shape, 1)).astype(BF16)
        table = mm(pick, basis[...]).astype(BF16)
        return mm(table, (at == row).astype(BF16))

    xy[...] = values(mode_x, x) * values(mode_y, y)
    zs = values(mode_z, z)

    def some(s, carry):
        rows = [(xy[pl.ds(s * 64 + i, 1), :] * zs).astype(F32) for i in range(64)]
        wave = jnp.concatenate(rows, axis=0).astype(BF16)
        out[pl.ds(s * 512, 512), :] = mm(wave, message[...]).astype(BF16)
        return carry

    lax.fori_loop(0, 4, some, 0)


def spectrum(message, tile, cell, basis, where, away):
    points = message.shape[0]
    return call(
        functools.partial(spectrum_body, away=away),
        jax.ShapeDtypeStruct((2048, 256), BF16),
        (message, tile, cell, basis, where),
        (pltpu.VMEM((256, points), F32),),
        flops=2 * 2048 * 2048 * 256,
        scalars=1,
    )


def add_body(*refs):
    count = len(refs) - 4
    total = refs[0][...].astype(F32)
    for r in refs[1:count]:
        total = total + r[...].astype(F32)
    rows = total.shape[0] // 4
    for s in range(4):
        refs[count + s][...] = total[s * rows : s * rows + rows].astype(BF16)


def add_and_cut(parts):
    rows, width = parts[0].shape
    piece = jax.ShapeDtypeStruct((rows // 4, width), BF16)
    return call(add_body, (piece,) * 4, parts, ())


def join_body(*refs):
    rows = refs[0].shape[0]
    for s in range(4):
        refs[4][s * rows : s * rows + rows, :] = refs[s][...]


def joined(parts):
    rows, width = parts[0].shape
    return call(join_body, jax.ShapeDtypeStruct((rows * 4, width), BF16), parts, ())


def collect_body(recv, latent, places, rows, ids):
    picks = jnp.where(
        iota((8, 128), 1) == 2 * iota((8, 128), 0),
        64.0,
        jnp.where(iota((8, 128), 1) == 2 * iota((8, 128), 0) + 1, 1.0, 0.0),
    ).astype(BF16)

    def unpack(step, carry):
        block = recv[pl.ds(step * 16, 16)].astype(F32)
        place = block[:, 48:56, :].reshape(128, 128).astype(BF16)
        places[pl.ds(step * 128, 128), :] = place
        ids[step] = mm_nt(picks, place).astype(jnp.int32)
        for g in range(3):
            left = block[:, g * 8 : g * 8 + 8, :].reshape(128, 128)
            right = block[:, 24 + g * 8 : 32 + g * 8, :].reshape(128, 128)
            both = jnp.concatenate([left, right], axis=1).astype(BF16)
            rows[pl.ds(step * 384 + g * 128, 128), :] = both
        return carry

    lax.fori_loop(0, 8, unpack, 0)
    tile = 512

    def total(step, carry):
        at = step * tile
        cells = iota((tile, 128), 0) + at
        hot = [
            (ids[i, g : g + 1, :] == cells).astype(BF16) for i in range(8) for g in range(3)
        ]
        latent[pl.ds(at, tile), :] = mm(jnp.concatenate(hot, axis=1), rows[...]).astype(BF16)
        return carry

    lax.fori_loop(0, latent.shape[0] // tile, total, 0)


def reply_body(latent, places, weight, out, built, saves):
    lane = iota((128, 128), 0)
    column = iota((128, 128), 1)

    def back(step, carry):
        place = places[pl.ds(step * 128, 128), :]
        tall = []
        for g in range(3):
            pick = jnp.where(lane == 2 * g, 64.0, jnp.where(lane == 2 * g + 1, 1.0, 0.0))
            cell = mm(place, pick.astype(BF16)).astype(jnp.int32)
            hot = [(cell == column + 128 * k).astype(BF16) for k in range(16)]
            tall.append(jnp.concatenate(hot, axis=1))
        got = mm(jnp.concatenate(tall, axis=0), latent[...])
        for g in range(3):
            piece = got[g * 128 : g * 128 + 128].reshape(16, 8, 256).astype(BF16)
            built[pl.ds(step * 16, 16), g * 8 : g * 8 + 8, :] = piece
        save(step).start()
        return carry

    def save(step):
        rows = pl.ds(step * 16, 16)
        return pltpu.make_async_copy(built.at[rows], out.at[rows], saves.at[step])

    lax.fori_loop(0, 8, back, 0)
    for step in range(8):
        save(step).wait()


def mix_body(a, b, c, d, weight, out):
    spec = a[...].astype(F32) + b[...].astype(F32) + c[...].astype(F32) + d[...].astype(F32)
    spec = spec.astype(BF16)
    row = iota((8, 256), 0)
    for j in range(4):
        mixed = jnp.zeros((8, 256), F32)
        for m in range(8):
            mixed = jnp.where(row == m, mm(spec[j * 8 : j * 8 + 8], weight[j, m]), mixed)
        out[j * 8 : j * 8 + 8, :] = mixed.astype(BF16)


def own_body(returned, slots, skip, out):
    def some(step, carry):
        at = step * 512
        hot = []
        for p in range(4):
            slot = as_column(slots[:, pl.ds(at + p * 128, 128)], 128)
            one = [(slot == iota((128, 128), 1) + 128 * k).astype(BF16) for k in range(24)]
            hot.append(jnp.concatenate(one, axis=1))
        own = mm(jnp.concatenate(hot, axis=0), returned[...]).astype(BF16)
        out[pl.ds(at, 512), :] = mm(own, skip[...])
        return carry

    lax.fori_loop(0, out.shape[0] // 512, some, 0)


def waves_body(tile, cell, basis, where, out_p, out_qz, spots, wide_p, wide_q, wide_z):
    at_z, at_y, at_core, at_b = device_at(where)
    lane = iota((16, 1024), 1)
    outer, last, j4 = bits(lane, 7, 3), bits(lane, 5, 3), bits(lane, 3, 3)
    mode_x = 4 * bits(at_z - outer, 0, 3) + bits(at_y - last, 0, 3)
    mode_y = 4 * bits(at_b - outer, 0, 3) + j4
    lane = iota((16, 256), 1)
    mode_z = 8 * lax.bitwise_xor(bits(lane, 7, 1), at_core) + bits(lane, 0, 7)

    def table(mode):
        return mm(basis[...], (mode == iota(mode.shape, 0)).astype(BF16))

    straight = lax.bitwise_xor(bits(iota((128, 1024), 1), 9, 1), at_core) == 0
    factor = table(mode_x)
    wide_p[0:128, :] = jnp.where(straight, factor, 0.0).astype(BF16)
    wide_q[0:128, :] = jnp.where(straight, 0.0, factor).astype(BF16)
    factor = table(mode_y)
    wide_p[128:256, :] = jnp.where(straight, 0.0, factor).astype(BF16)
    wide_q[128:256, :] = jnp.where(straight, factor, 0.0).astype(BF16)
    wide_z[...] = table(mode_z).astype(BF16)
    x, y, z = positions(tile[...], cell[...])
    spots[0:1, :] = x
    spots[1:2, :] = y
    spots[2:3, :] = z
    lane = lax.bitwise_and(iota((128, 128), 1), 63)

    def some(step, carry):
        at = step * 128

        def hot(which):
            col = as_column(spots[which : which + 1, pl.ds(at, 128)], 128)
            return (col == lane).astype(BF16)

        xy = jnp.concatenate([hot(0), hot(1)], axis=1)
        out_p[pl.ds(at, 128), :] = mm(xy, wide_p[...]).astype(BF16)
        q = mm(xy, wide_q[...])
        vz = mm(hot(2), wide_z[...])
        for h in range(2):
            for o in range(4):
                to = (h * 4 + o) * 128
                qz = q[:, to : to + 128] * vz[:, h * 128 : h * 128 + 128]
                out_qz[pl.ds(at, 128), to : to + 128] = qz.astype(BF16)
        return carry

    lax.fori_loop(0, out_p.shape[0] // 128, some, 0)


def wave_of(wave_p, wave_qz, at, rows, h, o):
    qz = wave_qz[pl.ds(at, rows), (h * 4 + o) * 128 : (h * 4 + o) * 128 + 128]
    wave = [
        qz * wave_p[pl.ds(at, rows), h * 512 + i * 128 : h * 512 + i * 128 + 128]
        for i in range(4)
    ]
    return jnp.concatenate(wave, axis=1)


def begin_body(near, far, wave_p, wave_qz, base, out):
    def some(step, carry):
        at = step * 512
        total = base[pl.ds(at, 512), :]
        total = total + mm(wave_of(wave_p, wave_qz, at, 512, 0, 0), near[...])
        out[pl.ds(at, 512), :] = total + mm(wave_of(wave_p, wave_qz, at, 512, 1, 0), far[...])
        return carry

    lax.fori_loop(0, out.shape[0] // 512, some, 0)


def decode_body(
    m1, m2, m3, m5, m6, m7, wave_p, wave_qz, base, read, hidden_weight, output_weight, out
):
    modes = ((m1, m2, m3), (m5, m6, m7))

    def some(step, carry):
        at = step * 512
        total = base[pl.ds(at, 512), :]
        for h in range(2):
            for o in range(3):
                wave = wave_of(wave_p, wave_qz, at, 512, h, o + 1)
                total = total + mm(wave, modes[h][o][...])
        value = jax.nn.gelu(total).astype(BF16).astype(F32)
        scale = jnp.concatenate(
            [as_column(read[:, pl.ds(at + 128 * part, 128)], 128) for part in range(4)], axis=0
        )
        gathered = (jnp.concatenate([scale, scale], axis=1) * value).astype(BF16)
        hidden = jax.nn.gelu(mm(gathered, hidden_weight[...])).astype(BF16)
        out[pl.ds(at, 512), :] = mm(hidden, output_weight[...]).astype(BF16)
        return carry

    lax.fori_loop(0, out.shape[0] // 512, some, 0)


def basis_terms():
    mode = np.arange(M)[:, None]
    frequency = np.where(mode < M // 2, mode, mode - M // 2 + 1)
    phase = 2.0 * np.pi * frequency * np.arange(G)[None, :] / G
    wave = np.where(mode < M // 2, np.cos(phase), np.sin(phase))
    wave = wave * np.where(mode == 0, np.sqrt(1.0 / G), np.sqrt(2.0 / G))
    high = wave.astype(np.float32).astype(jnp.bfloat16)
    low = (wave - high.astype(np.float64)).astype(np.float32).astype(jnp.bfloat16)
    return np.concatenate([high, low], axis=1)


def around(shard, stage, s):
    if stage == "y":
        return lax.ppermute(shard, "y", [(i, (i + s) % 4) for i in range(4)])
    pairs = []
    for z in range(4):
        for core in range(2):
            for b in range(4):
                along_b = (core == 0) == (stage == "wide")
                to = (z, (b + s) % 4) if along_b else ((z + s) % 4, b)
                pairs.append(((z * 2 + core) * 4 + b, (to[0] * 2 + core) * 4 + to[1]))
    return lax.ppermute(shard, ("z", "core", "ba"), pairs)


def from_others(pieces, stage):
    got = [pieces[0]]
    for s in (1, 2, 3):
        got.append(around(pieces[s], stage, s))
    return tuple(got)


def swapped(shard):
    return lax.ppermute(shard, "core", [(0, 1), (1, 0)])


def per_device(
    features,
    tile_ids,
    cell_ids,
    spread_weight,
    read_weight,
    message_weight,
    skip_weight,
    spectral_weight,
    hidden_weight,
    output_weight,
):
    points, width = features.shape
    everyone = ("z", "y", "core", "ba")
    devices = lax.axis_size(everyone)
    shape = jax.ShapeDtypeStruct
    where = lax.axis_index(everyone).astype(jnp.int32).reshape(1)
    tile = tile_ids.reshape(1, points)
    cell = cell_ids.reshape(1, points)
    terms = basis_terms()
    basis = jnp.asarray(terms)
    basis_tall = jnp.asarray(np.ascontiguousarray(terms.T))

    anywhere = pl.BlockSpec(memory_space=pl.ANY)
    send, slots, message = pl.pallas_call(
        spread_body,
        out_shape=(
            shape((devices, 56, 128), BF16),
            shape((1, points), jnp.int32),
            shape((points, width), BF16),
        ),
        in_specs=[VMEM] * 5,
        out_specs=[anywhere, VMEM, anywhere],
        scratch_shapes=[
            pltpu.VMEM((1, points), jnp.int32),
            pltpu.VMEM((points, width), BF16),
            pltpu.VMEM((points, 128), BF16),
            pltpu.VMEM((devices, 56, 128), BF16),
            pltpu.SemaphoreType.DMA((devices // 16 + 1,)),
        ],
        name="spread",
        compiler_params=pltpu.CompilerParams(vmem_limit_bytes=60 * 2**20),
    )(features, tile, cell, spread_weight.reshape(1, points), message_weight)
    recv = lax.all_to_all(send, everyone, 0, 0, tiled=True)
    away = spectrum(message, tile, cell, basis, where, True)
    near = spectrum(message, tile, cell, basis, where, False)
    wave_p, wave_qz = call(
        waves_body,
        (shape((points, 1024), BF16), shape((points, 1024), BF16)),
        (tile, cell, basis_tall, where),
        (
            pltpu.VMEM((8, points), jnp.int32),
            pltpu.VMEM((256, 1024), BF16),
            pltpu.VMEM((256, 1024), BF16),
            pltpu.VMEM((128, 256), BF16),
        ),
        flops=10**9,
        scalars=1,
    )
    parts = add_and_cut((near, swapped(away)))
    parts = add_and_cut(from_others(parts, "wide"))
    parts = add_and_cut(from_others(parts, "near"))
    latent, places = call(
        collect_body,
        (shape((2048, width), BF16), shape((1024, 128), BF16)),
        (recv,),
        (pltpu.VMEM((3072, width), BF16), pltpu.VMEM((8, 8, 128), jnp.int32)),
        flops=2 * 3072 * 2048 * 256,
    )
    back = pl.pallas_call(
        reply_body,
        out_shape=shape((devices, 24, width), BF16),
        in_specs=[VMEM, VMEM, anywhere],
        out_specs=anywhere,
        scratch_shapes=[
            pltpu.VMEM((devices, 24, width), BF16),
            pltpu.SemaphoreType.DMA((8,)),
        ],
        name="reply",
        compiler_params=pltpu.CompilerParams(vmem_limit_bytes=20 * 2**20),
        cost_estimate=pl.CostEstimate(
            flops=2 * 3072 * 2048 * 256, transcendentals=0, bytes_accessed=4000000
        ),
    )(latent, places, spectral_weight)
    mixed = call(
        mix_body, shape((32, width), BF16), from_others(parts, "y") + (spectral_weight,), ()
    )
    line = joined(from_others((mixed,) * 4, "y"))
    plane = joined(from_others((line,) * 4, "near"))
    modes = from_others((plane,) * 4, "wide")
    modes = modes + tuple(swapped(m) for m in modes)

    returned = lax.all_to_all(back, everyone, 0, 0, tiled=True)
    base = call(
        own_body,
        shape((points, width), F32),
        (returned.reshape(devices * 24, width), slots, skip_weight),
        (),
        flops=2 * 3072 * 2048 * 256,
    )
    base = call(
        begin_body,
        shape((points, width), F32),
        (modes[0], modes[4], wave_p, wave_qz, base),
        (),
        flops=2 * 1024 * 2048 * 256,
    )
    return call(
        decode_body,
        shape((points, width), BF16),
        modes[1:4]
        + modes[5:]
        + (wave_p, wave_qz, base, read_weight.reshape(1, points), hidden_weight, output_weight),
        (),
        limit=32,
        flops=2 * 4096 * 2048 * 256,
    )


def solution(mesh):
    finer = Mesh(mesh.devices.reshape(4, 4, 2, 4), ("z", "y", "core", "ba"))
    rows = P(("z", "y", "core", "ba"))
    every = P()
    placed = (
        P(("z", "y", "core", "ba"), None),
        P(("z", "y", "core", "ba"), None),
        rows,
        rows,
        rows,
        every,
        every,
        P("ba", ("z", "y", "core"), None, None),
        every,
        every,
    )

    return jax.shard_map(
        per_device,
        mesh=finer,
        in_specs=placed,
        out_specs=P(("z", "y", "core", "ba"), None),
        check_vma=False,
    )
```

```python
import functools

import jax
import jax.numpy as jnp
import numpy as np
from jax import lax
from jax.experimental import pallas as pl
from jax.experimental.pallas import tpu as pltpu
from jax.sharding import Mesh
from jax.sharding import PartitionSpec as P

G = 64
M = 16
F32 = jnp.float32
BF16 = jnp.bfloat16
VMEM = pl.BlockSpec(memory_space=pltpu.VMEM)
SMEM = pl.BlockSpec(memory_space=pltpu.SMEM)


def iota(shape, dim):
    return lax.broadcasted_iota(jnp.int32, shape, dim)


def mm(a, b):
    return lax.dot_general(a, b, (((1,), (0,)), ((), ())), preferred_element_type=F32)


def mm_nt(a, b):
    return lax.dot_general(a, b, (((1,), (1,)), ((), ())), preferred_element_type=F32)


def as_column(row, lanes):
    n = row.shape[1]
    return jnp.transpose(jnp.broadcast_to(row, (lanes, n)))


def call(body, outs, ins, scratch=(), limit=20, flops=1000000, scalars=0):
    single = not isinstance(outs, (tuple, list))
    fn = pl.pallas_call(
        body,
        out_shape=outs,
        in_specs=[VMEM] * (len(ins) - scalars) + [SMEM] * scalars,
        out_specs=VMEM if single else [VMEM] * len(outs),
        scratch_shapes=list(scratch),
        compiler_params=pltpu.CompilerParams(vmem_limit_bytes=limit * 2**20),
        cost_estimate=pl.CostEstimate(flops=flops, transcendentals=0, bytes_accessed=4000000),
    )
    return fn(*ins)


def spread_body(
    feat, tile, cell, spread, weight, send, slots, sent, rank_row, message, place, built, saves
):
    devices = built.shape[0]
    points = message.shape[0]
    cap = 24
    upper = (iota((256, 256), 0) < iota((256, 256), 1)).astype(BF16)
    ones = jnp.ones((256, 128), BF16)
    used = jnp.zeros((devices, 256), F32)
    for at in range(0, points, 256):
        hot = tile[:, at : at + 256] == iota((devices, 256), 0)
        hot = hot.astype(F32)
        hot16 = hot.astype(BF16)
        before = mm(hot16, upper) + used
        total = mm(hot16, ones)
        used = used + jnp.concatenate([total, total], axis=1)
        rank = jnp.sum(hot * before, axis=0, keepdims=True).astype(jnp.int32)
        rank_row[:, at : at + 256] = rank
        slots[:, at : at + 256] = tile[:, at : at + 256] * cap + rank
    lane = iota((128, 128), 1)

    def weigh(step, carry):
        at = step * 128
        product = mm(feat[pl.ds(at, 128), :], weight[...])
        scale = as_column(spread[:, pl.ds(at, 128)], 128)
        scale = jnp.concatenate([scale, scale], axis=1)
        message[pl.ds(at, 128), :] = (scale * product).astype(BF16)
        group = as_column(lax.shift_right_logical(rank_row[:, pl.ds(at, 128)], 3), 128)
        where = as_column(cell[:, pl.ds(at, 128)], 128)
        high_part = lax.shift_right_logical(where, 6).astype(F32)
        low_part = lax.bitwise_and(where, 63).astype(F32)
        both = jnp.where(lane == 2 * group, high_part, 0.0)
        both = jnp.where(lane == 2 * group + 1, low_part, both)
        place[pl.ds(at, 128), :] = both.astype(BF16)
        return carry

    lax.fori_loop(0, points // 128, weigh, 0, unroll=2)
    save_message = pltpu.make_async_copy(message, sent, saves.at[4])
    save_message.start()
    rank = rank_row[...]
    low = tile[...] * 8 + lax.bitwise_and(rank, 7)
    slot = slots[...]

    many = 32
    steps = devices // many

    def save(step):
        rows = pl.ds(step * many, many)
        return pltpu.make_async_copy(built.at[rows], send.at[rows], saves.at[step])

    def fill(step, carry):
        base = step * many
        hot = (slot - base * cap == iota((many * cap, points), 0)).astype(BF16)
        rows = mm(hot, message[...])
        left = rows[:, :128].reshape(many, cap, 128).astype(BF16)
        right = rows[:, 128:].reshape(many, cap, 128).astype(BF16)
        hot8 = (low - base * 8 == iota((many * 8, points), 0)).astype(BF16)
        placing = mm(hot8, place[...]).reshape(many, 8, 128).astype(BF16)
        built[pl.ds(base, many), 0:cap, :] = left
        built[pl.ds(base, many), cap : 2 * cap, :] = right
        built[pl.ds(base, many), 2 * cap :, :] = placing
        save(step).start()
        return carry

    lax.fori_loop(0, steps, fill, 0)
    save_message.wait()
    for step in range(steps):
        save(step).wait()


def positions(tile, cell):
    x = lax.shift_right_logical(tile, 2) * 2 + lax.shift_right_logical(cell, 10)
    y = lax.bitwise_and(tile, 3) * 16 + lax.bitwise_and(lax.shift_right_logical(cell, 6), 15)
    return x, y, lax.bitwise_and(cell, 63)


def device_at(where):
    d = where[0]
    return d // 32, d // 8 % 4, d // 4 % 2, d % 4


def bits(value, low, mask):
    return lax.bitwise_and(lax.shift_right_logical(value, low), mask)


def spectrum_body(message, tile, cell, basis, where, out, xy, away):
    points = message.shape[0]
    at_z, at_y, core, at_b = device_at(where)
    core = 1 - core if away else core
    r = iota((256, 16), 0)
    wide, near, last, j4 = bits(r, 6, 3), bits(r, 4, 3), bits(r, 2, 3), bits(r, 0, 3)
    shift_x = near + core * (wide - near)
    shift_y = wide + near - shift_x
    mode_x = 4 * bits(at_z + shift_x, 0, 3) + bits(at_y + last, 0, 3)
    mode_y = 4 * bits(at_b + shift_y, 0, 3) + j4
    mode_z = 8 * core + iota((8, 16), 0)
    x, y, z = positions(tile[...], cell[...])
    row = lax.bitwise_and(iota((128, points), 0), 63)

    def values(mode, at):
        pick = (mode == iota(mode.shape, 1)).astype(BF16)
        table = mm(pick, basis[...]).astype(BF16)
        return mm(table, (at == row).astype(BF16))

    xy[...] = values(mode_x, x) * values(mode_y, y)
    zs = values(mode_z, z)

    def some(s, carry):
        rows = [(xy[pl.ds(s * 64 + i, 1), :] * zs).astype(F32) for i in range(64)]
        wave = jnp.concatenate(rows, axis=0).astype(BF16)
        out[pl.ds(s * 512, 512), :] = mm(wave, message[...]).astype(BF16)
        return carry

    lax.fori_loop(0, 4, some, 0)


def spectrum(message, tile, cell, basis, where, away):
    points = message.shape[0]
    return call(
        functools.partial(spectrum_body, away=away),
        jax.ShapeDtypeStruct((2048, 256), BF16),
        (message, tile, cell, basis, where),
        (pltpu.VMEM((256, points), F32),),
        flops=2 * 2048 * 2048 * 256,
        scalars=1,
    )


def add_body(*refs):
    count = len(refs) - 4
    total = refs[0][...].astype(F32)
    for r in refs[1:count]:
        total = total + r[...].astype(F32)
    rows = total.shape[0] // 4
    for s in range(4):
        refs[count + s][...] = total[s * rows : s * rows + rows].astype(BF16)


def add_and_cut(parts):
    rows, width = parts[0].shape
    piece = jax.ShapeDtypeStruct((rows // 4, width), BF16)
    return call(add_body, (piece,) * 4, parts, ())


def join_body(*refs):
    rows = refs[0].shape[0]
    for s in range(4):
        refs[4][s * rows : s * rows + rows, :] = refs[s][...]


def joined(parts):
    rows, width = parts[0].shape
    return call(join_body, jax.ShapeDtypeStruct((rows * 4, width), BF16), parts, ())


def collect_body(recv, latent, places, rows, ids):
    picks = jnp.where(
        iota((8, 128), 1) == 2 * iota((8, 128), 0),
        64.0,
        jnp.where(iota((8, 128), 1) == 2 * iota((8, 128), 0) + 1, 1.0, 0.0),
    ).astype(BF16)

    def unpack(step, carry):
        block = recv[pl.ds(step * 16, 16)].astype(F32)
        place = block[:, 48:56, :].reshape(128, 128).astype(BF16)
        places[pl.ds(step * 128, 128), :] = place
        ids[step] = mm_nt(picks, place).astype(jnp.int32)
        for g in range(3):
            left = block[:, g * 8 : g * 8 + 8, :].reshape(128, 128)
            right = block[:, 24 + g * 8 : 32 + g * 8, :].reshape(128, 128)
            both = jnp.concatenate([left, right], axis=1).astype(BF16)
            rows[pl.ds(step * 384 + g * 128, 128), :] = both
        return carry

    lax.fori_loop(0, 8, unpack, 0)
    tile = 512

    def total(step, carry):
        at = step * tile
        cells = iota((tile, 128), 0) + at
        hot = [
            (ids[i, g : g + 1, :] == cells).astype(BF16) for i in range(8) for g in range(3)
        ]
        latent[pl.ds(at, tile), :] = mm(jnp.concatenate(hot, axis=1), rows[...]).astype(BF16)
        return carry

    lax.fori_loop(0, latent.shape[0] // tile, total, 0)


def reply_body(latent, places, weight, out, built, saves):
    lane = iota((128, 128), 0)
    column = iota((256, 128), 1)

    many = 32

    def back(step, carry):
        place = places[pl.ds(step * many * 8, many * 8), :]
        tall = []
        for g in range(3):
            pick = jnp.where(lane == 2 * g, 64.0, jnp.where(lane == 2 * g + 1, 1.0, 0.0))
            cell = mm(place, pick.astype(BF16)).astype(jnp.int32)
            hot = [(cell == column + 128 * k).astype(BF16) for k in range(16)]
            tall.append(jnp.concatenate(hot, axis=1))
        got = mm(jnp.concatenate(tall, axis=0), latent[...])
        for g in range(3):
            piece = got[g * many * 8 : (g + 1) * many * 8]
            piece = piece.reshape(many, 8, 256).astype(BF16)
            built[pl.ds(step * many, many), g * 8 : g * 8 + 8, :] = piece
        save(step).start()
        return carry

    def save(step):
        rows = pl.ds(step * many, many)
        return pltpu.make_async_copy(built.at[rows], out.at[rows], saves.at[step])

    lax.fori_loop(0, 4, back, 0)
    for step in range(4):
        save(step).wait()


def mix_body(a, b, c, d, weight, out):
    spec = a[...].astype(F32) + b[...].astype(F32) + c[...].astype(F32) + d[...].astype(F32)
    spec = spec.astype(BF16)
    row = iota((8, 256), 0)
    for j in range(4):
        mixed = jnp.zeros((8, 256), F32)
        for m in range(8):
            mixed = jnp.where(row == m, mm(spec[j * 8 : j * 8 + 8], weight[j, m]), mixed)
        out[j * 8 : j * 8 + 8, :] = mixed.astype(BF16)


def own_body(returned, slots, skip, out):
    def some(step, carry):
        at = step * 512
        hot = []
        for p in range(4):
            slot = as_column(slots[:, pl.ds(at + p * 128, 128)], 128)
            one = [(slot == iota((128, 128), 1) + 128 * k).astype(BF16) for k in range(24)]
            hot.append(jnp.concatenate(one, axis=1))
        own = mm(jnp.concatenate(hot, axis=0), returned[...]).astype(BF16)
        out[pl.ds(at, 512), :] = mm(own, skip[...])
        return carry

    lax.fori_loop(0, out.shape[0] // 512, some, 0)


def waves_body(tile, cell, basis, where, out_p, out_qz, spots, wide_p, wide_q, wide_z):
    at_z, at_y, at_core, at_b = device_at(where)
    lane = iota((16, 1024), 1)
    outer, last, j4 = bits(lane, 7, 3), bits(lane, 5, 3), bits(lane, 3, 3)
    mode_x = 4 * bits(at_z - outer, 0, 3) + bits(at_y - last, 0, 3)
    mode_y = 4 * bits(at_b - outer, 0, 3) + j4
    lane = iota((16, 256), 1)
    mode_z = 8 * lax.bitwise_xor(bits(lane, 7, 1), at_core) + bits(lane, 0, 7)

    def table(mode):
        return mm(basis[...], (mode == iota(mode.shape, 0)).astype(BF16))

    straight = lax.bitwise_xor(bits(iota((128, 1024), 1), 9, 1), at_core) == 0
    factor = table(mode_x)
    wide_p[0:128, :] = jnp.where(straight, factor, 0.0).astype(BF16)
    wide_q[0:128, :] = jnp.where(straight, 0.0, factor).astype(BF16)
    factor = table(mode_y)
    wide_p[128:256, :] = jnp.where(straight, 0.0, factor).astype(BF16)
    wide_q[128:256, :] = jnp.where(straight, factor, 0.0).astype(BF16)
    wide_z[...] = table(mode_z).astype(BF16)
    x, y, z = positions(tile[...], cell[...])
    spots[0:1, :] = x
    spots[1:2, :] = y
    spots[2:3, :] = z
    lane = lax.bitwise_and(iota((128, 128), 1), 63)

    def some(step, carry):
        at = step * 128

        def hot(which):
            col = as_column(spots[which : which + 1, pl.ds(at, 128)], 128)
            return (col == lane).astype(BF16)

        xy = jnp.concatenate([hot(0), hot(1)], axis=1)
        out_p[pl.ds(at, 128), :] = mm(xy, wide_p[...]).astype(BF16)
        q = mm(xy, wide_q[...])
        vz = mm(hot(2), wide_z[...])
        for h in range(2):
            for o in range(4):
                to = (h * 4 + o) * 128
                qz = q[:, to : to + 128] * vz[:, h * 128 : h * 128 + 128]
                out_qz[pl.ds(at, 128), to : to + 128] = qz.astype(BF16)
        return carry

    lax.fori_loop(0, out_p.shape[0] // 128, some, 0)


def wave_of(wave_p, wave_qz, at, rows, h, o):
    qz = wave_qz[pl.ds(at, rows), (h * 4 + o) * 128 : (h * 4 + o) * 128 + 128]
    wave = [
        qz * wave_p[pl.ds(at, rows), h * 512 + i * 128 : h * 512 + i * 128 + 128]
        for i in range(4)
    ]
    return jnp.concatenate(wave, axis=1)


def begin_body(near, far, wave_p, wave_qz, base, out):
    def some(step, carry):
        at = step * 512
        total = base[pl.ds(at, 512), :]
        total = total + mm(wave_of(wave_p, wave_qz, at, 512, 0, 0), near[...])
        out[pl.ds(at, 512), :] = total + mm(wave_of(wave_p, wave_qz, at, 512, 1, 0), far[...])
        return carry

    lax.fori_loop(0, out.shape[0] // 512, some, 0)


def decode_body(
    m1, m2, m3, m5, m6, m7, wave_p, wave_qz, base, read, hidden_weight, output_weight, out, built, saves
):
    modes = ((m1, m2, m3), (m5, m6, m7))

    def some(step, carry):
        at = step * 512
        total = base[pl.ds(at, 512), :]
        for h in range(2):
            for o in range(3):
                wave = wave_of(wave_p, wave_qz, at, 512, h, o + 1)
                total = total + mm(wave, modes[h][o][...])
        value = jax.nn.gelu(total).astype(BF16).astype(F32)
        scale = jnp.concatenate(
            [as_column(read[:, pl.ds(at + 128 * part, 128)], 128) for part in range(4)], axis=0
        )
        gathered = (jnp.concatenate([scale, scale], axis=1) * value).astype(BF16)
        hidden = jax.nn.gelu(mm(gathered, hidden_weight[...])).astype(BF16)
        built[pl.ds(at, 512), :] = mm(hidden, output_weight[...]).astype(BF16)
        save(step).start()
        return carry

    def save(step):
        rows = pl.ds(step * 512, 512)
        return pltpu.make_async_copy(built.at[rows], out.at[rows], saves.at[step])

    lax.fori_loop(0, 4, some, 0)
    for step in range(4):
        save(step).wait()


def basis_terms():
    mode = np.arange(M)[:, None]
    frequency = np.where(mode < M // 2, mode, mode - M // 2 + 1)
    phase = 2.0 * np.pi * frequency * np.arange(G)[None, :] / G
    wave = np.where(mode < M // 2, np.cos(phase), np.sin(phase))
    wave = wave * np.where(mode == 0, np.sqrt(1.0 / G), np.sqrt(2.0 / G))
    high = wave.astype(np.float32).astype(jnp.bfloat16)
    low = (wave - high.astype(np.float64)).astype(np.float32).astype(jnp.bfloat16)
    return np.concatenate([high, low], axis=1)


def around(shard, stage, s):
    if stage == "y":
        return lax.ppermute(shard, "y", [(i, (i + s) % 4) for i in range(4)])
    pairs = []
    for z in range(4):
        for core in range(2):
            for b in range(4):
                along_b = (core == 0) == (stage == "wide")
                to = (z, (b + s) % 4) if along_b else ((z + s) % 4, b)
                pairs.append(((z * 2 + core) * 4 + b, (to[0] * 2 + core) * 4 + to[1]))
    return lax.ppermute(shard, ("z", "core", "ba"), pairs)


def from_others(pieces, stage):
    got = [pieces[0]]
    for s in (1, 2, 3):
        got.append(around(pieces[s], stage, s))
    return tuple(got)


def swapped(shard):
    return lax.ppermute(shard, "core", [(0, 1), (1, 0)])


def per_device(
    features,
    tile_ids,
    cell_ids,
    spread_weight,
    read_weight,
    message_weight,
    skip_weight,
    spectral_weight,
    hidden_weight,
    output_weight,
):
    points, width = features.shape
    everyone = ("z", "y", "core", "ba")
    devices = lax.axis_size(everyone)
    shape = jax.ShapeDtypeStruct
    where = lax.axis_index(everyone).astype(jnp.int32).reshape(1)
    tile = tile_ids.reshape(1, points)
    cell = cell_ids.reshape(1, points)
    terms = basis_terms()
    basis = jnp.asarray(terms)
    basis_tall = jnp.asarray(np.ascontiguousarray(terms.T))

    anywhere = pl.BlockSpec(memory_space=pl.ANY)
    send, slots, message = pl.pallas_call(
        spread_body,
        out_shape=(
            shape((devices, 56, 128), BF16),
            shape((1, points), jnp.int32),
            shape((points, width), BF16),
        ),
        in_specs=[VMEM] * 5,
        out_specs=[anywhere, VMEM, anywhere],
        scratch_shapes=[
            pltpu.VMEM((1, points), jnp.int32),
            pltpu.VMEM((points, width), BF16),
            pltpu.VMEM((points, 128), BF16),
            pltpu.VMEM((devices, 56, 128), BF16),
            pltpu.SemaphoreType.DMA((5,)),
        ],
        name="spread",
        compiler_params=pltpu.CompilerParams(vmem_limit_bytes=60 * 2**20),
    )(features, tile, cell, spread_weight.reshape(1, points), message_weight)
    recv = lax.all_to_all(send, everyone, 0, 0, tiled=True)
    away = spectrum(message, tile, cell, basis, where, True)
    near = spectrum(message, tile, cell, basis, where, False)
    wave_p, wave_qz = call(
        waves_body,
        (shape((points, 1024), BF16), shape((points, 1024), BF16)),
        (tile, cell, basis_tall, where),
        (
            pltpu.VMEM((8, points), jnp.int32),
            pltpu.VMEM((256, 1024), BF16),
            pltpu.VMEM((256, 1024), BF16),
            pltpu.VMEM((128, 256), BF16),
        ),
        flops=10**9,
        scalars=1,
    )
    parts = add_and_cut((near, swapped(away)))
    parts = add_and_cut(from_others(parts, "wide"))
    parts = add_and_cut(from_others(parts, "near"))
    latent, places = call(
        collect_body,
        (shape((2048, width), BF16), shape((1024, 128), BF16)),
        (recv,),
        (pltpu.VMEM((3072, width), BF16), pltpu.VMEM((8, 8, 128), jnp.int32)),
        flops=2 * 3072 * 2048 * 256,
    )
    back = pl.pallas_call(
        reply_body,
        out_shape=shape((devices, 24, width), BF16),
        in_specs=[VMEM, VMEM, anywhere],
        out_specs=anywhere,
        scratch_shapes=[
            pltpu.VMEM((devices, 24, width), BF16),
            pltpu.SemaphoreType.DMA((4,)),
        ],
        name="reply",
        compiler_params=pltpu.CompilerParams(vmem_limit_bytes=20 * 2**20),
        cost_estimate=pl.CostEstimate(
            flops=2 * 3072 * 2048 * 256, transcendentals=0, bytes_accessed=4000000
        ),
    )(latent, places, spectral_weight)
    mixed = call(
        mix_body, shape((32, width), BF16), from_others(parts, "y") + (spectral_weight,), ()
    )
    line = joined(from_others((mixed,) * 4, "y"))
    plane = joined(from_others((line,) * 4, "near"))
    modes = from_others((plane,) * 4, "wide")
    modes = modes + tuple(swapped(m) for m in modes)

    returned = lax.all_to_all(back, everyone, 0, 0, tiled=True)
    base = call(
        own_body,
        shape((points, width), F32),
        (returned.reshape(devices * 24, width), slots, skip_weight),
        (),
        flops=2 * 3072 * 2048 * 256,
    )
    base = call(
        begin_body,
        shape((points, width), F32),
        (modes[0], modes[4], wave_p, wave_qz, base),
        (),
        flops=2 * 1024 * 2048 * 256,
    )
    arrays = modes[1:4] + modes[5:]
    arrays = arrays + (wave_p, wave_qz, base, read_weight.reshape(1, points))
    arrays = arrays + (hidden_weight, output_weight)
    return pl.pallas_call(
        decode_body,
        out_shape=shape((points, width), BF16),
        in_specs=[VMEM] * len(arrays),
        out_specs=anywhere,
        scratch_shapes=[pltpu.VMEM((points, width), BF16), pltpu.SemaphoreType.DMA((4,))],
        name="decode",
        compiler_params=pltpu.CompilerParams(vmem_limit_bytes=32 * 2**20),
        cost_estimate=pl.CostEstimate(
            flops=2 * 4096 * 2048 * 256, transcendentals=0, bytes_accessed=4000000
        ),
    )(*arrays)


def solution(mesh):
    finer = Mesh(mesh.devices.reshape(4, 4, 2, 4), ("z", "y", "core", "ba"))
    rows = P(("z", "y", "core", "ba"))
    every = P()
    placed = (
        P(("z", "y", "core", "ba"), None),
        P(("z", "y", "core", "ba"), None),
        rows,
        rows,
        rows,
        every,
        every,
        P("ba", ("z", "y", "core"), None, None),
        every,
        every,
    )

    return jax.shard_map(
        per_device,
        mesh=finer,
        in_specs=placed,
        out_specs=P(("z", "y", "core", "ba"), None),
        check_vma=False,
    )
```

```python
import functools

import jax
import jax.numpy as jnp
import numpy as np
from jax import lax
from jax.experimental import pallas as pl
from jax.experimental.pallas import tpu as pltpu
from jax.sharding import Mesh
from jax.sharding import PartitionSpec as P

G = 64
M = 16
F32 = jnp.float32
BF16 = jnp.bfloat16
VMEM = pl.BlockSpec(memory_space=pltpu.VMEM)
SMEM = pl.BlockSpec(memory_space=pltpu.SMEM)


def iota(shape, dim):
    return lax.broadcasted_iota(jnp.int32, shape, dim)


def mm(a, b):
    return lax.dot_general(a, b, (((1,), (0,)), ((), ())), preferred_element_type=F32)


def mm_nt(a, b):
    return lax.dot_general(a, b, (((1,), (1,)), ((), ())), preferred_element_type=F32)


def as_column(row, lanes):
    n = row.shape[1]
    return jnp.transpose(jnp.broadcast_to(row, (lanes, n)))


def call(body, outs, ins, scratch=(), limit=20, flops=1000000, scalars=0):
    single = not isinstance(outs, (tuple, list))
    fn = pl.pallas_call(
        body,
        out_shape=outs,
        in_specs=[VMEM] * (len(ins) - scalars) + [SMEM] * scalars,
        out_specs=VMEM if single else [VMEM] * len(outs),
        scratch_shapes=list(scratch),
        compiler_params=pltpu.CompilerParams(vmem_limit_bytes=limit * 2**20),
        cost_estimate=pl.CostEstimate(flops=flops, transcendentals=0, bytes_accessed=4000000),
    )
    return fn(*ins)


def spread_body(
    tile,
    far_feat,
    far_cell,
    far_spread,
    far_weight,
    send,
    slots,
    sent,
    rank_row,
    message,
    place,
    built,
    feat,
    cell,
    spread,
    weight,
    saves,
    loads,
):
    pairs = ((far_feat, feat), (far_weight, weight), (far_spread, spread), (far_cell, cell))
    copies = [pltpu.make_async_copy(a, b, loads.at[i]) for i, (a, b) in enumerate(pairs)]
    for copy in copies:
        copy.start()
    devices = built.shape[0]
    points = message.shape[0]
    cap = 24
    upper = (iota((256, 256), 0) < iota((256, 256), 1)).astype(BF16)
    ones = jnp.ones((256, 128), BF16)
    used = jnp.zeros((devices, 256), F32)
    for at in range(0, points, 256):
        hot = tile[:, at : at + 256] == iota((devices, 256), 0)
        hot = hot.astype(F32)
        hot16 = hot.astype(BF16)
        before = mm(hot16, upper) + used
        total = mm(hot16, ones)
        used = used + jnp.concatenate([total, total], axis=1)
        rank = jnp.sum(hot * before, axis=0, keepdims=True).astype(jnp.int32)
        rank_row[:, at : at + 256] = rank
        slots[:, at : at + 256] = tile[:, at : at + 256] * cap + rank
    for copy in copies:
        copy.wait()
    lane = iota((128, 128), 1)

    def weigh(step, carry):
        at = step * 128
        product = mm(feat[pl.ds(at, 128), :], weight[...])
        scale = as_column(spread[:, pl.ds(at, 128)], 128)
        scale = jnp.concatenate([scale, scale], axis=1)
        message[pl.ds(at, 128), :] = (scale * product).astype(BF16)
        group = as_column(lax.shift_right_logical(rank_row[:, pl.ds(at, 128)], 3), 128)
        where = as_column(cell[:, pl.ds(at, 128)], 128)
        high_part = lax.shift_right_logical(where, 6).astype(F32)
        low_part = lax.bitwise_and(where, 63).astype(F32)
        both = jnp.where(lane == 2 * group, high_part, 0.0)
        both = jnp.where(lane == 2 * group + 1, low_part, both)
        place[pl.ds(at, 128), :] = both.astype(BF16)
        return carry

    lax.fori_loop(0, points // 128, weigh, 0, unroll=2)
    save_message = pltpu.make_async_copy(message, sent, saves.at[4])
    save_message.start()
    rank = rank_row[...]
    low = tile[...] * 8 + lax.bitwise_and(rank, 7)
    slot = slots[...]

    many = 32
    steps = devices // many

    def save(step):
        rows = pl.ds(step * many, many)
        return pltpu.make_async_copy(built.at[rows], send.at[rows], saves.at[step])

    def fill(step, carry):
        base = step * many
        hot = (slot - base * cap == iota((many * cap, points), 0)).astype(BF16)
        rows = mm(hot, message[...])
        left = rows[:, :128].reshape(many, cap, 128).astype(BF16)
        right = rows[:, 128:].reshape(many, cap, 128).astype(BF16)
        hot8 = (low - base * 8 == iota((many * 8, points), 0)).astype(BF16)
        placing = mm(hot8, place[...]).reshape(many, 8, 128).astype(BF16)
        built[pl.ds(base, many), 0:cap, :] = left
        built[pl.ds(base, many), cap : 2 * cap, :] = right
        built[pl.ds(base, many), 2 * cap :, :] = placing
        save(step).start()
        return carry

    lax.fori_loop(0, steps, fill, 0)
    save_message.wait()
    for step in range(steps):
        save(step).wait()


def positions(tile, cell):
    x = lax.shift_right_logical(tile, 2) * 2 + lax.shift_right_logical(cell, 10)
    y = lax.bitwise_and(tile, 3) * 16 + lax.bitwise_and(lax.shift_right_logical(cell, 6), 15)
    return x, y, lax.bitwise_and(cell, 63)


def device_at(where):
    d = where[0]
    return d // 32, d // 8 % 4, d // 4 % 2, d % 4


def bits(value, low, mask):
    return lax.bitwise_and(lax.shift_right_logical(value, low), mask)


def spectrum_body(message, tile, cell, basis, where, out, xy, away):
    points = message.shape[0]
    at_z, at_y, core, at_b = device_at(where)
    core = 1 - core if away else core
    r = iota((256, 16), 0)
    wide, near, last, j4 = bits(r, 6, 3), bits(r, 4, 3), bits(r, 2, 3), bits(r, 0, 3)
    shift_x = near + core * (wide - near)
    shift_y = wide + near - shift_x
    mode_x = 4 * bits(at_z + shift_x, 0, 3) + bits(at_y + last, 0, 3)
    mode_y = 4 * bits(at_b + shift_y, 0, 3) + j4
    mode_z = 8 * core + iota((8, 16), 0)
    x, y, z = positions(tile[...], cell[...])
    row = lax.bitwise_and(iota((128, points), 0), 63)

    def values(mode, at):
        pick = (mode == iota(mode.shape, 1)).astype(BF16)
        table = mm(pick, basis[...]).astype(BF16)
        return mm(table, (at == row).astype(BF16))

    xy[...] = values(mode_x, x) * values(mode_y, y)
    zs = values(mode_z, z)

    def some(s, carry):
        rows = [(xy[pl.ds(s * 64 + i, 1), :] * zs).astype(F32) for i in range(64)]
        wave = jnp.concatenate(rows, axis=0).astype(BF16)
        out[pl.ds(s * 512, 512), :] = mm(wave, message[...]).astype(BF16)
        return carry

    lax.fori_loop(0, 4, some, 0)


def spectrum(message, tile, cell, basis, where, away):
    points = message.shape[0]
    return call(
        functools.partial(spectrum_body, away=away),
        jax.ShapeDtypeStruct((2048, 256), BF16),
        (message, tile, cell, basis, where),
        (pltpu.VMEM((256, points), F32),),
        flops=2 * 2048 * 2048 * 256,
        scalars=1,
    )


def add_body(*refs):
    count = len(refs) - 4
    total = refs[0][...].astype(F32)
    for r in refs[1:count]:
        total = total + r[...].astype(F32)
    rows = total.shape[0] // 4
    for s in range(4):
        refs[count + s][...] = total[s * rows : s * rows + rows].astype(BF16)


def add_and_cut(parts):
    rows, width = parts[0].shape
    piece = jax.ShapeDtypeStruct((rows // 4, width), BF16)
    return call(add_body, (piece,) * 4, parts, ())


def join_body(*refs):
    rows = refs[0].shape[0]
    for s in range(4):
        refs[4][s * rows : s * rows + rows, :] = refs[s][...]


def joined(parts):
    rows, width = parts[0].shape
    return call(join_body, jax.ShapeDtypeStruct((rows * 4, width), BF16), parts, ())


def collect_body(recv, latent, places, rows, ids):
    picks = jnp.where(
        iota((8, 128), 1) == 2 * iota((8, 128), 0),
        64.0,
        jnp.where(iota((8, 128), 1) == 2 * iota((8, 128), 0) + 1, 1.0, 0.0),
    ).astype(BF16)

    def unpack(step, carry):
        block = recv[pl.ds(step * 16, 16)].astype(F32)
        place = block[:, 48:56, :].reshape(128, 128).astype(BF16)
        places[pl.ds(step * 128, 128), :] = place
        ids[step] = mm_nt(picks, place).astype(jnp.int32)
        for g in range(3):
            left = block[:, g * 8 : g * 8 + 8, :].reshape(128, 128)
            right = block[:, 24 + g * 8 : 32 + g * 8, :].reshape(128, 128)
            both = jnp.concatenate([left, right], axis=1).astype(BF16)
            rows[pl.ds(step * 384 + g * 128, 128), :] = both
        return carry

    lax.fori_loop(0, 8, unpack, 0)
    tile = 512

    def total(step, carry):
        at = step * tile
        cells = iota((tile, 128), 0) + at
        hot = [
            (ids[i, g : g + 1, :] == cells).astype(BF16) for i in range(8) for g in range(3)
        ]
        latent[pl.ds(at, tile), :] = mm(jnp.concatenate(hot, axis=1), rows[...]).astype(BF16)
        return carry

    lax.fori_loop(0, latent.shape[0] // tile, total, 0)


def reply_body(latent, places, weight, out, built, saves):
    lane = iota((128, 128), 0)
    column = iota((256, 128), 1)

    many = 32

    def back(step, carry):
        place = places[pl.ds(step * many * 8, many * 8), :]
        tall = []
        for g in range(3):
            pick = jnp.where(lane == 2 * g, 64.0, jnp.where(lane == 2 * g + 1, 1.0, 0.0))
            cell = mm(place, pick.astype(BF16)).astype(jnp.int32)
            hot = [(cell == column + 128 * k).astype(BF16) for k in range(16)]
            tall.append(jnp.concatenate(hot, axis=1))
        got = mm(jnp.concatenate(tall, axis=0), latent[...])
        for g in range(3):
            piece = got[g * many * 8 : (g + 1) * many * 8]
            piece = piece.reshape(many, 8, 256).astype(BF16)
            built[pl.ds(step * many, many), g * 8 : g * 8 + 8, :] = piece
        save(step).start()
        return carry

    def save(step):
        rows = pl.ds(step * many, many)
        return pltpu.make_async_copy(built.at[rows], out.at[rows], saves.at[step])

    lax.fori_loop(0, 4, back, 0)
    for step in range(4):
        save(step).wait()


def mix_body(a, b, c, d, weight, out):
    spec = a[...].astype(F32) + b[...].astype(F32) + c[...].astype(F32) + d[...].astype(F32)
    spec = spec.astype(BF16)
    row = iota((8, 256), 0)
    for j in range(4):
        mixed = jnp.zeros((8, 256), F32)
        for m in range(8):
            mixed = jnp.where(row == m, mm(spec[j * 8 : j * 8 + 8], weight[j, m]), mixed)
        out[j * 8 : j * 8 + 8, :] = mixed.astype(BF16)


def own_body(returned, slots, skip, out):
    def some(step, carry):
        at = step * 512
        hot = []
        for p in range(4):
            slot = as_column(slots[:, pl.ds(at + p * 128, 128)], 128)
            one = [(slot == iota((128, 128), 1) + 128 * k).astype(BF16) for k in range(24)]
            hot.append(jnp.concatenate(one, axis=1))
        own = mm(jnp.concatenate(hot, axis=0), returned[...]).astype(BF16)
        out[pl.ds(at, 512), :] = mm(own, skip[...])
        return carry

    lax.fori_loop(0, out.shape[0] // 512, some, 0)


def waves_body(tile, cell, basis, where, out_p, out_qz, spots, wide_p, wide_q, wide_z):
    at_z, at_y, at_core, at_b = device_at(where)
    lane = iota((16, 1024), 1)
    outer, last, j4 = bits(lane, 7, 3), bits(lane, 5, 3), bits(lane, 3, 3)
    mode_x = 4 * bits(at_z - outer, 0, 3) + bits(at_y - last, 0, 3)
    mode_y = 4 * bits(at_b - outer, 0, 3) + j4
    lane = iota((16, 256), 1)
    mode_z = 8 * lax.bitwise_xor(bits(lane, 7, 1), at_core) + bits(lane, 0, 7)

    def table(mode):
        return mm(basis[...], (mode == iota(mode.shape, 0)).astype(BF16))

    straight = lax.bitwise_xor(bits(iota((128, 1024), 1), 9, 1), at_core) == 0
    factor = table(mode_x)
    wide_p[0:128, :] = jnp.where(straight, factor, 0.0).astype(BF16)
    wide_q[0:128, :] = jnp.where(straight, 0.0, factor).astype(BF16)
    factor = table(mode_y)
    wide_p[128:256, :] = jnp.where(straight, 0.0, factor).astype(BF16)
    wide_q[128:256, :] = jnp.where(straight, factor, 0.0).astype(BF16)
    wide_z[...] = table(mode_z).astype(BF16)
    x, y, z = positions(tile[...], cell[...])
    spots[0:1, :] = x
    spots[1:2, :] = y
    spots[2:3, :] = z
    lane = lax.bitwise_and(iota((128, 128), 1), 63)

    def some(step, carry):
        at = step * 128

        def hot(which):
            col = as_column(spots[which : which + 1, pl.ds(at, 128)], 128)
            return (col == lane).astype(BF16)

        xy = jnp.concatenate([hot(0), hot(1)], axis=1)
        out_p[pl.ds(at, 128), :] = mm(xy, wide_p[...]).astype(BF16)
        q = mm(xy, wide_q[...])
        vz = mm(hot(2), wide_z[...])
        for h in range(2):
            for o in range(4):
                to = (h * 4 + o) * 128
                qz = q[:, to : to + 128] * vz[:, h * 128 : h * 128 + 128]
                out_qz[pl.ds(at, 128), to : to + 128] = qz.astype(BF16)
        return carry

    lax.fori_loop(0, out_p.shape[0] // 128, some, 0)


def wave_of(wave_p, wave_qz, at, rows, h, o):
    qz = wave_qz[pl.ds(at, rows), (h * 4 + o) * 128 : (h * 4 + o) * 128 + 128]
    wave = [
        qz * wave_p[pl.ds(at, rows), h * 512 + i * 128 : h * 512 + i * 128 + 128]
        for i in range(4)
    ]
    return jnp.concatenate(wave, axis=1)


def begin_body(near, far, wave_p, wave_qz, base, out):
    def some(step, carry):
        at = step * 512
        total = base[pl.ds(at, 512), :]
        total = total + mm(wave_of(wave_p, wave_qz, at, 512, 0, 0), near[...])
        out[pl.ds(at, 512), :] = total + mm(wave_of(wave_p, wave_qz, at, 512, 1, 0), far[...])
        return carry

    lax.fori_loop(0, out.shape[0] // 512, some, 0)


def decode_body(
    m1, m2, m3, m5, m6, m7, wave_p, wave_qz, base, read, hidden_weight, output_weight, out, built, saves
):
    modes = ((m1, m2, m3), (m5, m6, m7))

    def some(step, carry):
        at = step * 512
        total = base[pl.ds(at, 512), :]
        for h in range(2):
            for o in range(3):
                wave = wave_of(wave_p, wave_qz, at, 512, h, o + 1)
                total = total + mm(wave, modes[h][o][...])
        value = jax.nn.gelu(total).astype(BF16).astype(F32)
        scale = jnp.concatenate(
            [as_column(read[:, pl.ds(at + 128 * part, 128)], 128) for part in range(4)], axis=0
        )
        gathered = (jnp.concatenate([scale, scale], axis=1) * value).astype(BF16)
        hidden = jax.nn.gelu(mm(gathered, hidden_weight[...])).astype(BF16)
        built[pl.ds(at, 512), :] = mm(hidden, output_weight[...]).astype(BF16)
        save(step).start()
        return carry

    def save(step):
        rows = pl.ds(step * 512, 512)
        return pltpu.make_async_copy(built.at[rows], out.at[rows], saves.at[step])

    lax.fori_loop(0, 4, some, 0)
    for step in range(4):
        save(step).wait()


def basis_terms():
    mode = np.arange(M)[:, None]
    frequency = np.where(mode < M // 2, mode, mode - M // 2 + 1)
    phase = 2.0 * np.pi * frequency * np.arange(G)[None, :] / G
    wave = np.where(mode < M // 2, np.cos(phase), np.sin(phase))
    wave = wave * np.where(mode == 0, np.sqrt(1.0 / G), np.sqrt(2.0 / G))
    high = wave.astype(np.float32).astype(jnp.bfloat16)
    low = (wave - high.astype(np.float64)).astype(np.float32).astype(jnp.bfloat16)
    return np.concatenate([high, low], axis=1)


def around(shard, stage, s):
    if stage == "y":
        return lax.ppermute(shard, "y", [(i, (i + s) % 4) for i in range(4)])
    pairs = []
    for z in range(4):
        for core in range(2):
            for b in range(4):
                along_b = (core == 0) == (stage == "wide")
                to = (z, (b + s) % 4) if along_b else ((z + s) % 4, b)
                pairs.append(((z * 2 + core) * 4 + b, (to[0] * 2 + core) * 4 + to[1]))
    return lax.ppermute(shard, ("z", "core", "ba"), pairs)


def from_others(pieces, stage):
    got = [pieces[0]]
    for s in (1, 2, 3):
        got.append(around(pieces[s], stage, s))
    return tuple(got)


def swapped(shard):
    return lax.ppermute(shard, "core", [(0, 1), (1, 0)])


def per_device(
    features,
    tile_ids,
    cell_ids,
    spread_weight,
    read_weight,
    message_weight,
    skip_weight,
    spectral_weight,
    hidden_weight,
    output_weight,
):
    points, width = features.shape
    everyone = ("z", "y", "core", "ba")
    devices = lax.axis_size(everyone)
    shape = jax.ShapeDtypeStruct
    where = lax.axis_index(everyone).astype(jnp.int32).reshape(1)
    tile = tile_ids.reshape(1, points)
    cell = cell_ids.reshape(1, points)
    terms = basis_terms()
    basis = jnp.asarray(terms)
    basis_tall = jnp.asarray(np.ascontiguousarray(terms.T))

    anywhere = pl.BlockSpec(memory_space=pl.ANY)
    send, slots, message = pl.pallas_call(
        spread_body,
        out_shape=(
            shape((devices, 56, 128), BF16),
            shape((1, points), jnp.int32),
            shape((points, width), BF16),
        ),
        in_specs=[VMEM] + [anywhere] * 4,
        out_specs=[anywhere, VMEM, anywhere],
        scratch_shapes=[
            pltpu.VMEM((1, points), jnp.int32),
            pltpu.VMEM((points, width), BF16),
            pltpu.VMEM((points, 128), BF16),
            pltpu.VMEM((devices, 56, 128), BF16),
            pltpu.VMEM((points, width), BF16),
            pltpu.VMEM((1, points), jnp.int32),
            pltpu.VMEM((1, points), F32),
            pltpu.VMEM((width, width), BF16),
            pltpu.SemaphoreType.DMA((5,)),
            pltpu.SemaphoreType.DMA((4,)),
        ],
        name="spread",
        compiler_params=pltpu.CompilerParams(vmem_limit_bytes=60 * 2**20),
    )(tile, features, cell, spread_weight.reshape(1, points), message_weight)
    recv = lax.all_to_all(send, everyone, 0, 0, tiled=True)
    away = spectrum(message, tile, cell, basis, where, True)
    near = spectrum(message, tile, cell, basis, where, False)
    wave_p, wave_qz = call(
        waves_body,
        (shape((points, 1024), BF16), shape((points, 1024), BF16)),
        (tile, cell, basis_tall, where),
        (
            pltpu.VMEM((8, points), jnp.int32),
            pltpu.VMEM((256, 1024), BF16),
            pltpu.VMEM((256, 1024), BF16),
            pltpu.VMEM((128, 256), BF16),
        ),
        flops=10**9,
        scalars=1,
    )
    parts = add_and_cut((near, swapped(away)))
    parts = add_and_cut(from_others(parts, "wide"))
    parts = add_and_cut(from_others(parts, "near"))
    latent, places = call(
        collect_body,
        (shape((2048, width), BF16), shape((1024, 128), BF16)),
        (recv,),
        (pltpu.VMEM((3072, width), BF16), pltpu.VMEM((8, 8, 128), jnp.int32)),
        flops=2 * 3072 * 2048 * 256,
    )
    back = pl.pallas_call(
        reply_body,
        out_shape=shape((devices, 24, width), BF16),
        in_specs=[VMEM, VMEM, anywhere],
        out_specs=anywhere,
        scratch_shapes=[
            pltpu.VMEM((devices, 24, width), BF16),
            pltpu.SemaphoreType.DMA((4,)),
        ],
        name="reply",
        compiler_params=pltpu.CompilerParams(vmem_limit_bytes=20 * 2**20),
        cost_estimate=pl.CostEstimate(
            flops=2 * 3072 * 2048 * 256, transcendentals=0, bytes_accessed=4000000
        ),
    )(latent, places, spectral_weight)
    mixed = call(
        mix_body, shape((32, width), BF16), from_others(parts, "y") + (spectral_weight,), ()
    )
    line = joined(from_others((mixed,) * 4, "y"))
    plane = joined(from_others((line,) * 4, "near"))
    modes = from_others((plane,) * 4, "wide")
    modes = modes + tuple(swapped(m) for m in modes)

    returned = lax.all_to_all(back, everyone, 0, 0, tiled=True)
    base = call(
        own_body,
        shape((points, width), F32),
        (returned.reshape(devices * 24, width), slots, skip_weight),
        (),
        flops=2 * 3072 * 2048 * 256,
    )
    base = call(
        begin_body,
        shape((points, width), F32),
        (modes[0], modes[4], wave_p, wave_qz, base),
        (),
        flops=2 * 1024 * 2048 * 256,
    )
    arrays = modes[1:4] + modes[5:]
    arrays = arrays + (wave_p, wave_qz, base, read_weight.reshape(1, points))
    arrays = arrays + (hidden_weight, output_weight)
    return pl.pallas_call(
        decode_body,
        out_shape=shape((points, width), BF16),
        in_specs=[VMEM] * len(arrays),
        out_specs=anywhere,
        scratch_shapes=[pltpu.VMEM((points, width), BF16), pltpu.SemaphoreType.DMA((4,))],
        name="decode",
        compiler_params=pltpu.CompilerParams(vmem_limit_bytes=32 * 2**20),
        cost_estimate=pl.CostEstimate(
            flops=2 * 4096 * 2048 * 256, transcendentals=0, bytes_accessed=4000000
        ),
    )(*arrays)


def solution(mesh):
    finer = Mesh(mesh.devices.reshape(4, 4, 2, 4), ("z", "y", "core", "ba"))
    rows = P(("z", "y", "core", "ba"))
    every = P()
    placed = (
        P(("z", "y", "core", "ba"), None),
        P(("z", "y", "core", "ba"), None),
        rows,
        rows,
        rows,
        every,
        every,
        P("ba", ("z", "y", "core"), None, None),
        every,
        every,
    )

    return jax.shard_map(
        per_device,
        mesh=finer,
        in_specs=placed,
        out_specs=P(("z", "y", "core", "ba"), None),
        check_vma=False,
    )
```

```python
import functools

import jax
import jax.numpy as jnp
import numpy as np
from jax import lax
from jax.experimental import pallas as pl
from jax.experimental.pallas import tpu as pltpu
from jax.sharding import Mesh
from jax.sharding import PartitionSpec as P

G = 64
M = 16
F32 = jnp.float32
BF16 = jnp.bfloat16
VMEM = pl.BlockSpec(memory_space=pltpu.VMEM)
SMEM = pl.BlockSpec(memory_space=pltpu.SMEM)


def iota(shape, dim):
    return lax.broadcasted_iota(jnp.int32, shape, dim)


def mm(a, b):
    return lax.dot_general(a, b, (((1,), (0,)), ((), ())), preferred_element_type=F32)


def mm_nt(a, b):
    return lax.dot_general(a, b, (((1,), (1,)), ((), ())), preferred_element_type=F32)


def as_column(row, lanes):
    n = row.shape[1]
    return jnp.transpose(jnp.broadcast_to(row, (lanes, n)))


def call(body, outs, ins, scratch=(), limit=20, flops=1000000, scalars=0):
    single = not isinstance(outs, (tuple, list))
    fn = pl.pallas_call(
        body,
        out_shape=outs,
        in_specs=[VMEM] * (len(ins) - scalars) + [SMEM] * scalars,
        out_specs=VMEM if single else [VMEM] * len(outs),
        scratch_shapes=list(scratch),
        compiler_params=pltpu.CompilerParams(vmem_limit_bytes=limit * 2**20),
        cost_estimate=pl.CostEstimate(flops=flops, transcendentals=0, bytes_accessed=4000000),
    )
    return fn(*ins)


def spread_body(
    feat, tile, cell, spread, weight, send, slots, sent, rank_row, message, place, built, saves
):
    devices = built.shape[0]
    points = message.shape[0]
    cap = 24
    upper = (iota((256, 256), 0) < iota((256, 256), 1)).astype(BF16)
    ones = jnp.ones((256, 128), BF16)
    used = jnp.zeros((devices, 256), F32)
    for at in range(0, points, 256):
        hot = tile[:, at : at + 256] == iota((devices, 256), 0)
        hot = hot.astype(F32)
        hot16 = hot.astype(BF16)
        before = mm(hot16, upper) + used
        total = mm(hot16, ones)
        used = used + jnp.concatenate([total, total], axis=1)
        rank = jnp.sum(hot * before, axis=0, keepdims=True).astype(jnp.int32)
        rank_row[:, at : at + 256] = rank
        slots[:, at : at + 256] = tile[:, at : at + 256] * cap + rank
    lane = iota((128, 128), 1)

    def weigh(step, carry):
        at = step * 128
        product = mm(feat[pl.ds(at, 128), :], weight[...])
        scale = as_column(spread[:, pl.ds(at, 128)], 128)
        scale = jnp.concatenate([scale, scale], axis=1)
        message[pl.ds(at, 128), :] = (scale * product).astype(BF16)
        group = as_column(lax.shift_right_logical(rank_row[:, pl.ds(at, 128)], 3), 128)
        where = as_column(cell[:, pl.ds(at, 128)], 128)
        high_part = lax.shift_right_logical(where, 6).astype(F32)
        low_part = lax.bitwise_and(where, 63).astype(F32)
        both = jnp.where(lane == 2 * group, high_part, 0.0)
        both = jnp.where(lane == 2 * group + 1, low_part, both)
        place[pl.ds(at, 128), :] = both.astype(BF16)
        return carry

    lax.fori_loop(0, points // 128, weigh, 0, unroll=2)
    save_message = pltpu.make_async_copy(message, sent, saves.at[4])
    save_message.start()
    rank = rank_row[...]
    low = tile[...] * 8 + lax.bitwise_and(rank, 7)
    slot = slots[...]

    many = 32
    steps = devices // many

    def save(step):
        rows = pl.ds(step * many, many)
        return pltpu.make_async_copy(built.at[rows], send.at[rows], saves.at[step])

    def fill(step, carry):
        base = step * many
        hot = (slot - base * cap == iota((many * cap, points), 0)).astype(BF16)
        rows = mm(hot, message[...])
        left = rows[:, :128].reshape(many, cap, 128).astype(BF16)
        right = rows[:, 128:].reshape(many, cap, 128).astype(BF16)
        hot8 = (low - base * 8 == iota((many * 8, points), 0)).astype(BF16)
        placing = mm(hot8, place[...]).reshape(many, 8, 128).astype(BF16)
        built[pl.ds(base, many), 0:cap, :] = left
        built[pl.ds(base, many), cap : 2 * cap, :] = right
        built[pl.ds(base, many), 2 * cap :, :] = placing
        save(step).start()
        return carry

    lax.fori_loop(0, steps, fill, 0)
    save_message.wait()
    for step in range(steps):
        save(step).wait()


def positions(tile, cell):
    x = lax.shift_right_logical(tile, 2) * 2 + lax.shift_right_logical(cell, 10)
    y = lax.bitwise_and(tile, 3) * 16 + lax.bitwise_and(lax.shift_right_logical(cell, 6), 15)
    return x, y, lax.bitwise_and(cell, 63)


def device_at(where):
    d = where[0]
    return d // 32, d // 8 % 4, d // 4 % 2, d % 4


def bits(value, low, mask):
    return lax.bitwise_and(lax.shift_right_logical(value, low), mask)


def flipped(at, group):
    low = bits(group, 0, 1)
    return lax.bitwise_xor(at, lax.bitwise_xor(low, bits(group, 1, 1)) + 2 * low)


def spectrum_body(message, tile, cell, basis, where, out, xy, away):
    points = message.shape[0]
    at_z, at_y, core, at_b = device_at(where)
    core = 1 - core if away else core
    r = iota((256, 16), 0)
    wide, near, last, j4 = bits(r, 6, 3), bits(r, 4, 3), bits(r, 2, 3), bits(r, 0, 3)
    straight = jnp.full(r.shape, core, jnp.int32) == 0
    turn_z, turn_b = flipped(at_z, near), flipped(at_b, near)
    mode_x = 4 * jnp.where(straight, turn_z, bits(at_z + wide, 0, 3)) + flipped(at_y, last)
    mode_y = 4 * jnp.where(straight, bits(at_b + wide, 0, 3), turn_b) + j4
    mode_z = 8 * core + iota((8, 16), 0)
    x, y, z = positions(tile[...], cell[...])
    row = lax.bitwise_and(iota((128, points), 0), 63)

    def values(mode, at):
        pick = (mode == iota(mode.shape, 1)).astype(BF16)
        table = mm(pick, basis[...]).astype(BF16)
        return mm(table, (at == row).astype(BF16))

    xy[...] = values(mode_x, x) * values(mode_y, y)
    zs = values(mode_z, z)

    def some(s, carry):
        rows = [(xy[pl.ds(s * 64 + i, 1), :] * zs).astype(F32) for i in range(64)]
        wave = jnp.concatenate(rows, axis=0).astype(BF16)
        out[pl.ds(s * 512, 512), :] = mm(wave, message[...]).astype(BF16)
        return carry

    lax.fori_loop(0, 4, some, 0)


def spectrum(message, tile, cell, basis, where, away):
    points = message.shape[0]
    return call(
        functools.partial(spectrum_body, away=away),
        jax.ShapeDtypeStruct((2048, 256), BF16),
        (message, tile, cell, basis, where),
        (pltpu.VMEM((256, points), F32),),
        flops=2 * 2048 * 2048 * 256,
        scalars=1,
    )


def add_body(*refs, cuts):
    count = len(refs) - cuts
    total = refs[0][...].astype(F32)
    for r in refs[1:count]:
        total = total + r[...].astype(F32)
    rows = total.shape[0] // cuts
    for s in range(cuts):
        refs[count + s][...] = total[s * rows : s * rows + rows].astype(BF16)


def add_and_cut(parts, cuts):
    rows, width = parts[0].shape
    piece = jax.ShapeDtypeStruct((rows // cuts, width), BF16)
    return call(functools.partial(add_body, cuts=cuts), (piece,) * cuts, parts, ())


def join_body(*refs):
    rows = refs[0].shape[0]
    for s in range(4):
        refs[4][s * rows : s * rows + rows, :] = refs[s][...]


def joined(parts):
    rows, width = parts[0].shape
    return call(join_body, jax.ShapeDtypeStruct((rows * 4, width), BF16), parts, ())


def total_cells(ids, rows, latent, first):
    tile = 512

    def total(step, carry):
        at = step * tile
        cells = iota((tile, 128), 0) + (at + first)
        hot = [
            (ids[i, g : g + 1, :] == cells).astype(BF16) for i in range(8) for g in range(3)
        ]
        latent[pl.ds(at, tile), :] = mm(jnp.concatenate(hot, axis=1), rows[...]).astype(BF16)
        return carry

    lax.fori_loop(0, latent.shape[0] // tile, total, 0)


def collect_body(recv, latent, places, rows, ids):
    picks = jnp.where(
        iota((8, 128), 1) == 2 * iota((8, 128), 0),
        64.0,
        jnp.where(iota((8, 128), 1) == 2 * iota((8, 128), 0) + 1, 1.0, 0.0),
    ).astype(BF16)

    def unpack(step, carry):
        block = recv[pl.ds(step * 16, 16)].astype(F32)
        place = block[:, 48:56, :].reshape(128, 128).astype(BF16)
        places[pl.ds(step * 128, 128), :] = place
        ids[step] = mm_nt(picks, place).astype(jnp.int32)
        for g in range(3):
            left = block[:, g * 8 : g * 8 + 8, :].reshape(128, 128)
            right = block[:, 24 + g * 8 : 32 + g * 8, :].reshape(128, 128)
            both = jnp.concatenate([left, right], axis=1).astype(BF16)
            rows[pl.ds(step * 384 + g * 128, 128), :] = both
        return carry

    lax.fori_loop(0, 8, unpack, 0)
    total_cells(ids, rows, latent, 0)


def collect_more_body(rows, ids, latent):
    total_cells(ids, rows, latent, latent.shape[0])


def reply_body(low, high, places, *refs, first):
    out, built, saves = refs[-3:]
    lane = iota((128, 128), 0)
    many = 32
    column = iota((many * 8, 128), 1)

    def back(step, carry):
        place = places[pl.ds((step + first) * many * 8, many * 8), :]
        tall = []
        for g in range(3):
            pick = jnp.where(lane == 2 * g, 64.0, jnp.where(lane == 2 * g + 1, 1.0, 0.0))
            cell = mm(place, pick.astype(BF16)).astype(jnp.int32)
            hot = [(cell == column + 128 * k).astype(BF16) for k in range(16)]
            tall.append(jnp.concatenate(hot, axis=1))
        tall = jnp.concatenate(tall, axis=0)
        got = mm(tall[:, :1024], low[...]) + mm(tall[:, 1024:], high[...])
        for g in range(3):
            piece = got[g * many * 8 : (g + 1) * many * 8]
            piece = piece.reshape(many, 8, 256).astype(BF16)
            built[pl.ds(step * many, many), g * 8 : g * 8 + 8, :] = piece
        save(step).start()
        return carry

    def save(step):
        source = built.at[pl.ds(step * many, many)]
        target = out.at[pl.ds((step + first) * many, many)]
        return pltpu.make_async_copy(source, target, saves.at[step])

    lax.fori_loop(0, 2, back, 0)
    for step in range(2):
        save(step).wait()


def reply(low, high, places, before):
    anywhere = pl.BlockSpec(memory_space=pl.ANY)
    return pl.pallas_call(
        functools.partial(reply_body, first=2 * (len(before) - 1)),
        out_shape=jax.ShapeDtypeStruct((128, 24, 256), BF16),
        in_specs=[VMEM, VMEM, VMEM] + [anywhere] * len(before),
        out_specs=anywhere,
        scratch_shapes=[
            pltpu.VMEM((64, 24, 256), BF16),
            pltpu.SemaphoreType.DMA((2,)),
        ],
        input_output_aliases={4: 0} if len(before) == 2 else {},
        compiler_params=pltpu.CompilerParams(vmem_limit_bytes=20 * 2**20),
        cost_estimate=pl.CostEstimate(
            flops=3072 * 2048 * 256, transcendentals=0, bytes_accessed=4000000
        ),
    )(low, high, places, *before)


def mix_body(a, b, weight, out):
    spec = a[...].astype(F32) + b[...].astype(F32)
    spec = spec.astype(BF16)
    row = iota((8, 256), 0)
    for j in range(4):
        mixed = jnp.zeros((8, 256), F32)
        for m in range(8):
            mixed = jnp.where(row == m, mm(spec[j * 8 : j * 8 + 8], weight[j, m]), mixed)
        out[j * 8 : j * 8 + 8, :] = mixed.astype(BF16)


def own_body(returned, slots, skip, out):
    def some(step, carry):
        at = step * 512
        hot = []
        for p in range(4):
            slot = as_column(slots[:, pl.ds(at + p * 128, 128)], 128)
            one = [(slot == iota((128, 128), 1) + 128 * k).astype(BF16) for k in range(24)]
            hot.append(jnp.concatenate(one, axis=1))
        own = mm(jnp.concatenate(hot, axis=0), returned[...]).astype(BF16)
        out[pl.ds(at, 512), :] = mm(own, skip[...])
        return carry

    lax.fori_loop(0, out.shape[0] // 512, some, 0)


def waves_body(tile, cell, basis, where, out_p, out_qz, spots, wide_p, wide_q, wide_z):
    at_z, at_y, at_core, at_b = device_at(where)
    lane = iota((16, 1024), 1)
    outer, last, j4 = bits(lane, 7, 3), bits(lane, 5, 3), bits(lane, 3, 3)
    mode_x = 4 * bits(at_z - outer, 0, 3) + bits(at_y - last, 0, 3)
    mode_y = 4 * bits(at_b - outer, 0, 3) + j4
    lane = iota((16, 256), 1)
    mode_z = 8 * lax.bitwise_xor(bits(lane, 7, 1), at_core) + bits(lane, 0, 7)

    def table(mode):
        return mm(basis[...], (mode == iota(mode.shape, 0)).astype(BF16))

    straight = lax.bitwise_xor(bits(iota((128, 1024), 1), 9, 1), at_core) == 0
    factor = table(mode_x)
    wide_p[0:128, :] = jnp.where(straight, factor, 0.0).astype(BF16)
    wide_q[0:128, :] = jnp.where(straight, 0.0, factor).astype(BF16)
    factor = table(mode_y)
    wide_p[128:256, :] = jnp.where(straight, 0.0, factor).astype(BF16)
    wide_q[128:256, :] = jnp.where(straight, factor, 0.0).astype(BF16)
    wide_z[...] = table(mode_z).astype(BF16)
    x, y, z = positions(tile[...], cell[...])
    spots[0:1, :] = x
    spots[1:2, :] = y
    spots[2:3, :] = z
    lane = lax.bitwise_and(iota((128, 128), 1), 63)

    def some(step, carry):
        at = step * 128

        def hot(which):
            col = as_column(spots[which : which + 1, pl.ds(at, 128)], 128)
            return (col == lane).astype(BF16)

        xy = jnp.concatenate([hot(0), hot(1)], axis=1)
        out_p[pl.ds(at, 128), :] = mm(xy, wide_p[...]).astype(BF16)
        q = mm(xy, wide_q[...])
        vz = mm(hot(2), wide_z[...])
        for h in range(2):
            for o in range(4):
                to = (h * 4 + o) * 128
                qz = q[:, to : to + 128] * vz[:, h * 128 : h * 128 + 128]
                out_qz[pl.ds(at, 128), to : to + 128] = qz.astype(BF16)
        return carry

    lax.fori_loop(0, out_p.shape[0] // 128, some, 0)


def wave_of(wave_p, wave_qz, at, rows, h, o):
    qz = wave_qz[pl.ds(at, rows), (h * 4 + o) * 128 : (h * 4 + o) * 128 + 128]
    wave = [
        qz * wave_p[pl.ds(at, rows), h * 512 + i * 128 : h * 512 + i * 128 + 128]
        for i in range(4)
    ]
    return jnp.concatenate(wave, axis=1)


def begin_body(near, far, wave_p, wave_qz, base, out):
    def some(step, carry):
        at = step * 512
        total = base[pl.ds(at, 512), :]
        total = total + mm(wave_of(wave_p, wave_qz, at, 512, 0, 0), near[...])
        out[pl.ds(at, 512), :] = total + mm(wave_of(wave_p, wave_qz, at, 512, 1, 0), far[...])
        return carry

    lax.fori_loop(0, out.shape[0] // 512, some, 0)


def decode_body(
    m1, m2, m3, m5, m6, m7, wave_p, wave_qz, base, read, hidden_weight, output_weight, out, built, saves
):
    modes = ((m1, m2, m3), (m5, m6, m7))

    def some(step, carry):
        at = step * 512
        total = base[pl.ds(at, 512), :]
        for h in range(2):
            for o in range(3):
                wave = wave_of(wave_p, wave_qz, at, 512, h, o + 1)
                total = total + mm(wave, modes[h][o][...])
        value = jax.nn.gelu(total).astype(BF16).astype(F32)
        scale = jnp.concatenate(
            [as_column(read[:, pl.ds(at + 128 * part, 128)], 128) for part in range(4)], axis=0
        )
        gathered = (jnp.concatenate([scale, scale], axis=1) * value).astype(BF16)
        hidden = jax.nn.gelu(mm(gathered, hidden_weight[...])).astype(BF16)
        built[pl.ds(at, 512), :] = mm(hidden, output_weight[...]).astype(BF16)
        save(step).start()
        return carry

    def save(step):
        rows = pl.ds(step * 512, 512)
        return pltpu.make_async_copy(built.at[rows], out.at[rows], saves.at[step])

    lax.fori_loop(0, 4, some, 0)
    for step in range(4):
        save(step).wait()


def basis_terms():
    mode = np.arange(M)[:, None]
    frequency = np.where(mode < M // 2, mode, mode - M // 2 + 1)
    phase = 2.0 * np.pi * frequency * np.arange(G)[None, :] / G
    wave = np.where(mode < M // 2, np.cos(phase), np.sin(phase))
    wave = wave * np.where(mode == 0, np.sqrt(1.0 / G), np.sqrt(2.0 / G))
    high = wave.astype(np.float32).astype(jnp.bfloat16)
    low = (wave - high.astype(np.float64)).astype(np.float32).astype(jnp.bfloat16)
    return np.concatenate([high, low], axis=1)


def around(shard, stage, s):
    if stage == "y":
        return lax.ppermute(shard, "y", [(i, (i + s) % 4) for i in range(4)])
    pairs = []
    for z in range(4):
        for core in range(2):
            for b in range(4):
                along_b = (core == 0) == (stage == "wide")
                to = (z, (b + s) % 4) if along_b else ((z + s) % 4, b)
                pairs.append(((z * 2 + core) * 4 + b, (to[0] * 2 + core) * 4 + to[1]))
    return lax.ppermute(shard, ("z", "core", "ba"), pairs)


def flip(shard, stage, turn):
    if stage == "y":
        return lax.ppermute(shard, "y", [(i, i ^ turn) for i in range(4)])
    pairs = []
    for z in range(4):
        for core in range(2):
            for b in range(4):
                to = (z ^ turn, b) if core == 0 else (z, b ^ turn)
                pairs.append(((z * 2 + core) * 4 + b, (to[0] * 2 + core) * 4 + to[1]))
    return lax.ppermute(shard, ("z", "core", "ba"), pairs)


def from_others(pieces, stage):
    got = [pieces[0]]
    for s in (1, 2, 3):
        got.append(around(pieces[s], stage, s))
    return tuple(got)


def swapped(shard):
    return lax.ppermute(shard, "core", [(0, 1), (1, 0)])


def per_device(
    features,
    tile_ids,
    cell_ids,
    spread_weight,
    read_weight,
    message_weight,
    skip_weight,
    spectral_weight,
    hidden_weight,
    output_weight,
):
    points, width = features.shape
    everyone = ("z", "y", "core", "ba")
    devices = lax.axis_size(everyone)
    shape = jax.ShapeDtypeStruct
    where = lax.axis_index(everyone).astype(jnp.int32).reshape(1)
    tile = tile_ids.reshape(1, points)
    cell = cell_ids.reshape(1, points)
    terms = basis_terms()
    basis = jnp.asarray(terms)
    basis_tall = jnp.asarray(np.ascontiguousarray(terms.T))

    anywhere = pl.BlockSpec(memory_space=pl.ANY)
    send, slots, message = pl.pallas_call(
        spread_body,
        out_shape=(
            shape((devices, 56, 128), BF16),
            shape((1, points), jnp.int32),
            shape((points, width), BF16),
        ),
        in_specs=[VMEM] * 5,
        out_specs=[anywhere, VMEM, anywhere],
        scratch_shapes=[
            pltpu.VMEM((1, points), jnp.int32),
            pltpu.VMEM((points, width), BF16),
            pltpu.VMEM((points, 128), BF16),
            pltpu.VMEM((devices, 56, 128), BF16),
            pltpu.SemaphoreType.DMA((5,)),
        ],
        name="spread",
        compiler_params=pltpu.CompilerParams(vmem_limit_bytes=60 * 2**20),
    )(features, tile, cell, spread_weight.reshape(1, points), message_weight)
    recv = lax.all_to_all(send, everyone, 0, 0, tiled=True)
    away = spectrum(message, tile, cell, basis, where, True)
    near = spectrum(message, tile, cell, basis, where, False)
    wave_p, wave_qz = call(
        waves_body,
        (shape((points, 1024), BF16), shape((points, 1024), BF16)),
        (tile, cell, basis_tall, where),
        (
            pltpu.VMEM((8, points), jnp.int32),
            pltpu.VMEM((256, 1024), BF16),
            pltpu.VMEM((256, 1024), BF16),
            pltpu.VMEM((128, 256), BF16),
        ),
        flops=10**9,
        scalars=1,
    )
    parts = add_and_cut((near, swapped(away)), 4)
    keep, give = add_and_cut(from_others(parts, "wide"), 2)
    keep, give = add_and_cut((keep, flip(give, "near", 1)), 2)
    keep, give = add_and_cut((keep, flip(give, "near", 3)), 2)
    keep, give = add_and_cut((keep, flip(give, "y", 1)), 2)
    low, places, sorted_rows, ids = call(
        collect_body,
        (
            shape((1024, width), BF16),
            shape((1024, 128), BF16),
            shape((3072, width), BF16),
            shape((8, 8, 128), jnp.int32),
        ),
        (recv,),
        (),
        flops=3072 * 2048 * 256,
    )
    high = call(
        collect_more_body,
        shape((1024, width), BF16),
        (sorted_rows, ids),
        (),
        flops=3072 * 2048 * 256,
    )
    back = reply(low, high, places, (spectral_weight,))
    back = reply(low, high, places, (spectral_weight, back))
    mixed = call(
        mix_body, shape((32, width), BF16), (keep, flip(give, "y", 3), spectral_weight), ()
    )
    line = joined(from_others((mixed,) * 4, "y"))
    plane = joined(from_others((line,) * 4, "near"))
    modes = from_others((plane,) * 4, "wide")
    modes = modes + tuple(swapped(m) for m in modes)

    returned = lax.all_to_all(back, everyone, 0, 0, tiled=True)
    base = call(
        own_body,
        shape((points, width), F32),
        (returned.reshape(devices * 24, width), slots, skip_weight),
        (),
        flops=2 * 3072 * 2048 * 256,
    )
    base = call(
        begin_body,
        shape((points, width), F32),
        (modes[0], modes[4], wave_p, wave_qz, base),
        (),
        flops=2 * 1024 * 2048 * 256,
    )
    arrays = modes[1:4] + modes[5:]
    arrays = arrays + (wave_p, wave_qz, base, read_weight.reshape(1, points))
    arrays = arrays + (hidden_weight, output_weight)
    return pl.pallas_call(
        decode_body,
        out_shape=shape((points, width), BF16),
        in_specs=[VMEM] * len(arrays),
        out_specs=anywhere,
        scratch_shapes=[pltpu.VMEM((points, width), BF16), pltpu.SemaphoreType.DMA((4,))],
        name="decode",
        compiler_params=pltpu.CompilerParams(vmem_limit_bytes=32 * 2**20),
        cost_estimate=pl.CostEstimate(
            flops=2 * 4096 * 2048 * 256, transcendentals=0, bytes_accessed=4000000
        ),
    )(*arrays)


def solution(mesh):
    finer = Mesh(mesh.devices.reshape(4, 4, 2, 4), ("z", "y", "core", "ba"))
    rows = P(("z", "y", "core", "ba"))
    every = P()
    placed = (
        P(("z", "y", "core", "ba"), None),
        P(("z", "y", "core", "ba"), None),
        rows,
        rows,
        rows,
        every,
        every,
        P("ba", ("z", "y", "core"), None, None),
        every,
        every,
    )

    return jax.shard_map(
        per_device,
        mesh=finer,
        in_specs=placed,
        out_specs=P(("z", "y", "core", "ba"), None),
        check_vma=False,
    )
```

```python
import functools

import jax
import jax.numpy as jnp
import numpy as np
from jax import lax
from jax.experimental import pallas as pl
from jax.experimental.pallas import tpu as pltpu
from jax.sharding import Mesh
from jax.sharding import PartitionSpec as P

G = 64
M = 16
F32 = jnp.float32
BF16 = jnp.bfloat16
VMEM = pl.BlockSpec(memory_space=pltpu.VMEM)
SMEM = pl.BlockSpec(memory_space=pltpu.SMEM)


def iota(shape, dim):
    return lax.broadcasted_iota(jnp.int32, shape, dim)


def mm(a, b):
    return lax.dot_general(a, b, (((1,), (0,)), ((), ())), preferred_element_type=F32)


def mm_nt(a, b):
    return lax.dot_general(a, b, (((1,), (1,)), ((), ())), preferred_element_type=F32)


def as_column(row, lanes):
    n = row.shape[1]
    return jnp.transpose(jnp.broadcast_to(row, (lanes, n)))


def call(body, outs, ins, scratch=(), limit=20, flops=1000000, scalars=0):
    single = not isinstance(outs, (tuple, list))
    fn = pl.pallas_call(
        body,
        out_shape=outs,
        in_specs=[VMEM] * (len(ins) - scalars) + [SMEM] * scalars,
        out_specs=VMEM if single else [VMEM] * len(outs),
        scratch_shapes=list(scratch),
        compiler_params=pltpu.CompilerParams(vmem_limit_bytes=limit * 2**20),
        cost_estimate=pl.CostEstimate(flops=flops, transcendentals=0, bytes_accessed=4000000),
    )
    return fn(*ins)


def spread_body(
    feat, tile, cell, spread, weight, send, slots, sent, rank_row, message, place, built, saves
):
    devices = built.shape[0]
    points = message.shape[0]
    cap = 24
    upper = (iota((256, 256), 0) < iota((256, 256), 1)).astype(BF16)
    ones = jnp.ones((256, 128), BF16)
    used = jnp.zeros((devices, 256), F32)
    for at in range(0, points, 256):
        hot = tile[:, at : at + 256] == iota((devices, 256), 0)
        hot = hot.astype(F32)
        hot16 = hot.astype(BF16)
        before = mm(hot16, upper) + used
        total = mm(hot16, ones)
        used = used + jnp.concatenate([total, total], axis=1)
        rank = jnp.sum(hot * before, axis=0, keepdims=True).astype(jnp.int32)
        rank_row[:, at : at + 256] = rank
        slots[:, at : at + 256] = tile[:, at : at + 256] * cap + rank
    lane = iota((128, 128), 1)

    def weigh(step, carry):
        at = step * 128
        product = mm(feat[pl.ds(at, 128), :], weight[...])
        scale = as_column(spread[:, pl.ds(at, 128)], 128)
        scale = jnp.concatenate([scale, scale], axis=1)
        message[pl.ds(at, 128), :] = (scale * product).astype(BF16)
        group = as_column(lax.shift_right_logical(rank_row[:, pl.ds(at, 128)], 3), 128)
        where = as_column(cell[:, pl.ds(at, 128)], 128)
        high_part = lax.shift_right_logical(where, 6).astype(F32)
        low_part = lax.bitwise_and(where, 63).astype(F32)
        both = jnp.where(lane == 2 * group, high_part, 0.0)
        both = jnp.where(lane == 2 * group + 1, low_part, both)
        place[pl.ds(at, 128), :] = both.astype(BF16)
        return carry

    lax.fori_loop(0, points // 128, weigh, 0, unroll=2)
    save_message = pltpu.make_async_copy(message, sent, saves.at[4])
    save_message.start()
    rank = rank_row[...]
    low = tile[...] * 8 + lax.bitwise_and(rank, 7)
    slot = slots[...]

    many = 32
    steps = devices // many

    def save(step):
        rows = pl.ds(step * many, many)
        return pltpu.make_async_copy(built.at[rows], send.at[rows], saves.at[step])

    def fill(step, carry):
        base = step * many
        hot = (slot - base * cap == iota((many * cap, points), 0)).astype(BF16)
        rows = mm(hot, message[...])
        left = rows[:, :128].reshape(many, cap, 128).astype(BF16)
        right = rows[:, 128:].reshape(many, cap, 128).astype(BF16)
        hot8 = (low - base * 8 == iota((many * 8, points), 0)).astype(BF16)
        placing = mm(hot8, place[...]).reshape(many, 8, 128).astype(BF16)
        built[pl.ds(base, many), 0:cap, :] = left
        built[pl.ds(base, many), cap : 2 * cap, :] = right
        built[pl.ds(base, many), 2 * cap :, :] = placing
        save(step).start()
        return carry

    lax.fori_loop(0, steps, fill, 0)
    save_message.wait()
    for step in range(steps):
        save(step).wait()


def positions(tile, cell):
    x = lax.shift_right_logical(tile, 2) * 2 + lax.shift_right_logical(cell, 10)
    y = lax.bitwise_and(tile, 3) * 16 + lax.bitwise_and(lax.shift_right_logical(cell, 6), 15)
    return x, y, lax.bitwise_and(cell, 63)


def device_at(where):
    d = where[0]
    return d // 32, d // 8 % 4, d // 4 % 2, d % 4


def bits(value, low, mask):
    return lax.bitwise_and(lax.shift_right_logical(value, low), mask)


def spectrum_body(message, tile, cell, basis, where, out, xy, away):
    points = message.shape[0]
    at_z, at_y, core, at_b = device_at(where)
    core = 1 - core if away else core
    r = iota((256, 16), 0)
    wide, near, last, j4 = bits(r, 6, 3), bits(r, 4, 3), bits(r, 2, 3), bits(r, 0, 3)
    shift_x = near + core * (wide - near)
    shift_y = wide + near - shift_x
    mode_x = 4 * bits(at_z + shift_x, 0, 3) + bits(at_y + last, 0, 3)
    mode_y = 4 * bits(at_b + shift_y, 0, 3) + j4
    mode_z = 8 * core + iota((8, 16), 0)
    x, y, z = positions(tile[...], cell[...])
    row = lax.bitwise_and(iota((128, points), 0), 63)

    def values(mode, at):
        pick = (mode == iota(mode.shape, 1)).astype(BF16)
        table = mm(pick, basis[...]).astype(BF16)
        return mm(table, (at == row).astype(BF16))

    xy[...] = values(mode_x, x) * values(mode_y, y)
    zs = values(mode_z, z)

    def some(s, carry):
        rows = [(xy[pl.ds(s * 64 + i, 1), :] * zs).astype(F32) for i in range(64)]
        wave = jnp.concatenate(rows, axis=0).astype(BF16)
        out[pl.ds(s * 512, 512), :] = mm(wave, message[...]).astype(BF16)
        return carry

    lax.fori_loop(0, 4, some, 0)


def spectrum(message, tile, cell, basis, where, away):
    points = message.shape[0]
    return call(
        functools.partial(spectrum_body, away=away),
        jax.ShapeDtypeStruct((2048, 256), BF16),
        (message, tile, cell, basis, where),
        (pltpu.VMEM((256, points), F32),),
        flops=2 * 2048 * 2048 * 256,
        scalars=1,
    )


def add_body(*refs):
    count = len(refs) - 4
    total = refs[0][...].astype(F32)
    for r in refs[1:count]:
        total = total + r[...].astype(F32)
    rows = total.shape[0] // 4
    for s in range(4):
        refs[count + s][...] = total[s * rows : s * rows + rows].astype(BF16)


def add_and_cut(parts):
    rows, width = parts[0].shape
    piece = jax.ShapeDtypeStruct((rows // 4, width), BF16)
    return call(add_body, (piece,) * 4, parts, ())


def join_body(*refs):
    rows = refs[0].shape[0]
    for s in range(4):
        refs[4][s * rows : s * rows + rows, :] = refs[s][...]


def joined(parts):
    rows, width = parts[0].shape
    return call(join_body, jax.ShapeDtypeStruct((rows * 4, width), BF16), parts, ())


def collect_body(recv, latent, places, rows, ids):
    picks = jnp.where(
        iota((8, 128), 1) == 2 * iota((8, 128), 0),
        64.0,
        jnp.where(iota((8, 128), 1) == 2 * iota((8, 128), 0) + 1, 1.0, 0.0),
    ).astype(BF16)

    def unpack(step, carry):
        block = recv[pl.ds(step * 16, 16)].astype(F32)
        place = block[:, 48:56, :].reshape(128, 128).astype(BF16)
        places[pl.ds(step * 128, 128), :] = place
        ids[step] = mm_nt(picks, place).astype(jnp.int32)
        for g in range(3):
            left = block[:, g * 8 : g * 8 + 8, :].reshape(128, 128)
            right = block[:, 24 + g * 8 : 32 + g * 8, :].reshape(128, 128)
            both = jnp.concatenate([left, right], axis=1).astype(BF16)
            rows[pl.ds(step * 384 + g * 128, 128), :] = both
        return carry

    lax.fori_loop(0, 8, unpack, 0)
    tile = 1024

    def total(step, carry):
        at = step * tile
        cells = iota((tile, 128), 0) + at
        hot = [
            (ids[i, g : g + 1, :] == cells).astype(BF16) for i in range(8) for g in range(3)
        ]
        latent[pl.ds(at, tile), :] = mm(jnp.concatenate(hot, axis=1), rows[...]).astype(BF16)
        return carry

    lax.fori_loop(0, latent.shape[0] // tile, total, 0)


def reply_body(latent, places, weight, out, built, saves):
    lane = iota((128, 128), 0)
    column = iota((256, 128), 1)

    many = 32

    def back(step, carry):
        place = places[pl.ds(step * many * 8, many * 8), :]
        tall = []
        for g in range(3):
            pick = jnp.where(lane == 2 * g, 64.0, jnp.where(lane == 2 * g + 1, 1.0, 0.0))
            cell = mm(place, pick.astype(BF16)).astype(jnp.int32)
            hot = [(cell == column + 128 * k).astype(BF16) for k in range(16)]
            tall.append(jnp.concatenate(hot, axis=1))
        got = mm(jnp.concatenate(tall, axis=0), latent[...])
        for g in range(3):
            piece = got[g * many * 8 : (g + 1) * many * 8]
            piece = piece.reshape(many, 8, 256).astype(BF16)
            built[pl.ds(step * many, many), g * 8 : g * 8 + 8, :] = piece
        save(step).start()
        return carry

    def save(step):
        rows = pl.ds(step * many, many)
        return pltpu.make_async_copy(built.at[rows], out.at[rows], saves.at[step])

    lax.fori_loop(0, 4, back, 0)
    for step in range(4):
        save(step).wait()


def mix_body(a, b, c, d, weight, out):
    spec = a[...].astype(F32) + b[...].astype(F32) + c[...].astype(F32) + d[...].astype(F32)
    spec = spec.astype(BF16)
    row = iota((8, 256), 0)
    for j in range(4):
        mixed = jnp.zeros((8, 256), F32)
        for m in range(8):
            mixed = jnp.where(row == m, mm(spec[j * 8 : j * 8 + 8], weight[j, m]), mixed)
        out[j * 8 : j * 8 + 8, :] = mixed.astype(BF16)


def own_body(returned, slots, skip, out):
    def some(step, carry):
        at = step * 1024
        hot = []
        for p in range(8):
            slot = as_column(slots[:, pl.ds(at + p * 128, 128)], 128)
            one = [(slot == iota((128, 128), 1) + 128 * k).astype(BF16) for k in range(24)]
            hot.append(jnp.concatenate(one, axis=1))
        own = mm(jnp.concatenate(hot, axis=0), returned[...]).astype(BF16)
        out[pl.ds(at, 1024), :] = mm(own, skip[...])
        return carry

    lax.fori_loop(0, out.shape[0] // 1024, some, 0)


def waves_body(tile, cell, basis, where, out_p, out_qz, spots, wide_p, wide_q, wide_z):
    at_z, at_y, at_core, at_b = device_at(where)
    lane = iota((16, 1024), 1)
    outer, last, j4 = bits(lane, 7, 3), bits(lane, 5, 3), bits(lane, 3, 3)
    mode_x = 4 * bits(at_z - outer, 0, 3) + bits(at_y - last, 0, 3)
    mode_y = 4 * bits(at_b - outer, 0, 3) + j4
    lane = iota((16, 256), 1)
    mode_z = 8 * lax.bitwise_xor(bits(lane, 7, 1), at_core) + bits(lane, 0, 7)

    def table(mode):
        return mm(basis[...], (mode == iota(mode.shape, 0)).astype(BF16))

    straight = lax.bitwise_xor(bits(iota((128, 1024), 1), 9, 1), at_core) == 0
    factor = table(mode_x)
    wide_p[0:128, :] = jnp.where(straight, factor, 0.0).astype(BF16)
    wide_q[0:128, :] = jnp.where(straight, 0.0, factor).astype(BF16)
    factor = table(mode_y)
    wide_p[128:256, :] = jnp.where(straight, 0.0, factor).astype(BF16)
    wide_q[128:256, :] = jnp.where(straight, factor, 0.0).astype(BF16)
    wide_z[...] = table(mode_z).astype(BF16)
    x, y, z = positions(tile[...], cell[...])
    spots[0:1, :] = x
    spots[1:2, :] = y
    spots[2:3, :] = z
    lane = lax.bitwise_and(iota((128, 128), 1), 63)

    def some(step, carry):
        at = step * 128

        def hot(which):
            col = as_column(spots[which : which + 1, pl.ds(at, 128)], 128)
            return (col == lane).astype(BF16)

        xy = jnp.concatenate([hot(0), hot(1)], axis=1)
        out_p[pl.ds(at, 128), :] = mm(xy, wide_p[...]).astype(BF16)
        q = mm(xy, wide_q[...])
        vz = mm(hot(2), wide_z[...])
        for h in range(2):
            for o in range(4):
                to = (h * 4 + o) * 128
                qz = q[:, to : to + 128] * vz[:, h * 128 : h * 128 + 128]
                out_qz[pl.ds(at, 128), to : to + 128] = qz.astype(BF16)
        return carry

    lax.fori_loop(0, out_p.shape[0] // 128, some, 0)


def wave_of(wave_p, wave_qz, at, rows, h, o):
    qz = wave_qz[pl.ds(at, rows), (h * 4 + o) * 128 : (h * 4 + o) * 128 + 128]
    wave = [
        qz * wave_p[pl.ds(at, rows), h * 512 + i * 128 : h * 512 + i * 128 + 128]
        for i in range(4)
    ]
    return jnp.concatenate(wave, axis=1)


def begin_body(near, far, wave_p, wave_qz, base, out):
    def some(step, carry):
        at = step * 512
        total = base[pl.ds(at, 512), :]
        total = total + mm(wave_of(wave_p, wave_qz, at, 512, 0, 0), near[...])
        out[pl.ds(at, 512), :] = total + mm(wave_of(wave_p, wave_qz, at, 512, 1, 0), far[...])
        return carry

    lax.fori_loop(0, out.shape[0] // 512, some, 0)


def decode_body(
    m1, m2, m3, m5, m6, m7, wave_p, wave_qz, base, read, hidden_weight, output_weight, out, built, saves
):
    modes = ((m1, m2, m3), (m5, m6, m7))

    def some(step, carry):
        at = step * 1024
        total = base[pl.ds(at, 1024), :]
        for h in range(2):
            for o in range(3):
                wave = wave_of(wave_p, wave_qz, at, 1024, h, o + 1)
                total = total + mm(wave, modes[h][o][...])
        value = jax.nn.gelu(total).astype(BF16).astype(F32)
        scale = jnp.concatenate(
            [as_column(read[:, pl.ds(at + 128 * part, 128)], 128) for part in range(8)], axis=0
        )
        gathered = (jnp.concatenate([scale, scale], axis=1) * value).astype(BF16)
        hidden = jax.nn.gelu(mm(gathered, hidden_weight[...])).astype(BF16)
        built[pl.ds(at, 1024), :] = mm(hidden, output_weight[...]).astype(BF16)
        save(step).start()
        return carry

    def save(step):
        rows = pl.ds(step * 1024, 1024)
        return pltpu.make_async_copy(built.at[rows], out.at[rows], saves.at[step])

    lax.fori_loop(0, 2, some, 0)
    for step in range(2):
        save(step).wait()


def basis_terms():
    mode = np.arange(M)[:, None]
    frequency = np.where(mode < M // 2, mode, mode - M // 2 + 1)
    phase = 2.0 * np.pi * frequency * np.arange(G)[None, :] / G
    wave = np.where(mode < M // 2, np.cos(phase), np.sin(phase))
    wave = wave * np.where(mode == 0, np.sqrt(1.0 / G), np.sqrt(2.0 / G))
    high = wave.astype(np.float32).astype(jnp.bfloat16)
    low = (wave - high.astype(np.float64)).astype(np.float32).astype(jnp.bfloat16)
    return np.concatenate([high, low], axis=1)


def around(shard, stage, s):
    if stage == "y":
        return lax.ppermute(shard, "y", [(i, (i + s) % 4) for i in range(4)])
    pairs = []
    for z in range(4):
        for core in range(2):
            for b in range(4):
                along_b = (core == 0) == (stage == "wide")
                to = (z, (b + s) % 4) if along_b else ((z + s) % 4, b)
                pairs.append(((z * 2 + core) * 4 + b, (to[0] * 2 + core) * 4 + to[1]))
    return lax.ppermute(shard, ("z", "core", "ba"), pairs)


def from_others(pieces, stage):
    got = [pieces[0]]
    for s in (1, 2, 3):
        got.append(around(pieces[s], stage, s))
    return tuple(got)


def swapped(shard):
    return lax.ppermute(shard, "core", [(0, 1), (1, 0)])


def per_device(
    features,
    tile_ids,
    cell_ids,
    spread_weight,
    read_weight,
    message_weight,
    skip_weight,
    spectral_weight,
    hidden_weight,
    output_weight,
):
    points, width = features.shape
    everyone = ("z", "y", "core", "ba")
    devices = lax.axis_size(everyone)
    shape = jax.ShapeDtypeStruct
    where = lax.axis_index(everyone).astype(jnp.int32).reshape(1)
    tile = tile_ids.reshape(1, points)
    cell = cell_ids.reshape(1, points)
    terms = basis_terms()
    basis = jnp.asarray(terms)
    basis_tall = jnp.asarray(np.ascontiguousarray(terms.T))

    anywhere = pl.BlockSpec(memory_space=pl.ANY)
    send, slots, message = pl.pallas_call(
        spread_body,
        out_shape=(
            shape((devices, 56, 128), BF16),
            shape((1, points), jnp.int32),
            shape((points, width), BF16),
        ),
        in_specs=[VMEM] * 5,
        out_specs=[anywhere, VMEM, anywhere],
        scratch_shapes=[
            pltpu.VMEM((1, points), jnp.int32),
            pltpu.VMEM((points, width), BF16),
            pltpu.VMEM((points, 128), BF16),
            pltpu.VMEM((devices, 56, 128), BF16),
            pltpu.SemaphoreType.DMA((5,)),
        ],
        name="spread",
        compiler_params=pltpu.CompilerParams(vmem_limit_bytes=60 * 2**20),
    )(features, tile, cell, spread_weight.reshape(1, points), message_weight)
    recv = lax.all_to_all(send, everyone, 0, 0, tiled=True)
    away = spectrum(message, tile, cell, basis, where, True)
    near = spectrum(message, tile, cell, basis, where, False)
    wave_p, wave_qz = call(
        waves_body,
        (shape((points, 1024), BF16), shape((points, 1024), BF16)),
        (tile, cell, basis_tall, where),
        (
            pltpu.VMEM((8, points), jnp.int32),
            pltpu.VMEM((256, 1024), BF16),
            pltpu.VMEM((256, 1024), BF16),
            pltpu.VMEM((128, 256), BF16),
        ),
        flops=10**9,
        scalars=1,
    )
    parts = add_and_cut((near, swapped(away)))
    parts = add_and_cut(from_others(parts, "wide"))
    parts = add_and_cut(from_others(parts, "near"))
    latent, places = call(
        collect_body,
        (shape((2048, width), BF16), shape((1024, 128), BF16)),
        (recv,),
        (pltpu.VMEM((3072, width), BF16), pltpu.VMEM((8, 8, 128), jnp.int32)),
        flops=2 * 3072 * 2048 * 256,
    )
    back = pl.pallas_call(
        reply_body,
        out_shape=shape((devices, 24, width), BF16),
        in_specs=[VMEM, VMEM, anywhere],
        out_specs=anywhere,
        scratch_shapes=[
            pltpu.VMEM((devices, 24, width), BF16),
            pltpu.SemaphoreType.DMA((4,)),
        ],
        name="reply",
        compiler_params=pltpu.CompilerParams(vmem_limit_bytes=20 * 2**20),
        cost_estimate=pl.CostEstimate(
            flops=2 * 3072 * 2048 * 256, transcendentals=0, bytes_accessed=4000000
        ),
    )(latent, places, spectral_weight)
    mixed = call(
        mix_body, shape((32, width), BF16), from_others(parts, "y") + (spectral_weight,), ()
    )
    line = joined(from_others((mixed,) * 4, "y"))
    plane = joined(from_others((line,) * 4, "near"))
    modes = from_others((plane,) * 4, "wide")
    modes = modes + tuple(swapped(m) for m in modes)

    returned = lax.all_to_all(back, everyone, 0, 0, tiled=True)
    base = call(
        own_body,
        shape((points, width), F32),
        (returned.reshape(devices * 24, width), slots, skip_weight),
        (),
        flops=2 * 3072 * 2048 * 256,
    )
    base = call(
        begin_body,
        shape((points, width), F32),
        (modes[0], modes[4], wave_p, wave_qz, base),
        (),
        flops=2 * 1024 * 2048 * 256,
    )
    arrays = modes[1:4] + modes[5:]
    arrays = arrays + (wave_p, wave_qz, base, read_weight.reshape(1, points))
    arrays = arrays + (hidden_weight, output_weight)
    return pl.pallas_call(
        decode_body,
        out_shape=shape((points, width), BF16),
        in_specs=[VMEM] * len(arrays),
        out_specs=anywhere,
        scratch_shapes=[pltpu.VMEM((points, width), BF16), pltpu.SemaphoreType.DMA((2,))],
        name="decode",
        compiler_params=pltpu.CompilerParams(vmem_limit_bytes=32 * 2**20),
        cost_estimate=pl.CostEstimate(
            flops=2 * 4096 * 2048 * 256, transcendentals=0, bytes_accessed=4000000
        ),
    )(*arrays)


def solution(mesh):
    finer = Mesh(mesh.devices.reshape(4, 4, 2, 4), ("z", "y", "core", "ba"))
    rows = P(("z", "y", "core", "ba"))
    every = P()
    placed = (
        P(("z", "y", "core", "ba"), None),
        P(("z", "y", "core", "ba"), None),
        rows,
        rows,
        rows,
        every,
        every,
        P("ba", ("z", "y", "core"), None, None),
        every,
        every,
    )

    return jax.shard_map(
        per_device,
        mesh=finer,
        in_specs=placed,
        out_specs=P(("z", "y", "core", "ba"), None),
        check_vma=False,
    )
```
